32 devices in a mesh: gx: 4 (over z), gy: 8 (over y, x, core).
Axes of the slice: x: 2, y: 2, z: 4, core: 2. Of those that a mesh axis runs over, the one named last changes fastest.
Arguments:
- matrix_rows: float32 [4096, 1024], P(('gx', 'gy')), may hold values from -1.1 to 1.1
- tile_owner: int32 [136], replicated, may hold values from 0 to 31, as said below
- tile_slot: int32 [136], replicated, may hold values from 0 to 4, as said below
Outputs:
- packed_tiles: float32 [160, 256, 256], P(('gx', 'gy'))
The draws below stay inside these ranges and needn't reach their ends.
Inputs may be any that keep to these rules, and one draw needn't show every extreme that they name: `tile_owner`: give tile (I, J) the class (c, r) as follows, with a = I // 4, b = J // 4, i = I % 4, j = J % 4: if a == b, c = a and r = i when i - j < 2, else r = j; if a > b and (a - b > 2, or a - b == 2 with i + j even), c = b and r = i; otherwise c = a and r = j. The owner of a class (c, r) tile is one of the devices c * 8 to c * 8 + 7. Every owner holds 4 or 5 tiles. At most 2 tiles of one class share an owner, and in every draw some owner holds exactly 2 tiles of one class. `tile_slot`: the tiles of one owner take the slots 0 to their count - 1, each once.
All inputs are finite; a program needn't handle non-finite values.
Results may differ from the reference program's by a relative error of at most 0.0003.
Values sent between devices are 32-bit elements; how exact they have to be, the bound alone decides.
A program may use at most 128 MiB of HBM per device.

```python
import jax
import jax.numpy as jnp
import numpy as np
from jax import lax

WIDTH = 1024
TILE = 256
ORDER = 4096
TILE_COUNT = 16
HALF_TILES = 4
LOWER_COUNT = 136
SLOTS = 5
N_GX = 4
N_GY = 8
DEVICES = 32


def tile_classes():
    lower_i, lower_j = np.tril_indices(TILE_COUNT)
    group_a = lower_i // HALF_TILES
    group_b = lower_j // HALF_TILES
    inner_i = lower_i % HALF_TILES
    inner_j = lower_j % HALF_TILES
    same = group_a == group_b
    within_row = inner_i - inner_j < HALF_TILES // 2
    gap = group_a - group_b
    across_row = (gap > N_GX // 2) | (gap == N_GX // 2) & ((inner_i + inner_j) % 2 == 0)
    rowwise = np.where(same, within_row, across_row)
    class_x = np.where(same | ~rowwise, group_a, group_b)
    class_r = np.where(rowwise, inner_i, inner_j)
    return (class_x.astype(np.int32), class_r.astype(np.int32))


def owner_table(key):
    class_x, class_r = tile_classes()
    set_id = jnp.asarray(class_x * HALF_TILES + class_r, jnp.int32)
    row_of = jnp.asarray(class_x, jnp.int32)
    set_rank = jax.random.permutation(jax.random.fold_in(key, 11), TILE_COUNT).astype(jnp.int32)
    tile_rank = jax.random.permutation(jax.random.fold_in(key, 12), LOWER_COUNT).astype(jnp.int32)
    score = (row_of * TILE_COUNT + set_rank[set_id]) * LOWER_COUNT + tile_rank
    order = jnp.argsort(score, stable=True).astype(jnp.int32)
    position = jnp.zeros((LOWER_COUNT,), jnp.int32).at[order].set(jnp.arange(LOWER_COUNT, dtype=jnp.int32))
    per_row = LOWER_COUNT // N_GX
    inside_row = position % per_row
    row_keys = jax.random.split(jax.random.fold_in(key, 13), N_GX)
    owner_order = jax.vmap(lambda one: jax.random.permutation(one, N_GY))(row_keys).astype(jnp.int32)
    owners = row_of * N_GY + owner_order[row_of, inside_row % N_GY]
    slot_index = inside_row // N_GY
    return (owners.astype(jnp.int32), slot_index.astype(jnp.int32))


def draw_tile_owner(key, part):
    return owner_table(key)[0]


def draw_tile_slot(key, part):
    return owner_table(key)[1]


def shard_levels(own_key, dims, shards, smallest, largest):
    def one(dim, shards_of):
        heights = jax.random.uniform(jax.random.fold_in(jax.random.fold_in(own_key, 6), dim), (shards_of,), jnp.float32, smallest / len(shards), largest / len(shards))
        return jnp.repeat(jnp.exp(heights), dims[dim] // shards_of).reshape((-1,) + (1,) * (len(dims) - dim - 1))

    level = one(*shards[0])
    for cut in shards[1:]:
        level = level * one(*cut)
    return level


def normal_values(stream_key, extent, width, limit, pieces=(), kind=jnp.bfloat16):
    gain = shard_levels(stream_key, extent, pieces, -0.22, 0.18) if pieces else 1.0
    values = jax.random.normal(stream_key, extent, jnp.float32) * width * gain
    return jnp.minimum(jnp.maximum(values, -limit), limit).astype(kind)


def setup_inputs(seed: int = 0) -> dict:
    splits = jax.random.split(jax.random.key(seed), 4)
    matrix_rows = normal_values(splits[0], (ORDER, WIDTH), 0.177, 1.1, ((0, 32),), jnp.float32)
    tile_owner = draw_tile_owner(jax.random.fold_in(splits[3], 71), 0)
    tile_slot = draw_tile_slot(jax.random.fold_in(splits[3], 71), 0)
    return dict(matrix_rows=matrix_rows, tile_owner=tile_owner, tile_slot=tile_slot)


def reference(matrix_rows, tile_owner, tile_slot):
    lower_i, lower_j = np.tril_indices(TILE_COUNT)
    row_table = jnp.asarray(lower_i, jnp.int32)
    col_table = jnp.asarray(lower_j, jnp.int32)
    blocks = matrix_rows.reshape(TILE_COUNT, TILE, WIDTH)
    inside = lax.broadcasted_iota(jnp.int32, (TILE, TILE), 0)
    across = lax.broadcasted_iota(jnp.int32, (TILE, TILE), 1)

    def one_tile(index):
        row_tile = row_table[index]
        col_tile = col_table[index]
        product = lax.dot_general(blocks[row_tile], blocks[col_tile], (((1,), (1,)), ((), ())),
                                  precision=lax.Precision.HIGHEST, preferred_element_type=jnp.float32)
        upper = jnp.logical_and(row_tile == col_tile, inside < across)
        return jnp.where(upper, jnp.float32(0.0), product)

    tiles = lax.map(one_tile, jnp.arange(LOWER_COUNT, dtype=jnp.int32))
    packed = jnp.zeros((DEVICES, SLOTS, TILE, TILE), jnp.float32)
    packed = packed.at[tile_owner, tile_slot].set(tiles)
    return packed.reshape(DEVICES * SLOTS, TILE, TILE)
```

```python
import functools

import jax
import jax.numpy as jnp
from jax import lax
from jax.experimental import pallas as pl
from jax.experimental.pallas import tpu as pltpu
from jax.sharding import PartitionSpec as P

MESH = pl.DeviceIdType.MESH


def chip_position(chip, chips):
    row, col = lax.div(chip, 2), lax.rem(chip, 2)
    return col * (1 + row) + (1 - col) * lax.rem(chips - row, chips)


def chip_at(position, chips):
    behind = lax.rem(position + chips - 1, chips)
    far = lax.div(behind, chips // 2)
    return (1 - far) * (2 * behind + 1) + far * 2 * (chips - 1 - behind)


def piece_lists(half_tiles, half_x):
    lists, start = [], 0
    for step in range(half_x + 1):
        if step == 0:
            count = half_tiles // 2 + 1
        elif step < half_x:
            count = half_tiles
        else:
            count = half_tiles // 2
        lists.append((step, start, count))
        start += count
    return lists, start


def piece(x, r, step, i, nx, half_tiles, half_x):
    source = lax.rem(x - step + nx, nx)
    if step == 0:
        col = lax.rem(r - i + half_tiles, half_tiles)
        valid = jnp.logical_or(i < half_tiles // 2, r < half_tiles // 2)
        rowwise = col <= r
    elif step < half_x:
        col = i
        valid = i >= 0
        rowwise = source > x
    else:
        flag = jnp.where(x >= half_x, 1, 0)
        col = 2 * i + lax.rem(r + flag, 2)
        valid = i >= 0
        rowwise = source > x
    other, mine = source * half_tiles + r, x * half_tiles + col
    row_tile = jnp.where(rowwise, other, mine)
    col_tile = jnp.where(rowwise, mine, other)
    tile = jnp.where(valid, row_tile * (row_tile + 1) // 2 + col_tile, 0)
    return col, valid, rowwise, tile


def kernel(
    dims, rows_ref, owner_ref, slot_ref, out_ref,
    gath, zbuf, chi, clo, zsplit, pieces, outgoing, incoming, targets,
    gs_r, gr_r, gs_l, gr_l, ss, sr, zs, zr, xs, xr,
):
    nx, ny, half_tiles, half_x, capacity, slots = dims
    rows = rows_ref.shape[0]
    half = rows // 2
    chips = ny // 2
    reach = chips // 2
    x = lax.axis_index("gx")
    y = lax.axis_index("gy")
    core = lax.rem(y, 2)
    chip = lax.div(y, 2)
    right_x, left_x = lax.rem(x + 1, nx), lax.rem(x + nx - 1, nx)
    sibling = y + 1 - 2 * core
    place = chip_position(chip, chips)

    def at(position):
        return 2 * chip_at(lax.rem(position + chips, chips), chips) + core

    next_y, prev_y = at(place + 1), at(place - 1)
    lists, piece_count = piece_lists(half_tiles, half_x)

    barrier = pltpu.get_barrier_semaphore()
    for other in (right_x, left_x):
        pl.semaphore_signal(barrier, inc=1, device_id=(other, y), device_id_type=MESH)
    for offset in range(1, ny):
        pl.semaphore_signal(
            barrier, inc=1, device_id=(x, lax.rem(y + offset, ny)), device_id_type=MESH
        )
    pl.semaphore_wait(barrier, ny + 1)

    started = []

    def send(src, dst, send_sem, recv_sem, target):
        copy = pltpu.make_async_remote_copy(
            src_ref=src, dst_ref=dst, send_sem=send_sem, recv_sem=recv_sem,
            device_id=target, device_id_type=MESH,
        )
        copy.start()
        started.append(copy)

    def part(h):
        return pl.ds(h * half, half)

    def zcopy(step, h):
        src = rows_ref.at[part(h)] if step == 1 else zbuf.at[step - 2, part(h)]
        send(src, zbuf.at[step - 1, part(h)], zs.at[step - 1, h], zr.at[step - 1, h], (right_x, y))

    def block(owner, h):
        return gath.at[owner, part(h)]

    def ring(direction, distance, h):
        owner = at(place - direction * (distance - 1))
        src = rows_ref.at[part(h)] if distance == 1 else block(owner, h)
        s, r = (gs_r, gr_r) if direction == 1 else (gs_l, gr_l)
        target = next_y if direction == 1 else prev_y
        send(src, block(owner, h), s.at[distance - 1, h], r.at[distance - 1, h], (x, target))

    def cross(number, owner, h):
        src = rows_ref.at[part(h)] if number == 0 else block(owner, h)
        send(src, block(owner, h), ss.at[number, h], sr.at[number, h], (x, sibling))

    def halves_of(direction, distance):
        if distance < reach:
            return (0, 1) if direction == 1 else (1, 0)
        return (0,) if direction == 1 else (1,)

    def split(value, hi_ref, lo_ref, index):
        hi = value.astype(jnp.bfloat16)
        hi_ref[index] = hi
        lo_ref[index] = (value - hi.astype(jnp.float32)).astype(jnp.bfloat16)

    zcopy(1, 0)
    ring(1, 1, 0)
    if reach > 1:
        ring(-1, 1, 1)
        zcopy(1, 1)
        ring(1, 1, 1)
        ring(-1, 1, 0)
    else:
        ring(-1, 1, 1)
        zcopy(1, 1)
    cross(0, y, 0)
    cross(0, y, 1)

    for step, first, count in lists:
        def fill(i, carry, step=step, first=first):
            _, valid, _, tile = piece(x, chip, step, i, nx, half_tiles, half_x)
            targets[first + i] = jnp.where(valid, lax.rem(owner_ref[tile], ny), ny)
            return carry
        lax.fori_loop(0, count, fill, 0)

    me = x * ny + y

    def class_loop(r, carry):
        state = (jnp.int32(0),) + carry
        for step, first, count in lists:
            def look(i, state, step=step):
                seen, found = state[0], state[1:]
                _, valid, rowwise, tile = piece(x, r, step, i, nx, half_tiles, half_x)
                mine = jnp.where(valid, jnp.where(owner_ref[tile] == me, 1, 0), 0)
                slot = slot_ref[tile]
                code = 2 * (r * capacity + jnp.minimum(seen, capacity - 1))
                code = code + jnp.where(rowwise, 1, 0)
                key = jnp.where(mine == 1, slot, slots)
                found = tuple(jnp.where(key == s, code, found[s]) for s in range(slots))
                return (seen + mine,) + found
            state = lax.fori_loop(0, count, look, state)
        return state[1:]

    found = lax.fori_loop(0, half_tiles, class_loop, (jnp.int32(-1),) * slots)

    chosen = []
    for offset in range(ny):
        dest = lax.rem(y + offset, ny)

        def pick(p, state, dest=dest):
            hit = jnp.where(targets[p] == dest, 1, 0)
            seen = state[0]
            key = jnp.where(hit == 1, seen, capacity)
            picks = tuple(jnp.where(key == k, p, state[1 + k]) for k in range(capacity))
            return (seen + hit,) + picks

        chosen.append(lax.fori_loop(0, piece_count, pick, (jnp.int32(0),) * (capacity + 1))[1:])

    def wait_recv(dst, sem):
        pltpu.make_async_remote_copy(
            src_ref=dst, dst_ref=dst, send_sem=sem, recv_sem=sem,
            device_id=(x, sibling), device_id_type=MESH,
        ).wait_recv()

    def split_other(step, h):
        ref = rows_ref.at[part(h)] if step == 0 else zbuf.at[step - 1, part(h)]
        value = ref[...]
        hi = value.astype(jnp.bfloat16)
        zsplit[step, h, :half] = hi
        zsplit[step, h, half:] = (value - hi.astype(jnp.float32)).astype(jnp.bfloat16)

    def take_other(step, h):
        wait_recv(zbuf.at[step - 1, part(h)], zr.at[step - 1, h])
        if step < half_x:
            zcopy(step + 1, h)

    split_other(0, 0)
    split_other(0, 1)
    split(rows_ref[...], chi, clo, y)

    def take_cross(number, owner, halves):
        for h in halves:
            wait_recv(block(owner, h), sr.at[number, h])

    one = functools.partial(
        lax.dot_general,
        dimension_numbers=(((1,), (1,)), ((), ())),
        preferred_element_type=jnp.float32,
    )
    width = rows_ref.shape[1]
    row_inside = core * rows + lax.broadcasted_iota(jnp.int32, (half, 2 * rows), 0)
    col_inside = lax.broadcasted_iota(jnp.int32, (half, 2 * rows), 1)

    def one_piece_of(h):
        above = jnp.where(row_inside + h * half < col_inside, 1, 0)

        def one_piece(i, step, first, col):
            b_hi = chi[pl.ds(2 * col, 2)].reshape(2 * rows, width)
            b_lo = clo[pl.ds(2 * col, 2)].reshape(2 * rows, width)
            both = one(zsplit[step, h], b_hi)
            full = both[:half] + (both[half:] + one(zsplit[step, h, :half], b_lo))
            if step == 0:
                full = jnp.where(above * jnp.where(i == 0, 1, 0) == 1, 0.0, full)
            pieces[h, first + i, 0] = full[:, :rows]
            pieces[h, first + i, 1] = full[:, rows:]

        return one_piece

    farthest = chip_at(lax.rem(place + reach, chips), chips)
    soon = min(reach, half_x) if reach > 1 else 0

    def multiply(h, mode):
        one_piece = one_piece_of(h)
        for step, first, count in lists:
            if mode == "early" and step >= soon:
                continue

            def make(i, carry, step=step, first=first):
                col, _, _, _ = piece(x, chip, step, i, nx, half_tiles, half_x)
                if mode == "all" or step >= soon:
                    one_piece(i, step, first, col)
                else:
                    wanted = (col != farthest) if mode == "early" else (col == farthest)
                    pl.when(wanted)(lambda: one_piece(i, step, first, col))
                return carry
            lax.fori_loop(0, count, make, 0)

    pending = [(0, sibling, (0, 1))]
    for distance in range(1, reach + 1):
        if distance == reach:
            for number, owner, halves in pending[1:]:
                take_cross(number, owner, halves)
                split(gath[owner], chi, clo, owner)
            multiply(0, "early")
        if distance <= half_x:
            for h in (0, 1):
                if (distance, h) != (half_x, 1):
                    take_other(distance, h)
                if h in halves_of(1, distance):
                    owner = at(place - distance)
                    wait_recv(block(owner, h), gr_r.at[distance - 1, h])
                    if distance < reach and h in halves_of(1, distance + 1):
                        ring(1, distance + 1, h)
                    cross(2 * distance - 1, owner, h)
                g = 1 - h
                if g in halves_of(-1, distance):
                    owner = at(place + distance)
                    wait_recv(block(owner, g), gr_l.at[distance - 1, g])
                    if distance < reach and g in halves_of(-1, distance + 1):
                        ring(-1, distance + 1, g)
                    cross(2 * distance, owner, g)
            split_other(distance, 0)
            if distance < half_x:
                split_other(distance, 1)
        behind, ahead = at(place - distance), at(place + distance)
        pending.append((2 * distance - 1, behind + 1 - 2 * core, halves_of(1, distance)))
        pending.append((2 * distance, ahead + 1 - 2 * core, halves_of(-1, distance)))
        split(gath[behind], chi, clo, behind)
        if distance < reach:
            split(gath[ahead], chi, clo, ahead)
        for number, owner, halves in pending[: (1 if distance == 1 else 0)]:
            take_cross(number, owner, halves)
            split(gath[owner], chi, clo, owner)
    for number, owner, halves in pending[-2:]:
        take_cross(number, owner, halves)
    split(gath[pending[-1][1]], chi, clo, pending[-1][1])
    for step in range(reach + 1, half_x + 1):
        for h in (0, 1):
            if (step, h) != (half_x, 1):
                take_other(step, h)
                split_other(step, h)

    def arrival(offset):
        return pl.ds(offset * capacity * 2, capacity * 2)

    def exchange(h, offset):
        send(
            outgoing.at[h, offset], incoming.at[h, arrival(offset)],
            xs.at[h, offset], xr.at[h, offset], (x, lax.rem(y + offset, ny)),
        )

    for h in (0, 1):
        if h == 1:
            take_other(half_x, 1)
            split_other(half_x, 1)
        multiply(h, "all" if h == 1 else "late")
        for offset in range(1, ny):
            for k in range(capacity):
                outgoing[h, offset, 2 * k:2 * k + 2] = pieces[h, chosen[offset][k]]
            if offset > 1:
                exchange(h, offset - 1)
        for k in range(capacity):
            incoming[h, 2 * k:2 * k + 2] = pieces[h, chosen[0][k]]
        exchange(h, ny - 1)
    for h in (0, 1):
        for offset in range(1, ny):
            wait_recv(incoming.at[h, arrival(offset)], xr.at[h, offset])

    for s in range(slots):
        code = found[s]
        there = code >= 0
        safe = jnp.maximum(code, 0)
        rowwise = lax.rem(safe, 2) == 1
        rank = lax.rem(safe // 2, capacity)
        first_source = 2 * (safe // (2 * capacity))
        bases = [
            (lax.rem(y - first_source - h + ny, ny) * capacity + rank) * 2 for h in (0, 1)
        ]
        for i in (0, 1):
            for j in (0, 1):
                place_of = jnp.where(rowwise, bases[i] + j, bases[j] + i)
                value = jnp.concatenate([incoming[0, place_of], incoming[1, place_of]], axis=0)
                value = jnp.where(rowwise, value, value.T)
                out_ref[s, i * rows:(i + 1) * rows, j * rows:(j + 1) * rows] = jnp.where(
                    there, value, 0.0
                )
    for copy in started:
        copy.wait_send()


def copy_out(in_ref, out_ref, sem):
    copy = pltpu.make_async_copy(in_ref, out_ref, sem)
    copy.start()
    copy.wait()


def per_device(mesh_shape, matrix_rows, tile_owner, tile_slot):
    nx, ny = mesh_shape
    rows, width = matrix_rows.shape
    half_tiles, half_x = ny // 2, nx // 2
    capacity = nx // 4 + 1
    slots = -(-tile_owner.shape[0] // (nx * ny))
    _, piece_count = piece_lists(half_tiles, half_x)
    reach = max(ny // 4, 1)
    f32, bf16 = jnp.float32, jnp.bfloat16
    dma = pltpu.SemaphoreType.DMA
    packed = pl.pallas_call(
        functools.partial(kernel, (nx, ny, half_tiles, half_x, capacity, slots)),
        out_shape=jax.ShapeDtypeStruct((slots, 2 * rows, 2 * rows), f32),
        in_specs=[
            pl.BlockSpec(memory_space=pltpu.VMEM),
            pl.BlockSpec(memory_space=pltpu.SMEM),
            pl.BlockSpec(memory_space=pltpu.SMEM),
        ],
        out_specs=pl.BlockSpec(memory_space=pltpu.VMEM),
        scratch_shapes=[
            pltpu.VMEM((ny, rows, width), f32),
            pltpu.VMEM((half_x, rows, width), f32),
            pltpu.VMEM((ny, rows, width), bf16),
            pltpu.VMEM((ny, rows, width), bf16),
            pltpu.VMEM((half_x + 1, 2, rows, width), bf16),
            pltpu.VMEM((2, piece_count, 2, rows // 2, rows), f32),
            pltpu.VMEM((2, ny, 2 * capacity, rows // 2, rows), f32),
            pltpu.VMEM((2, ny * 2 * capacity, rows // 2, rows), f32),
            pltpu.SMEM((piece_count,), jnp.int32),
            dma((reach, 2)), dma((reach, 2)), dma((reach, 2)), dma((reach, 2)),
            dma((2 * reach + 1, 2)), dma((2 * reach + 1, 2)),
            dma((half_x, 2)), dma((half_x, 2)),
            dma((2, ny)), dma((2, ny)),
        ],
        compiler_params=pltpu.CompilerParams(
            collective_id=0, has_side_effects=True, vmem_limit_bytes=44 * 1024 * 1024
        ),
    )(matrix_rows, tile_owner, tile_slot)
    return pl.pallas_call(
        copy_out,
        out_shape=jax.ShapeDtypeStruct(packed.shape, packed.dtype),
        in_specs=[pl.BlockSpec(memory_space=pltpu.VMEM)],
        out_specs=pl.BlockSpec(memory_space=pl.ANY),
        scratch_shapes=[pltpu.SemaphoreType.DMA(())],
        compiler_params=pltpu.CompilerParams(vmem_limit_bytes=4 * 1024 * 1024),
    )(packed)


def solution(mesh):
    placed = (P(("gx", "gy"), None), P(), P())
    return jax.shard_map(
        functools.partial(per_device, (mesh.shape["gx"], mesh.shape["gy"])),
        mesh=mesh,
        in_specs=placed,
        out_specs=P(("gx", "gy"), None, None),
        check_vma=False,
    )
```

```python
import functools

import jax
import jax.numpy as jnp
from jax import lax
from jax.experimental import pallas as pl
from jax.experimental.pallas import tpu as pltpu
from jax.sharding import PartitionSpec as P

MESH = pl.DeviceIdType.MESH


def chip_position(chip, chips):
    row, col = lax.div(chip, 2), lax.rem(chip, 2)
    return col * (1 + row) + (1 - col) * lax.rem(chips - row, chips)


def chip_at(position, chips):
    behind = lax.rem(position + chips - 1, chips)
    far = lax.div(behind, chips // 2)
    return (1 - far) * (2 * behind + 1) + far * 2 * (chips - 1 - behind)


def piece_lists(half_tiles, half_x):
    lists, start = [], 0
    for step in range(half_x + 1):
        if step == 0:
            count = half_tiles // 2 + 1
        elif step < half_x:
            count = half_tiles
        else:
            count = half_tiles // 2
        lists.append((step, start, count))
        start += count
    return lists, start


def piece(x, r, step, i, nx, half_tiles, half_x):
    source = lax.rem(x - step + nx, nx)
    if step == 0:
        col = lax.rem(r - i + half_tiles, half_tiles)
        valid = jnp.logical_or(i < half_tiles // 2, r < half_tiles // 2)
        rowwise = col <= r
    elif step < half_x:
        col = i
        valid = i >= 0
        rowwise = source > x
    else:
        flag = jnp.where(x >= half_x, 1, 0)
        col = 2 * i + lax.rem(r + flag, 2)
        valid = i >= 0
        rowwise = source > x
    other, mine = source * half_tiles + r, x * half_tiles + col
    row_tile = jnp.where(rowwise, other, mine)
    col_tile = jnp.where(rowwise, mine, other)
    tile = jnp.where(valid, row_tile * (row_tile + 1) // 2 + col_tile, 0)
    return col, valid, rowwise, tile


def kernel(
    dims, rows_ref, owner_ref, slot_ref, out_ref,
    gath, zbuf, chi, clo, zsplit, pieces, outgoing, incoming, targets,
    gs_r, gr_r, gs_l, gr_l, ss, sr, zs, zr, xs, xr,
):
    nx, ny, half_tiles, half_x, capacity, slots = dims
    rows = rows_ref.shape[0]
    half = rows // 2
    chips = ny // 2
    reach = chips // 2
    x = lax.axis_index("gx")
    y = lax.axis_index("gy")
    core = lax.rem(y, 2)
    chip = lax.div(y, 2)
    right_x, left_x = lax.rem(x + 1, nx), lax.rem(x + nx - 1, nx)
    sibling = y + 1 - 2 * core
    place = chip_position(chip, chips)

    def at(position):
        return 2 * chip_at(lax.rem(position + chips, chips), chips) + core

    next_y, prev_y = at(place + 1), at(place - 1)
    lists, piece_count = piece_lists(half_tiles, half_x)

    barrier = pltpu.get_barrier_semaphore()
    for other in (right_x, left_x):
        pl.semaphore_signal(barrier, inc=1, device_id=(other, y), device_id_type=MESH)
    for offset in range(1, ny):
        pl.semaphore_signal(
            barrier, inc=1, device_id=(x, lax.rem(y + offset, ny)), device_id_type=MESH
        )
    pl.semaphore_wait(barrier, ny + 1)

    started = []

    def send(src, dst, send_sem, recv_sem, target):
        copy = pltpu.make_async_remote_copy(
            src_ref=src, dst_ref=dst, send_sem=send_sem, recv_sem=recv_sem,
            device_id=target, device_id_type=MESH,
        )
        copy.start()
        started.append(copy)

    def part(h):
        return pl.ds(h * half, half)

    def zcopy(step, h):
        src = rows_ref.at[part(h)] if step == 1 else zbuf.at[step - 2, part(h)]
        send(src, zbuf.at[step - 1, part(h)], zs.at[step - 1, h], zr.at[step - 1, h], (right_x, y))

    def block(owner, h):
        return gath.at[owner, part(h)]

    def ring(direction, distance, h):
        owner = at(place - direction * (distance - 1))
        src = rows_ref.at[part(h)] if distance == 1 else block(owner, h)
        s, r = (gs_r, gr_r) if direction == 1 else (gs_l, gr_l)
        target = next_y if direction == 1 else prev_y
        send(src, block(owner, h), s.at[distance - 1, h], r.at[distance - 1, h], (x, target))

    def cross(number, owner, h):
        src = rows_ref.at[part(h)] if number == 0 else block(owner, h)
        send(src, block(owner, h), ss.at[number, h], sr.at[number, h], (x, sibling))

    def halves_of(direction, distance):
        if distance < reach:
            return (0, 1) if direction == 1 else (1, 0)
        return (0,) if direction == 1 else (1,)

    def split(value, hi_ref, lo_ref, index):
        hi = value.astype(jnp.bfloat16)
        hi_ref[index] = hi
        lo_ref[index] = (value - hi.astype(jnp.float32)).astype(jnp.bfloat16)

    zcopy(1, 0)
    ring(1, 1, 0)
    if reach > 1:
        ring(-1, 1, 1)
        zcopy(1, 1)
        ring(1, 1, 1)
        ring(-1, 1, 0)
    else:
        ring(-1, 1, 1)
        zcopy(1, 1)
    cross(0, y, 0)
    cross(0, y, 1)

    for step, first, count in lists:
        def fill(i, carry, step=step, first=first):
            _, valid, _, tile = piece(x, chip, step, i, nx, half_tiles, half_x)
            targets[first + i] = jnp.where(valid, lax.rem(owner_ref[tile], ny), ny)
            return carry
        lax.fori_loop(0, count, fill, 0)

    me = x * ny + y

    def class_loop(r, carry):
        state = (jnp.int32(0),) + carry
        for step, first, count in lists:
            def look(i, state, step=step):
                seen, found = state[0], state[1:]
                _, valid, rowwise, tile = piece(x, r, step, i, nx, half_tiles, half_x)
                mine = jnp.where(valid, jnp.where(owner_ref[tile] == me, 1, 0), 0)
                slot = slot_ref[tile]
                code = 2 * (r * capacity + jnp.minimum(seen, capacity - 1))
                code = code + jnp.where(rowwise, 1, 0)
                key = jnp.where(mine == 1, slot, slots)
                found = tuple(jnp.where(key == s, code, found[s]) for s in range(slots))
                return (seen + mine,) + found
            state = lax.fori_loop(0, count, look, state)
        return state[1:]

    found = lax.fori_loop(0, half_tiles, class_loop, (jnp.int32(-1),) * slots)

    chosen = []
    for offset in range(ny):
        dest = lax.rem(y + offset, ny)

        def pick(p, state, dest=dest):
            hit = jnp.where(targets[p] == dest, 1, 0)
            seen = state[0]
            key = jnp.where(hit == 1, seen, capacity)
            picks = tuple(jnp.where(key == k, p, state[1 + k]) for k in range(capacity))
            return (seen + hit,) + picks

        chosen.append(lax.fori_loop(0, piece_count, pick, (jnp.int32(0),) * (capacity + 1))[1:])

    def wait_recv(dst, sem):
        pltpu.make_async_remote_copy(
            src_ref=dst, dst_ref=dst, send_sem=sem, recv_sem=sem,
            device_id=(x, sibling), device_id_type=MESH,
        ).wait_recv()

    def split_other(step, h):
        ref = rows_ref.at[part(h)] if step == 0 else zbuf.at[step - 1, part(h)]
        value = ref[...]
        hi = value.astype(jnp.bfloat16)
        zsplit[step, h, :half] = hi
        zsplit[step, h, half:] = (value - hi.astype(jnp.float32)).astype(jnp.bfloat16)

    def take_other(step, h):
        wait_recv(zbuf.at[step - 1, part(h)], zr.at[step - 1, h])
        if step < half_x:
            zcopy(step + 1, h)

    split_other(0, 0)
    split_other(0, 1)
    split(rows_ref[...], chi, clo, y)

    def take_cross(number, owner, halves):
        for h in halves:
            wait_recv(block(owner, h), sr.at[number, h])

    one = functools.partial(
        lax.dot_general,
        dimension_numbers=(((1,), (1,)), ((), ())),
        preferred_element_type=jnp.float32,
    )
    width = rows_ref.shape[1]
    row_inside = core * rows + lax.broadcasted_iota(jnp.int32, (half, 2 * rows), 0)
    col_inside = lax.broadcasted_iota(jnp.int32, (half, 2 * rows), 1)

    def one_piece_of(h):
        above = jnp.where(row_inside + h * half < col_inside, 1, 0)

        def one_piece(i, step, first, col):
            b_hi = chi[pl.ds(2 * col, 2)].reshape(2 * rows, width)
            b_lo = clo[pl.ds(2 * col, 2)].reshape(2 * rows, width)
            both = one(zsplit[step, h], b_hi)
            full = both[:half] + (both[half:] + one(zsplit[step, h, :half], b_lo))
            if step == 0:
                full = jnp.where(above * jnp.where(i == 0, 1, 0) == 1, 0.0, full)
            pieces[h, first + i, 0] = full[:, :rows]
            pieces[h, first + i, 1] = full[:, rows:]

        return one_piece

    farthest = chip_at(lax.rem(place + reach, chips), chips)
    soon = min(reach, half_x) if reach > 1 else 0

    def multiply(h, mode):
        one_piece = one_piece_of(h)
        for step, first, count in lists:
            if mode == "early" and step >= soon:
                continue

            def make(i, carry, step=step, first=first):
                col, _, _, _ = piece(x, chip, step, i, nx, half_tiles, half_x)
                if mode == "all" or step >= soon:
                    one_piece(i, step, first, col)
                else:
                    wanted = (col != farthest) if mode == "early" else (col == farthest)
                    pl.when(wanted)(lambda: one_piece(i, step, first, col))
                return carry
            lax.fori_loop(0, count, make, 0)

    pending = [(0, sibling, (0, 1))]
    for distance in range(1, reach + 1):
        if distance == reach:
            for number, owner, halves in pending[1:]:
                take_cross(number, owner, halves)
                split(gath[owner], chi, clo, owner)
            multiply(0, "early")
        if distance <= half_x:
            for h in (0, 1):
                if (distance, h) != (half_x, 1):
                    take_other(distance, h)
                if h in halves_of(1, distance):
                    owner = at(place - distance)
                    wait_recv(block(owner, h), gr_r.at[distance - 1, h])
                    if distance < reach and h in halves_of(1, distance + 1):
                        ring(1, distance + 1, h)
                    cross(2 * distance - 1, owner, h)
                g = 1 - h
                if g in halves_of(-1, distance):
                    owner = at(place + distance)
                    wait_recv(block(owner, g), gr_l.at[distance - 1, g])
                    if distance < reach and g in halves_of(-1, distance + 1):
                        ring(-1, distance + 1, g)
                    cross(2 * distance, owner, g)
            split_other(distance, 0)
            if distance < half_x:
                split_other(distance, 1)
        behind, ahead = at(place - distance), at(place + distance)
        pending.append((2 * distance - 1, behind + 1 - 2 * core, halves_of(1, distance)))
        pending.append((2 * distance, ahead + 1 - 2 * core, halves_of(-1, distance)))
        split(gath[behind], chi, clo, behind)
        if distance < reach:
            split(gath[ahead], chi, clo, ahead)
        for number, owner, halves in pending[: (1 if distance == 1 else 0)]:
            take_cross(number, owner, halves)
            split(gath[owner], chi, clo, owner)
    for number, owner, halves in pending[-2:]:
        take_cross(number, owner, halves)
    split(gath[pending[-1][1]], chi, clo, pending[-1][1])
    for step in range(reach + 1, half_x + 1):
        for h in (0, 1):
            if (step, h) != (half_x, 1):
                take_other(step, h)
                split_other(step, h)

    def arrival(offset):
        return pl.ds(offset * capacity * 2, capacity * 2)

    def exchange(h, offset):
        send(
            outgoing.at[h, offset], incoming.at[h, arrival(offset)],
            xs.at[h, offset], xr.at[h, offset], (x, lax.rem(y + offset, ny)),
        )

    for h in (0, 1):
        if h == 1:
            take_other(half_x, 1)
            split_other(half_x, 1)
        multiply(h, "all" if h == 1 else "late")
        for offset in range(1, ny):
            for k in range(capacity):
                outgoing[h, offset, 2 * k:2 * k + 2] = pieces[h, chosen[offset][k]]
            if offset > 1:
                exchange(h, offset - 1)
        for k in range(capacity):
            incoming[h, 2 * k:2 * k + 2] = pieces[h, chosen[0][k]]
        exchange(h, ny - 1)
    for h in (0, 1):
        for offset in range(1, ny):
            wait_recv(incoming.at[h, arrival(offset)], xr.at[h, offset])

    for s in range(slots):
        code = found[s]
        there = code >= 0
        safe = jnp.maximum(code, 0)
        rowwise = lax.rem(safe, 2) == 1
        rank = lax.rem(safe // 2, capacity)
        first_source = 2 * (safe // (2 * capacity))
        bases = [
            (lax.rem(y - first_source - h + ny, ny) * capacity + rank) * 2 for h in (0, 1)
        ]
        for i in (0, 1):
            for j in (0, 1):
                place_of = jnp.where(rowwise, bases[i] + j, bases[j] + i)
                value = jnp.concatenate([incoming[0, place_of], incoming[1, place_of]], axis=0)
                value = jnp.where(rowwise, value, value.T)
                out_ref[s, i * rows:(i + 1) * rows, j * rows:(j + 1) * rows] = jnp.where(
                    there, value, 0.0
                )
    for copy in started:
        copy.wait_send()


def plane_kernel(
    dims, rows_hbm, owner_hbm, slot_hbm, out_ref,
    gath, zfar, parts, far_parts, far, extra, owner_ref, slot_ref, todo,
    ins, ss, rs,
):
    nx, ny, half_tiles, slots = dims
    rows, width = zfar.shape
    half = rows // 2
    x = lax.axis_index("gx")
    y = lax.axis_index("gy")
    core = lax.rem(y, 2)
    chip = lax.div(y, 2)
    twin = 1 - core
    right, left = (lax.rem(x + 1, nx), y), (lax.rem(x + nx - 1, nx), y)
    sibling = (x, y + 1 - 2 * core)
    across = (x, y + 2 - 4 * lax.rem(chip, 2))
    along = (x, lax.rem(y + 4, ny))

    barrier = pltpu.get_barrier_semaphore()
    peers = (sibling, across, along, right, left)
    for other in peers:
        pl.semaphore_signal(barrier, inc=1, device_id=other, device_id_type=MESH)
    loads = [
        pltpu.make_async_copy(rows_hbm, gath.at[0, core], ins.at[0]),
        pltpu.make_async_copy(owner_hbm, owner_ref, ins.at[1]),
        pltpu.make_async_copy(slot_hbm, slot_ref, ins.at[2]),
    ]
    for copy in loads:
        copy.start()
    pl.semaphore_wait(barrier, len(peers))
    loads[0].wait()

    started, numbers = [], {}

    def number(name):
        return numbers.setdefault(name, len(numbers))

    def send(name, src, dst, target):
        i = number(name)
        copy = pltpu.make_async_remote_copy(
            src_ref=src, dst_ref=dst, send_sem=ss.at[i], recv_sem=rs.at[i],
            device_id=target, device_id_type=MESH,
        )
        copy.start()
        started.append(copy)

    def got(name, dst):
        i = number(name)
        pltpu.make_async_remote_copy(
            src_ref=dst, dst_ref=dst, send_sem=rs.at[i], recv_sem=rs.at[i],
            device_id=sibling, device_id_type=MESH,
        ).wait_recv()

    def block(where, side, h):
        return gath.at[where, side, pl.ds(h * half, half)]

    def cross(where, h):
        send(("cross", where, h), block(where, core, h), block(where, core, h), sibling)

    def crossed(where, h):
        got(("cross", where, h), block(where, twin, h))
        split(where, twin, h)

    def split(where, side, h):
        value = gath[where, side, h * half:(h + 1) * half]
        hi = value.astype(jnp.bfloat16)
        parts[where, 0, side, h * half:(h + 1) * half] = hi
        parts[where, 1, side, h * half:(h + 1) * half] = (
            value - hi.astype(jnp.float32)
        ).astype(jnp.bfloat16)

    for h in (0, 1):
        send(("z", 0, h), block(0, core, h), block(4, core, h), right)
        send(("x", 0, h), block(0, core, h), block(1, core, h), across)
        send(("y", 0, 1 - h), block(0, core, 1 - h), block(2, core, 1 - h), along)
    for h in (0, 1):
        cross(0, h)
    for h in (0, 1):
        split(0, core, h)
    for copy in loads[1:]:
        copy.wait()

    me = x * ny + y

    def look(tile, state):
        i_tile, j_tile = state[0], state[1]
        a, i = lax.div(i_tile, half_tiles), lax.rem(i_tile, half_tiles)
        b, j = lax.div(j_tile, half_tiles), lax.rem(j_tile, half_tiles)
        i_chip, j_chip = jnp.bitwise_xor(i, chip), jnp.bitwise_xor(j, chip)
        i_near, j_near = jnp.where(a == x, 0, half_tiles), jnp.where(b == x, 0, half_tiles)
        same = jnp.where(i_tile == j_tile, 256, 0)
        last = jnp.where((i_near + i_chip == 7) | (j_near + j_chip == 7), 64, 0)
        near = i_near + i_chip + 8 * (j_near + j_chip) + same + last
        far_code = 128 + jnp.where(
            a == x, j_chip + 8 * lax.div(i, 2), i_chip + 8 * lax.div(j, 2)
        )
        code = jnp.where(a - b == nx // 2, far_code, near)
        key = jnp.where(owner_ref[tile] == me, slot_ref[tile], slots)
        found = tuple(jnp.where(key == s, code, state[2 + s]) for s in range(slots))
        wrap = j_tile == i_tile
        return (
            jnp.where(wrap, i_tile + 1, i_tile), jnp.where(wrap, 0, j_tile + 1)
        ) + found

    codes = lax.fori_loop(
        0, owner_ref.shape[0], look, (jnp.int32(0),) * 2 + (jnp.int32(-1),) * slots
    )[2:]
    seen, picks, ranks = jnp.int32(0), [jnp.int32(0)] * 2, []
    kinds = []
    for s in range(slots):
        code = codes[s]
        kind = jnp.where(code < 0, 3, lax.rem(lax.div(code, 64), 4))
        kinds.append(kind)
        todo[s] = jnp.where(kind == 0, code, 0)
        is_last = jnp.where(kind == 1, 1, 0)
        ranks.append(seen)
        picks = [
            jnp.where(is_last * jnp.where(seen == k, 1, 0) == 1, code, picks[k])
            for k in range(2)
        ]
        seen = seen + is_last
    for k in range(2):
        todo[slots + k] = picks[k]

    one = functools.partial(
        lax.dot_general,
        dimension_numbers=(((1,), (1,)), ((), ())),
        preferred_element_type=jnp.float32,
    )

    def product(code):
        first, second = lax.rem(code, 8), lax.rem(lax.div(code, 8), 8)
        both = one(
            parts[first].reshape(4 * rows, width), parts[second, 0].reshape(2 * rows, width)
        )
        return both[:2 * rows] + (
            both[2 * rows:]
            + one(
                parts[first, 0].reshape(2 * rows, width),
                parts[second, 1].reshape(2 * rows, width),
            )
        )

    got(("x", 0, 0), block(1, core, 0))
    send(("y", 3, 0), block(1, core, 0), block(3, core, 0), along)
    got(("y", 0, 1), block(2, core, 1))
    send(("x", 3, 1), block(2, core, 1), block(3, core, 1), across)
    cross(1, 0)
    cross(2, 1)
    got(("z", 0, 0), block(4, core, 0))
    send(("z", 1, 0), block(4, core, 0), zfar.at[pl.ds(0, half)], right)
    cross(4, 0)
    split(1, core, 0)
    split(2, core, 1)
    split(4, core, 0)
    crossed(0, 0)
    crossed(0, 1)
    crossed(1, 0)
    crossed(2, 1)
    crossed(4, 0)
    got(("x", 0, 1), block(1, core, 1))
    cross(1, 1)
    got(("y", 0, 0), block(2, core, 0))
    cross(2, 0)
    got(("z", 0, 1), block(4, core, 1))
    send(("z", 1, 1), block(4, core, 1), zfar.at[pl.ds(half, half)], right)
    for h in (0, 1):
        send(("x", 4, h), block(4, core, h), block(5, core, h), across)
        send(("y", 4, h), block(4, core, h), block(6, core, h), along)
    cross(4, 1)
    split(1, core, 1)
    split(2, core, 0)
    split(4, core, 1)
    crossed(1, 1)
    crossed(2, 0)
    crossed(4, 1)
    got(("y", 3, 0), block(3, core, 0))
    cross(3, 0)
    got(("x", 3, 1), block(3, core, 1))
    cross(3, 1)
    for h in (0, 1):
        send(("z", 3, h), block(3, core, h), block(7, core, h), right)
    split(3, core, 0)
    split(3, core, 1)
    crossed(3, 0)
    crossed(3, 1)

    def split_far(h):
        part = slice(h * half, (h + 1) * half)
        value = zfar[part]
        hi = value.astype(jnp.bfloat16)
        far_parts[0, part] = hi
        far_parts[1, part] = (value - hi.astype(jnp.float32)).astype(jnp.bfloat16)

    flag = jnp.where(x >= nx // 2, 1, 0)
    got(("z", 1, 0), zfar.at[pl.ds(0, half)])
    split_far(0)
    got(("z", 1, 1), zfar.at[pl.ds(half, half)])
    split_far(1)
    for t in (0, 1):
        col = flag + 2 * lax.rem(t + lax.div(chip, 2), 2)
        both = one(
            far_parts[...].reshape(2 * rows, width), parts[col, 0].reshape(2 * rows, width)
        )
        full = both[:rows] + (
            both[rows:] + one(far_parts[0], parts[col, 1].reshape(2 * rows, width))
        )
        for k in (0, 1):
            piece_k = full[:, k * rows:(k + 1) * rows]
            far[0, core, t, k] = jnp.where(flag == 0, piece_k, piece_k.T)

    def far_at(where, side, t):
        return far.at[where, side, t]

    def far_cross(where, t):
        send(("fcross", where, t), far_at(where, core, t), far_at(where, core, t), sibling)

    for t in (0, 1):
        send(("fx", 0, t), far_at(0, core, t), far_at(1, core, t), across)
        send(("fy", 0, 1 - t), far_at(0, core, 1 - t), far_at(2, core, 1 - t), along)
    for t in (0, 1):
        far_cross(0, t)

    for h in (0, 1):
        got(("x", 4, h), block(5, core, h))
        cross(5, h)
        got(("y", 4, h), block(6, core, h))
        cross(6, h)
        split(5, core, h)
        split(6, core, h)
        crossed(5, h)
        crossed(6, h)

    above = jnp.where(
        lax.broadcasted_iota(jnp.int32, (2 * rows, 2 * rows), 0)
        < lax.broadcasted_iota(jnp.int32, (2 * rows, 2 * rows), 1), 1, 0,
    )

    def local(s, carry):
        code = todo[s]
        masked = jnp.where(code >= 256, 1, 0)
        out_ref[s] = jnp.where(above * masked == 1, 0.0, product(code))
        return carry

    middle = slots // 2
    lax.fori_loop(0, middle, local, 0)
    got(("fx", 0, 0), far_at(1, core, 0))
    send(("fy", 3, 0), far_at(1, core, 0), far_at(3, core, 0), along)
    got(("fy", 0, 1), far_at(2, core, 1))
    send(("fx", 3, 1), far_at(2, core, 1), far_at(3, core, 1), across)
    far_cross(1, 0)
    far_cross(2, 1)
    got(("z", 3, 0), block(7, core, 0))
    cross(7, 0)
    lax.fori_loop(middle, slots, local, 0)
    split(7, core, 0)
    crossed(7, 0)
    got(("fx", 0, 1), far_at(1, core, 1))
    far_cross(1, 1)
    got(("fy", 0, 0), far_at(2, core, 0))
    far_cross(2, 0)
    got(("z", 3, 1), block(7, core, 1))
    cross(7, 1)
    split(7, core, 1)
    crossed(7, 1)

    def behind(k, carry):
        extra[k] = product(todo[slots + k])
        return carry

    lax.fori_loop(0, 2, behind, 0)
    got(("fy", 3, 0), far_at(3, core, 0))
    far_cross(3, 0)
    got(("fx", 3, 1), far_at(3, core, 1))
    far_cross(3, 1)
    for where in range(4):
        for t in (0, 1):
            got(("fcross", where, t), far_at(where, twin, t))

    for s in range(slots):
        kind, code = kinds[s], jnp.maximum(codes[s], 0)
        where = lax.rem(code, 4)
        t = lax.rem(lax.div(code, 8), 2)
        rank = jnp.minimum(ranks[s], 1)
        for i in (0, 1):
            for j in (0, 1):
                side, k = jnp.where(flag == 0, i, j), jnp.where(flag == 0, j, i)
                at = (s, slice(i * rows, (i + 1) * rows), slice(j * rows, (j + 1) * rows))
                value = jnp.where(kind == 1, extra[rank, at[1], at[2]], out_ref[at])
                value = jnp.where(kind == 2, far[where, side, t, k], value)
                out_ref[at] = jnp.where(kind == 3, 0.0, value)
    for copy in started:
        copy.wait_send()


def plane_call(dims, matrix_rows, tile_owner, tile_slot):
    nx, ny, half_tiles, slots = dims
    rows, width = matrix_rows.shape
    f32, bf16 = jnp.float32, jnp.bfloat16
    dma = pltpu.SemaphoreType.DMA
    hbm = pl.BlockSpec(memory_space=pltpu.HBM)
    return pl.pallas_call(
        functools.partial(plane_kernel, dims),
        out_shape=jax.ShapeDtypeStruct((slots, 2 * rows, 2 * rows), f32),
        in_specs=[hbm, hbm, hbm],
        out_specs=pl.BlockSpec(memory_space=pltpu.VMEM),
        scratch_shapes=[
            pltpu.VMEM((8, 2, rows, width), f32),
            pltpu.VMEM((rows, width), f32),
            pltpu.VMEM((8, 2, 2, rows, width), bf16),
            pltpu.VMEM((2, rows, width), bf16),
            pltpu.VMEM((4, 2, 2, 2, rows, rows), f32),
            pltpu.VMEM((2, 2 * rows, 2 * rows), f32),
            pltpu.SMEM(tile_owner.shape, jnp.int32),
            pltpu.SMEM(tile_slot.shape, jnp.int32),
            pltpu.SMEM((slots + 2,), jnp.int32),
            dma((3,)), dma((64,)), dma((64,)),
        ],
        compiler_params=pltpu.CompilerParams(
            collective_id=0, has_side_effects=True,
            vmem_limit_bytes=44 * 1024 * 1024,
        ),
    )(matrix_rows, tile_owner, tile_slot)


def copy_out(in_ref, out_ref, sem):
    copy = pltpu.make_async_copy(in_ref, out_ref, sem)
    copy.start()
    copy.wait()


def ring_call(mesh_shape, matrix_rows, tile_owner, tile_slot):
    nx, ny = mesh_shape
    rows, width = matrix_rows.shape
    half_tiles, half_x = ny // 2, nx // 2
    capacity = nx // 4 + 1
    slots = -(-tile_owner.shape[0] // (nx * ny))
    _, piece_count = piece_lists(half_tiles, half_x)
    reach = max(ny // 4, 1)
    f32, bf16 = jnp.float32, jnp.bfloat16
    dma = pltpu.SemaphoreType.DMA
    return pl.pallas_call(
        functools.partial(kernel, (nx, ny, half_tiles, half_x, capacity, slots)),
        out_shape=jax.ShapeDtypeStruct((slots, 2 * rows, 2 * rows), f32),
        in_specs=[
            pl.BlockSpec(memory_space=pltpu.VMEM),
            pl.BlockSpec(memory_space=pltpu.SMEM),
            pl.BlockSpec(memory_space=pltpu.SMEM),
        ],
        out_specs=pl.BlockSpec(memory_space=pltpu.VMEM),
        scratch_shapes=[
            pltpu.VMEM((ny, rows, width), f32),
            pltpu.VMEM((half_x, rows, width), f32),
            pltpu.VMEM((ny, rows, width), bf16),
            pltpu.VMEM((ny, rows, width), bf16),
            pltpu.VMEM((half_x + 1, 2, rows, width), bf16),
            pltpu.VMEM((2, piece_count, 2, rows // 2, rows), f32),
            pltpu.VMEM((2, ny, 2 * capacity, rows // 2, rows), f32),
            pltpu.VMEM((2, ny * 2 * capacity, rows // 2, rows), f32),
            pltpu.SMEM((piece_count,), jnp.int32),
            dma((reach, 2)), dma((reach, 2)), dma((reach, 2)), dma((reach, 2)),
            dma((2 * reach + 1, 2)), dma((2 * reach + 1, 2)),
            dma((half_x, 2)), dma((half_x, 2)),
            dma((2, ny)), dma((2, ny)),
        ],
        compiler_params=pltpu.CompilerParams(
            collective_id=0, has_side_effects=True, vmem_limit_bytes=44 * 1024 * 1024
        ),
    )(matrix_rows, tile_owner, tile_slot)


def per_device(mesh_shape, matrix_rows, tile_owner, tile_slot):
    nx, ny = mesh_shape
    if ny // 2 == 4 and nx == 4:
        slots = -(-tile_owner.shape[0] // (nx * ny))
        packed = plane_call((nx, ny, ny // 2, slots), matrix_rows, tile_owner, tile_slot)
    else:
        packed = ring_call(mesh_shape, matrix_rows, tile_owner, tile_slot)
    return pl.pallas_call(
        copy_out,
        out_shape=jax.ShapeDtypeStruct(packed.shape, packed.dtype),
        in_specs=[pl.BlockSpec(memory_space=pltpu.VMEM)],
        out_specs=pl.BlockSpec(memory_space=pl.ANY),
        scratch_shapes=[pltpu.SemaphoreType.DMA(())],
        compiler_params=pltpu.CompilerParams(vmem_limit_bytes=4 * 1024 * 1024),
    )(packed)


def solution(mesh):
    placed = (P(("gx", "gy"), None), P(), P())
    return jax.shard_map(
        functools.partial(per_device, (mesh.shape["gx"], mesh.shape["gy"])),
        mesh=mesh,
        in_specs=placed,
        out_specs=P(("gx", "gy"), None, None),
        check_vma=False,
    )
```

```python
import functools

import jax
import jax.numpy as jnp
from jax import lax
from jax.experimental import pallas as pl
from jax.experimental.pallas import tpu as pltpu
from jax.sharding import PartitionSpec as P

MESH = pl.DeviceIdType.MESH


def chip_position(chip, chips):
    row, col = lax.div(chip, 2), lax.rem(chip, 2)
    return col * (1 + row) + (1 - col) * lax.rem(chips - row, chips)


def chip_at(position, chips):
    behind = lax.rem(position + chips - 1, chips)
    far = lax.div(behind, chips // 2)
    return (1 - far) * (2 * behind + 1) + far * 2 * (chips - 1 - behind)


def piece_lists(half_tiles, half_x):
    lists, start = [], 0
    for step in range(half_x + 1):
        if step == 0:
            count = half_tiles // 2 + 1
        elif step < half_x:
            count = half_tiles
        else:
            count = half_tiles // 2
        lists.append((step, start, count))
        start += count
    return lists, start


def piece(x, r, step, i, nx, half_tiles, half_x):
    source = lax.rem(x - step + nx, nx)
    if step == 0:
        col = lax.rem(r - i + half_tiles, half_tiles)
        valid = jnp.logical_or(i < half_tiles // 2, r < half_tiles // 2)
        rowwise = col <= r
    elif step < half_x:
        col = i
        valid = i >= 0
        rowwise = source > x
    else:
        flag = jnp.where(x >= half_x, 1, 0)
        col = 2 * i + lax.rem(r + flag, 2)
        valid = i >= 0
        rowwise = source > x
    other, mine = source * half_tiles + r, x * half_tiles + col
    row_tile = jnp.where(rowwise, other, mine)
    col_tile = jnp.where(rowwise, mine, other)
    tile = jnp.where(valid, row_tile * (row_tile + 1) // 2 + col_tile, 0)
    return col, valid, rowwise, tile


def kernel(
    dims, rows_ref, owner_ref, slot_ref, out_ref,
    gath, zbuf, chi, clo, zsplit, pieces, outgoing, incoming, targets,
    gs_r, gr_r, gs_l, gr_l, ss, sr, zs, zr, xs, xr,
):
    nx, ny, half_tiles, half_x, capacity, slots = dims
    rows = rows_ref.shape[0]
    half = rows // 2
    chips = ny // 2
    reach = chips // 2
    x = lax.axis_index("gx")
    y = lax.axis_index("gy")
    core = lax.rem(y, 2)
    chip = lax.div(y, 2)
    right_x, left_x = lax.rem(x + 1, nx), lax.rem(x + nx - 1, nx)
    sibling = y + 1 - 2 * core
    place = chip_position(chip, chips)

    def at(position):
        return 2 * chip_at(lax.rem(position + chips, chips), chips) + core

    next_y, prev_y = at(place + 1), at(place - 1)
    lists, piece_count = piece_lists(half_tiles, half_x)

    barrier = pltpu.get_barrier_semaphore()
    for other in (right_x, left_x):
        pl.semaphore_signal(barrier, inc=1, device_id=(other, y), device_id_type=MESH)
    for offset in range(1, ny):
        pl.semaphore_signal(
            barrier, inc=1, device_id=(x, lax.rem(y + offset, ny)), device_id_type=MESH
        )
    pl.semaphore_wait(barrier, ny + 1)

    started = []

    def send(src, dst, send_sem, recv_sem, target):
        copy = pltpu.make_async_remote_copy(
            src_ref=src, dst_ref=dst, send_sem=send_sem, recv_sem=recv_sem,
            device_id=target, device_id_type=MESH,
        )
        copy.start()
        started.append(copy)

    def part(h):
        return pl.ds(h * half, half)

    def zcopy(step, h):
        src = rows_ref.at[part(h)] if step == 1 else zbuf.at[step - 2, part(h)]
        send(src, zbuf.at[step - 1, part(h)], zs.at[step - 1, h], zr.at[step - 1, h], (right_x, y))

    def block(owner, h):
        return gath.at[owner, part(h)]

    def ring(direction, distance, h):
        owner = at(place - direction * (distance - 1))
        src = rows_ref.at[part(h)] if distance == 1 else block(owner, h)
        s, r = (gs_r, gr_r) if direction == 1 else (gs_l, gr_l)
        target = next_y if direction == 1 else prev_y
        send(src, block(owner, h), s.at[distance - 1, h], r.at[distance - 1, h], (x, target))

    def cross(number, owner, h):
        src = rows_ref.at[part(h)] if number == 0 else block(owner, h)
        send(src, block(owner, h), ss.at[number, h], sr.at[number, h], (x, sibling))

    def halves_of(direction, distance):
        if distance < reach:
            return (0, 1) if direction == 1 else (1, 0)
        return (0,) if direction == 1 else (1,)

    def split(value, hi_ref, lo_ref, index):
        hi = value.astype(jnp.bfloat16)
        hi_ref[index] = hi
        lo_ref[index] = (value - hi.astype(jnp.float32)).astype(jnp.bfloat16)

    zcopy(1, 0)
    ring(1, 1, 0)
    if reach > 1:
        ring(-1, 1, 1)
        zcopy(1, 1)
        ring(1, 1, 1)
        ring(-1, 1, 0)
    else:
        ring(-1, 1, 1)
        zcopy(1, 1)
    cross(0, y, 0)
    cross(0, y, 1)

    for step, first, count in lists:
        def fill(i, carry, step=step, first=first):
            _, valid, _, tile = piece(x, chip, step, i, nx, half_tiles, half_x)
            targets[first + i] = jnp.where(valid, lax.rem(owner_ref[tile], ny), ny)
            return carry
        lax.fori_loop(0, count, fill, 0)

    me = x * ny + y

    def class_loop(r, carry):
        state = (jnp.int32(0),) + carry
        for step, first, count in lists:
            def look(i, state, step=step):
                seen, found = state[0], state[1:]
                _, valid, rowwise, tile = piece(x, r, step, i, nx, half_tiles, half_x)
                mine = jnp.where(valid, jnp.where(owner_ref[tile] == me, 1, 0), 0)
                slot = slot_ref[tile]
                code = 2 * (r * capacity + jnp.minimum(seen, capacity - 1))
                code = code + jnp.where(rowwise, 1, 0)
                key = jnp.where(mine == 1, slot, slots)
                found = tuple(jnp.where(key == s, code, found[s]) for s in range(slots))
                return (seen + mine,) + found
            state = lax.fori_loop(0, count, look, state)
        return state[1:]

    found = lax.fori_loop(0, half_tiles, class_loop, (jnp.int32(-1),) * slots)

    chosen = []
    for offset in range(ny):
        dest = lax.rem(y + offset, ny)

        def pick(p, state, dest=dest):
            hit = jnp.where(targets[p] == dest, 1, 0)
            seen = state[0]
            key = jnp.where(hit == 1, seen, capacity)
            picks = tuple(jnp.where(key == k, p, state[1 + k]) for k in range(capacity))
            return (seen + hit,) + picks

        chosen.append(lax.fori_loop(0, piece_count, pick, (jnp.int32(0),) * (capacity + 1))[1:])

    def wait_recv(dst, sem):
        pltpu.make_async_remote_copy(
            src_ref=dst, dst_ref=dst, send_sem=sem, recv_sem=sem,
            device_id=(x, sibling), device_id_type=MESH,
        ).wait_recv()

    def split_other(step, h):
        ref = rows_ref.at[part(h)] if step == 0 else zbuf.at[step - 1, part(h)]
        value = ref[...]
        hi = value.astype(jnp.bfloat16)
        zsplit[step, h, :half] = hi
        zsplit[step, h, half:] = (value - hi.astype(jnp.float32)).astype(jnp.bfloat16)

    def take_other(step, h):
        wait_recv(zbuf.at[step - 1, part(h)], zr.at[step - 1, h])
        if step < half_x:
            zcopy(step + 1, h)

    split_other(0, 0)
    split_other(0, 1)
    split(rows_ref[...], chi, clo, y)

    def take_cross(number, owner, halves):
        for h in halves:
            wait_recv(block(owner, h), sr.at[number, h])

    one = functools.partial(
        lax.dot_general,
        dimension_numbers=(((1,), (1,)), ((), ())),
        preferred_element_type=jnp.float32,
    )
    width = rows_ref.shape[1]
    row_inside = core * rows + lax.broadcasted_iota(jnp.int32, (half, 2 * rows), 0)
    col_inside = lax.broadcasted_iota(jnp.int32, (half, 2 * rows), 1)

    def one_piece_of(h):
        above = jnp.where(row_inside + h * half < col_inside, 1, 0)

        def one_piece(i, step, first, col):
            b_hi = chi[pl.ds(2 * col, 2)].reshape(2 * rows, width)
            b_lo = clo[pl.ds(2 * col, 2)].reshape(2 * rows, width)
            both = one(zsplit[step, h], b_hi)
            full = both[:half] + (both[half:] + one(zsplit[step, h, :half], b_lo))
            if step == 0:
                full = jnp.where(above * jnp.where(i == 0, 1, 0) == 1, 0.0, full)
            pieces[h, first + i, 0] = full[:, :rows]
            pieces[h, first + i, 1] = full[:, rows:]

        return one_piece

    farthest = chip_at(lax.rem(place + reach, chips), chips)
    soon = min(reach, half_x) if reach > 1 else 0

    def multiply(h, mode):
        one_piece = one_piece_of(h)
        for step, first, count in lists:
            if mode == "early" and step >= soon:
                continue

            def make(i, carry, step=step, first=first):
                col, _, _, _ = piece(x, chip, step, i, nx, half_tiles, half_x)
                if mode == "all" or step >= soon:
                    one_piece(i, step, first, col)
                else:
                    wanted = (col != farthest) if mode == "early" else (col == farthest)
                    pl.when(wanted)(lambda: one_piece(i, step, first, col))
                return carry
            lax.fori_loop(0, count, make, 0)

    pending = [(0, sibling, (0, 1))]
    for distance in range(1, reach + 1):
        if distance == reach:
            for number, owner, halves in pending[1:]:
                take_cross(number, owner, halves)
                split(gath[owner], chi, clo, owner)
            multiply(0, "early")
        if distance <= half_x:
            for h in (0, 1):
                if (distance, h) != (half_x, 1):
                    take_other(distance, h)
                if h in halves_of(1, distance):
                    owner = at(place - distance)
                    wait_recv(block(owner, h), gr_r.at[distance - 1, h])
                    if distance < reach and h in halves_of(1, distance + 1):
                        ring(1, distance + 1, h)
                    cross(2 * distance - 1, owner, h)
                g = 1 - h
                if g in halves_of(-1, distance):
                    owner = at(place + distance)
                    wait_recv(block(owner, g), gr_l.at[distance - 1, g])
                    if distance < reach and g in halves_of(-1, distance + 1):
                        ring(-1, distance + 1, g)
                    cross(2 * distance, owner, g)
            split_other(distance, 0)
            if distance < half_x:
                split_other(distance, 1)
        behind, ahead = at(place - distance), at(place + distance)
        pending.append((2 * distance - 1, behind + 1 - 2 * core, halves_of(1, distance)))
        pending.append((2 * distance, ahead + 1 - 2 * core, halves_of(-1, distance)))
        split(gath[behind], chi, clo, behind)
        if distance < reach:
            split(gath[ahead], chi, clo, ahead)
        for number, owner, halves in pending[: (1 if distance == 1 else 0)]:
            take_cross(number, owner, halves)
            split(gath[owner], chi, clo, owner)
    for number, owner, halves in pending[-2:]:
        take_cross(number, owner, halves)
    split(gath[pending[-1][1]], chi, clo, pending[-1][1])
    for step in range(reach + 1, half_x + 1):
        for h in (0, 1):
            if (step, h) != (half_x, 1):
                take_other(step, h)
                split_other(step, h)

    def arrival(offset):
        return pl.ds(offset * capacity * 2, capacity * 2)

    def exchange(h, offset):
        send(
            outgoing.at[h, offset], incoming.at[h, arrival(offset)],
            xs.at[h, offset], xr.at[h, offset], (x, lax.rem(y + offset, ny)),
        )

    for h in (0, 1):
        if h == 1:
            take_other(half_x, 1)
            split_other(half_x, 1)
        multiply(h, "all" if h == 1 else "late")
        for offset in range(1, ny):
            for k in range(capacity):
                outgoing[h, offset, 2 * k:2 * k + 2] = pieces[h, chosen[offset][k]]
            if offset > 1:
                exchange(h, offset - 1)
        for k in range(capacity):
            incoming[h, 2 * k:2 * k + 2] = pieces[h, chosen[0][k]]
        exchange(h, ny - 1)
    for h in (0, 1):
        for offset in range(1, ny):
            wait_recv(incoming.at[h, arrival(offset)], xr.at[h, offset])

    for s in range(slots):
        code = found[s]
        there = code >= 0
        safe = jnp.maximum(code, 0)
        rowwise = lax.rem(safe, 2) == 1
        rank = lax.rem(safe // 2, capacity)
        first_source = 2 * (safe // (2 * capacity))
        bases = [
            (lax.rem(y - first_source - h + ny, ny) * capacity + rank) * 2 for h in (0, 1)
        ]
        for i in (0, 1):
            for j in (0, 1):
                place_of = jnp.where(rowwise, bases[i] + j, bases[j] + i)
                value = jnp.concatenate([incoming[0, place_of], incoming[1, place_of]], axis=0)
                value = jnp.where(rowwise, value, value.T)
                out_ref[s, i * rows:(i + 1) * rows, j * rows:(j + 1) * rows] = jnp.where(
                    there, value, 0.0
                )
    for copy in started:
        copy.wait_send()


def plane_kernel(
    dims, rows_hbm, owner_hbm, slot_hbm, out_ref,
    gath, zfar, parts, far_parts, far, extra, owner_ref, slot_ref, todo,
    ins, ss, rs,
):
    nx, ny, half_tiles, slots = dims
    rows, width = zfar.shape
    half = rows // 2
    x = lax.axis_index("gx")
    y = lax.axis_index("gy")
    core = lax.rem(y, 2)
    chip = lax.div(y, 2)
    twin = 1 - core
    right, left = (lax.rem(x + 1, nx), y), (lax.rem(x + nx - 1, nx), y)
    sibling = (x, y + 1 - 2 * core)
    across = (x, y + 2 - 4 * lax.rem(chip, 2))
    along = (x, lax.rem(y + 4, ny))

    barrier = pltpu.get_barrier_semaphore()
    peers = (sibling, across, along, right, left)
    for other in peers:
        pl.semaphore_signal(barrier, inc=1, device_id=other, device_id_type=MESH)
    loads = [
        pltpu.make_async_copy(rows_hbm, gath.at[0, core], ins.at[0]),
        pltpu.make_async_copy(owner_hbm, owner_ref, ins.at[1]),
        pltpu.make_async_copy(slot_hbm, slot_ref, ins.at[2]),
    ]
    for copy in loads:
        copy.start()
    pl.semaphore_wait(barrier, len(peers))
    loads[0].wait()

    started, numbers = [], {}

    def number(name):
        return numbers.setdefault(name, len(numbers))

    def send(name, src, dst, target):
        i = number(name)
        copy = pltpu.make_async_remote_copy(
            src_ref=src, dst_ref=dst, send_sem=ss.at[i], recv_sem=rs.at[i],
            device_id=target, device_id_type=MESH,
        )
        copy.start()
        started.append(copy)

    def got(name, dst):
        i = number(name)
        pltpu.make_async_remote_copy(
            src_ref=dst, dst_ref=dst, send_sem=rs.at[i], recv_sem=rs.at[i],
            device_id=sibling, device_id_type=MESH,
        ).wait_recv()

    def block(where, side, h):
        return gath.at[where, side, pl.ds(h * half, half)]

    def cross(where, h):
        send(("cross", where, h), block(where, core, h), block(where, core, h), sibling)

    def crossed(where, h):
        got(("cross", where, h), block(where, twin, h))
        split(where, twin, h)

    def split(where, side, h):
        value = gath[where, side, h * half:(h + 1) * half]
        hi = value.astype(jnp.bfloat16)
        parts[where, 0, side, h * half:(h + 1) * half] = hi
        parts[where, 1, side, h * half:(h + 1) * half] = (
            value - hi.astype(jnp.float32)
        ).astype(jnp.bfloat16)

    for h in (0, 1):
        send(("z", 0, h), block(0, core, h), block(4, core, h), right)
        send(("x", 0, h), block(0, core, h), block(1, core, h), across)
        send(("y", 0, 1 - h), block(0, core, 1 - h), block(2, core, 1 - h), along)
    for h in (0, 1):
        cross(0, h)
    for h in (0, 1):
        split(0, core, h)
    for copy in loads[1:]:
        copy.wait()

    me = x * ny + y

    def look(tile, state):
        i_tile, j_tile = state[0], state[1]
        a, i = lax.div(i_tile, half_tiles), lax.rem(i_tile, half_tiles)
        b, j = lax.div(j_tile, half_tiles), lax.rem(j_tile, half_tiles)
        i_chip, j_chip = jnp.bitwise_xor(i, chip), jnp.bitwise_xor(j, chip)
        i_near, j_near = jnp.where(a == x, 0, half_tiles), jnp.where(b == x, 0, half_tiles)
        same = jnp.where(i_tile == j_tile, 256, 0)
        last = jnp.where((i_near + i_chip == 7) | (j_near + j_chip == 7), 64, 0)
        near = i_near + i_chip + 8 * (j_near + j_chip) + same + last
        far_code = 128 + jnp.where(
            a == x, j_chip + 8 * lax.div(i, 2), i_chip + 8 * lax.div(j, 2)
        )
        code = jnp.where(a - b == nx // 2, far_code, near)
        key = jnp.where(owner_ref[tile] == me, slot_ref[tile], slots)
        found = tuple(jnp.where(key == s, code, state[2 + s]) for s in range(slots))
        wrap = j_tile == i_tile
        return (
            jnp.where(wrap, i_tile + 1, i_tile), jnp.where(wrap, 0, j_tile + 1)
        ) + found

    codes = lax.fori_loop(
        0, owner_ref.shape[0], look, (jnp.int32(0),) * 2 + (jnp.int32(-1),) * slots
    )[2:]
    seen, picks, ranks = jnp.int32(0), [jnp.int32(0)] * 2, []
    kinds = []
    for s in range(slots):
        code = codes[s]
        kind = jnp.where(code < 0, 3, lax.rem(lax.div(code, 64), 4))
        kinds.append(kind)
        todo[s] = jnp.where(kind == 0, code, 0)
        is_last = jnp.where(kind == 1, 1, 0)
        ranks.append(seen)
        picks = [
            jnp.where(is_last * jnp.where(seen == k, 1, 0) == 1, code, picks[k])
            for k in range(2)
        ]
        seen = seen + is_last
    for k in range(2):
        todo[slots + k] = picks[k]

    one = functools.partial(
        lax.dot_general,
        dimension_numbers=(((1,), (1,)), ((), ())),
        preferred_element_type=jnp.float32,
    )

    def product(code):
        first, second = lax.rem(code, 8), lax.rem(lax.div(code, 8), 8)
        both = one(
            parts[first].reshape(4 * rows, width), parts[second, 0].reshape(2 * rows, width)
        )
        return both[:2 * rows] + (
            both[2 * rows:]
            + one(
                parts[first, 0].reshape(2 * rows, width),
                parts[second, 1].reshape(2 * rows, width),
            )
        )

    got(("x", 0, 0), block(1, core, 0))
    send(("y", 3, 0), block(1, core, 0), block(3, core, 0), along)
    got(("y", 0, 1), block(2, core, 1))
    send(("x", 3, 1), block(2, core, 1), block(3, core, 1), across)
    cross(1, 0)
    cross(2, 1)
    got(("z", 0, 0), block(4, core, 0))
    send(("z", 1, 0), block(4, core, 0), zfar.at[pl.ds(0, half)], right)
    cross(4, 0)
    split(1, core, 0)
    split(2, core, 1)
    split(4, core, 0)
    crossed(0, 0)
    crossed(0, 1)
    crossed(1, 0)
    crossed(2, 1)
    crossed(4, 0)
    got(("x", 0, 1), block(1, core, 1))
    cross(1, 1)
    got(("y", 0, 0), block(2, core, 0))
    cross(2, 0)
    got(("z", 0, 1), block(4, core, 1))
    send(("z", 1, 1), block(4, core, 1), zfar.at[pl.ds(half, half)], right)
    for h in (0, 1):
        send(("x", 4, h), block(4, core, h), block(5, core, h), across)
        send(("y", 4, h), block(4, core, h), block(6, core, h), along)
    cross(4, 1)
    split(1, core, 1)
    split(2, core, 0)
    split(4, core, 1)
    crossed(1, 1)
    crossed(2, 0)
    crossed(4, 1)
    got(("y", 3, 0), block(3, core, 0))
    cross(3, 0)
    got(("x", 3, 1), block(3, core, 1))
    cross(3, 1)
    for h in (0, 1):
        send(("z", 3, h), block(3, core, h), block(7, core, h), right)
    split(3, core, 0)
    split(3, core, 1)
    crossed(3, 0)
    crossed(3, 1)

    def split_far(h):
        part = slice(h * half, (h + 1) * half)
        value = zfar[part]
        hi = value.astype(jnp.bfloat16)
        far_parts[0, part] = hi
        far_parts[1, part] = (value - hi.astype(jnp.float32)).astype(jnp.bfloat16)

    flag = jnp.where(x >= nx // 2, 1, 0)
    got(("z", 1, 0), zfar.at[pl.ds(0, half)])
    split_far(0)
    got(("z", 1, 1), zfar.at[pl.ds(half, half)])
    split_far(1)
    for t in (0, 1):
        col = flag + 2 * lax.rem(t + lax.div(chip, 2), 2)
        both = one(
            far_parts[...].reshape(2 * rows, width), parts[col, 0].reshape(2 * rows, width)
        )
        full = both[:rows] + (
            both[rows:] + one(far_parts[0], parts[col, 1].reshape(2 * rows, width))
        )
        for k in (0, 1):
            piece_k = full[:, k * rows:(k + 1) * rows]
            far[0, core, t, k] = jnp.where(flag == 0, piece_k, piece_k.T)

    def far_at(where, side, t):
        return far.at[where, side, t]

    def far_cross(where, t):
        send(("fcross", where, t), far_at(where, core, t), far_at(where, core, t), sibling)

    for t in (0, 1):
        send(("fx", 0, t), far_at(0, core, t), far_at(1, core, t), across)
        send(("fy", 0, 1 - t), far_at(0, core, 1 - t), far_at(2, core, 1 - t), along)
    for t in (0, 1):
        far_cross(0, t)

    for h in (0, 1):
        got(("x", 4, h), block(5, core, h))
        cross(5, h)
        got(("y", 4, h), block(6, core, h))
        cross(6, h)
        split(5, core, h)
        split(6, core, h)
        crossed(5, h)
        crossed(6, h)

    above = jnp.where(
        lax.broadcasted_iota(jnp.int32, (2 * rows, 2 * rows), 0)
        < lax.broadcasted_iota(jnp.int32, (2 * rows, 2 * rows), 1), 1, 0,
    )

    def local(s, carry):
        code = todo[s]
        masked = jnp.where(code >= 256, 1, 0)
        out_ref[s] = jnp.where(above * masked == 1, 0.0, product(code))
        return carry

    middle = slots // 2
    lax.fori_loop(0, middle, local, 0)
    got(("fx", 0, 0), far_at(1, core, 0))
    send(("fy", 3, 0), far_at(1, core, 0), far_at(3, core, 0), along)
    got(("fy", 0, 1), far_at(2, core, 1))
    send(("fx", 3, 1), far_at(2, core, 1), far_at(3, core, 1), across)
    far_cross(1, 0)
    far_cross(2, 1)
    got(("z", 3, 0), block(7, core, 0))
    cross(7, 0)
    lax.fori_loop(middle, slots, local, 0)
    split(7, core, 0)
    crossed(7, 0)
    got(("fx", 0, 1), far_at(1, core, 1))
    far_cross(1, 1)
    got(("fy", 0, 0), far_at(2, core, 0))
    far_cross(2, 0)
    got(("z", 3, 1), block(7, core, 1))
    cross(7, 1)
    split(7, core, 1)
    crossed(7, 1)

    def behind(k, carry):
        extra[k] = product(todo[slots + k])
        return carry

    lax.fori_loop(0, 2, behind, 0)
    got(("fy", 3, 0), far_at(3, core, 0))
    far_cross(3, 0)
    got(("fx", 3, 1), far_at(3, core, 1))
    far_cross(3, 1)
    for where in range(4):
        for t in (0, 1):
            got(("fcross", where, t), far_at(where, twin, t))

    for s in range(slots):
        kind, code = kinds[s], jnp.maximum(codes[s], 0)
        where = lax.rem(code, 4)
        t = lax.rem(lax.div(code, 8), 2)
        rank = jnp.minimum(ranks[s], 1)
        for i in (0, 1):
            for j in (0, 1):
                side, k = jnp.where(flag == 0, i, j), jnp.where(flag == 0, j, i)
                at = (s, slice(i * rows, (i + 1) * rows), slice(j * rows, (j + 1) * rows))
                value = jnp.where(kind == 1, extra[rank, at[1], at[2]], out_ref[at])
                value = jnp.where(kind == 2, far[where, side, t, k], value)
                out_ref[at] = jnp.where(kind == 3, 0.0, value)
    for copy in started:
        copy.wait_send()


def plane_call(dims, *arrays):
    nx, ny, half_tiles, slots = dims
    matrix_rows, tile_owner, tile_slot = arrays
    rows, width = matrix_rows.shape
    f32, bf16 = jnp.float32, jnp.bfloat16
    dma = pltpu.SemaphoreType.DMA
    hbm = pl.BlockSpec(memory_space=pltpu.HBM)
    return pl.pallas_call(
        functools.partial(plane_kernel, dims),
        out_shape=jax.ShapeDtypeStruct((slots, 2 * rows, 2 * rows), f32),
        in_specs=[hbm, hbm, hbm],
        out_specs=pl.BlockSpec(memory_space=pltpu.VMEM),
        scratch_shapes=[
            pltpu.VMEM((8, 2, rows, width), f32),
            pltpu.VMEM((rows, width), f32),
            pltpu.VMEM((8, 2, 2, rows, width), bf16),
            pltpu.VMEM((2, rows, width), bf16),
            pltpu.VMEM((4, 2, 2, 2, rows, rows), f32),
            pltpu.VMEM((2, 2 * rows, 2 * rows), f32),
            pltpu.SMEM(tile_owner.shape, jnp.int32),
            pltpu.SMEM(tile_slot.shape, jnp.int32),
            pltpu.SMEM((slots + 2,), jnp.int32),
            dma((3,)), dma((64,)), dma((64,)),
        ],
        compiler_params=pltpu.CompilerParams(
            collective_id=0, has_side_effects=True,
            vmem_limit_bytes=44 * 1024 * 1024,
        ),
    )(*(pltpu.with_memory_space_constraint(a, pltpu.HBM) for a in arrays))


def copy_out(in_ref, out_ref, sem):
    copy = pltpu.make_async_copy(in_ref, out_ref, sem)
    copy.start()
    copy.wait()


def ring_call(mesh_shape, matrix_rows, tile_owner, tile_slot):
    nx, ny = mesh_shape
    rows, width = matrix_rows.shape
    half_tiles, half_x = ny // 2, nx // 2
    capacity = nx // 4 + 1
    slots = -(-tile_owner.shape[0] // (nx * ny))
    _, piece_count = piece_lists(half_tiles, half_x)
    reach = max(ny // 4, 1)
    f32, bf16 = jnp.float32, jnp.bfloat16
    dma = pltpu.SemaphoreType.DMA
    return pl.pallas_call(
        functools.partial(kernel, (nx, ny, half_tiles, half_x, capacity, slots)),
        out_shape=jax.ShapeDtypeStruct((slots, 2 * rows, 2 * rows), f32),
        in_specs=[
            pl.BlockSpec(memory_space=pltpu.VMEM),
            pl.BlockSpec(memory_space=pltpu.SMEM),
            pl.BlockSpec(memory_space=pltpu.SMEM),
        ],
        out_specs=pl.BlockSpec(memory_space=pltpu.VMEM),
        scratch_shapes=[
            pltpu.VMEM((ny, rows, width), f32),
            pltpu.VMEM((half_x, rows, width), f32),
            pltpu.VMEM((ny, rows, width), bf16),
            pltpu.VMEM((ny, rows, width), bf16),
            pltpu.VMEM((half_x + 1, 2, rows, width), bf16),
            pltpu.VMEM((2, piece_count, 2, rows // 2, rows), f32),
            pltpu.VMEM((2, ny, 2 * capacity, rows // 2, rows), f32),
            pltpu.VMEM((2, ny * 2 * capacity, rows // 2, rows), f32),
            pltpu.SMEM((piece_count,), jnp.int32),
            dma((reach, 2)), dma((reach, 2)), dma((reach, 2)), dma((reach, 2)),
            dma((2 * reach + 1, 2)), dma((2 * reach + 1, 2)),
            dma((half_x, 2)), dma((half_x, 2)),
            dma((2, ny)), dma((2, ny)),
        ],
        compiler_params=pltpu.CompilerParams(
            collective_id=0, has_side_effects=True, vmem_limit_bytes=44 * 1024 * 1024
        ),
    )(matrix_rows, tile_owner, tile_slot)


def per_device(mesh_shape, matrix_rows, tile_owner, tile_slot):
    nx, ny = mesh_shape
    if ny // 2 == 4 and nx == 4:
        slots = -(-tile_owner.shape[0] // (nx * ny))
        packed = plane_call((nx, ny, ny // 2, slots), matrix_rows, tile_owner, tile_slot)
    else:
        packed = ring_call(mesh_shape, matrix_rows, tile_owner, tile_slot)
    return pl.pallas_call(
        copy_out,
        out_shape=jax.ShapeDtypeStruct(packed.shape, packed.dtype),
        in_specs=[pl.BlockSpec(memory_space=pltpu.VMEM)],
        out_specs=pl.BlockSpec(memory_space=pl.ANY),
        scratch_shapes=[pltpu.SemaphoreType.DMA(())],
        compiler_params=pltpu.CompilerParams(vmem_limit_bytes=4 * 1024 * 1024),
    )(packed)


def solution(mesh):
    placed = (P(("gx", "gy"), None), P(), P())
    return jax.shard_map(
        functools.partial(per_device, (mesh.shape["gx"], mesh.shape["gy"])),
        mesh=mesh,
        in_specs=placed,
        out_specs=P(("gx", "gy"), None, None),
        check_vma=False,
    )
```

```python
import functools

import jax
import jax.numpy as jnp
from jax import lax
from jax.experimental import pallas as pl
from jax.experimental.pallas import tpu as pltpu
from jax.sharding import PartitionSpec as P

MESH = pl.DeviceIdType.MESH


def chip_position(chip, chips):
    row, col = lax.div(chip, 2), lax.rem(chip, 2)
    return col * (1 + row) + (1 - col) * lax.rem(chips - row, chips)


def chip_at(position, chips):
    behind = lax.rem(position + chips - 1, chips)
    far = lax.div(behind, chips // 2)
    return (1 - far) * (2 * behind + 1) + far * 2 * (chips - 1 - behind)


def piece_lists(half_tiles, half_x):
    lists, start = [], 0
    for step in range(half_x + 1):
        if step == 0:
            count = half_tiles // 2 + 1
        elif step < half_x:
            count = half_tiles
        else:
            count = half_tiles // 2
        lists.append((step, start, count))
        start += count
    return lists, start


def piece(x, r, step, i, nx, half_tiles, half_x):
    source = lax.rem(x - step + nx, nx)
    if step == 0:
        col = lax.rem(r - i + half_tiles, half_tiles)
        valid = jnp.logical_or(i < half_tiles // 2, r < half_tiles // 2)
        rowwise = col <= r
    elif step < half_x:
        col = i
        valid = i >= 0
        rowwise = source > x
    else:
        flag = jnp.where(x >= half_x, 1, 0)
        col = 2 * i + lax.rem(r + flag, 2)
        valid = i >= 0
        rowwise = source > x
    other, mine = source * half_tiles + r, x * half_tiles + col
    row_tile = jnp.where(rowwise, other, mine)
    col_tile = jnp.where(rowwise, mine, other)
    tile = jnp.where(valid, row_tile * (row_tile + 1) // 2 + col_tile, 0)
    return col, valid, rowwise, tile


def kernel(
    dims, rows_ref, owner_ref, slot_ref, out_ref,
    gath, zbuf, chi, clo, zsplit, pieces, outgoing, incoming, targets,
    gs_r, gr_r, gs_l, gr_l, ss, sr, zs, zr, xs, xr,
):
    nx, ny, half_tiles, half_x, capacity, slots = dims
    rows = rows_ref.shape[0]
    half = rows // 2
    chips = ny // 2
    reach = chips // 2
    x = lax.axis_index("gx")
    y = lax.axis_index("gy")
    core = lax.rem(y, 2)
    chip = lax.div(y, 2)
    right_x, left_x = lax.rem(x + 1, nx), lax.rem(x + nx - 1, nx)
    sibling = y + 1 - 2 * core
    place = chip_position(chip, chips)

    def at(position):
        return 2 * chip_at(lax.rem(position + chips, chips), chips) + core

    next_y, prev_y = at(place + 1), at(place - 1)
    lists, piece_count = piece_lists(half_tiles, half_x)

    barrier = pltpu.get_barrier_semaphore()
    for other in (right_x, left_x):
        pl.semaphore_signal(barrier, inc=1, device_id=(other, y), device_id_type=MESH)
    for offset in range(1, ny):
        pl.semaphore_signal(
            barrier, inc=1, device_id=(x, lax.rem(y + offset, ny)), device_id_type=MESH
        )
    pl.semaphore_wait(barrier, ny + 1)

    started = []

    def send(src, dst, send_sem, recv_sem, target):
        copy = pltpu.make_async_remote_copy(
            src_ref=src, dst_ref=dst, send_sem=send_sem, recv_sem=recv_sem,
            device_id=target, device_id_type=MESH,
        )
        copy.start()
        started.append(copy)

    def part(h):
        return pl.ds(h * half, half)

    def zcopy(step, h):
        src = rows_ref.at[part(h)] if step == 1 else zbuf.at[step - 2, part(h)]
        send(src, zbuf.at[step - 1, part(h)], zs.at[step - 1, h], zr.at[step - 1, h], (right_x, y))

    def block(owner, h):
        return gath.at[owner, part(h)]

    def ring(direction, distance, h):
        owner = at(place - direction * (distance - 1))
        src = rows_ref.at[part(h)] if distance == 1 else block(owner, h)
        s, r = (gs_r, gr_r) if direction == 1 else (gs_l, gr_l)
        target = next_y if direction == 1 else prev_y
        send(src, block(owner, h), s.at[distance - 1, h], r.at[distance - 1, h], (x, target))

    def cross(number, owner, h):
        src = rows_ref.at[part(h)] if number == 0 else block(owner, h)
        send(src, block(owner, h), ss.at[number, h], sr.at[number, h], (x, sibling))

    def halves_of(direction, distance):
        if distance < reach:
            return (0, 1) if direction == 1 else (1, 0)
        return (0,) if direction == 1 else (1,)

    def split(value, hi_ref, lo_ref, index):
        hi = value.astype(jnp.bfloat16)
        hi_ref[index] = hi
        lo_ref[index] = (value - hi.astype(jnp.float32)).astype(jnp.bfloat16)

    zcopy(1, 0)
    ring(1, 1, 0)
    if reach > 1:
        ring(-1, 1, 1)
        zcopy(1, 1)
        ring(1, 1, 1)
        ring(-1, 1, 0)
    else:
        ring(-1, 1, 1)
        zcopy(1, 1)
    cross(0, y, 0)
    cross(0, y, 1)

    for step, first, count in lists:
        def fill(i, carry, step=step, first=first):
            _, valid, _, tile = piece(x, chip, step, i, nx, half_tiles, half_x)
            targets[first + i] = jnp.where(valid, lax.rem(owner_ref[tile], ny), ny)
            return carry
        lax.fori_loop(0, count, fill, 0)

    me = x * ny + y

    def class_loop(r, carry):
        state = (jnp.int32(0),) + carry
        for step, first, count in lists:
            def look(i, state, step=step):
                seen, found = state[0], state[1:]
                _, valid, rowwise, tile = piece(x, r, step, i, nx, half_tiles, half_x)
                mine = jnp.where(valid, jnp.where(owner_ref[tile] == me, 1, 0), 0)
                slot = slot_ref[tile]
                code = 2 * (r * capacity + jnp.minimum(seen, capacity - 1))
                code = code + jnp.where(rowwise, 1, 0)
                key = jnp.where(mine == 1, slot, slots)
                found = tuple(jnp.where(key == s, code, found[s]) for s in range(slots))
                return (seen + mine,) + found
            state = lax.fori_loop(0, count, look, state)
        return state[1:]

    found = lax.fori_loop(0, half_tiles, class_loop, (jnp.int32(-1),) * slots)

    chosen = []
    for offset in range(ny):
        dest = lax.rem(y + offset, ny)

        def pick(p, state, dest=dest):
            hit = jnp.where(targets[p] == dest, 1, 0)
            seen = state[0]
            key = jnp.where(hit == 1, seen, capacity)
            picks = tuple(jnp.where(key == k, p, state[1 + k]) for k in range(capacity))
            return (seen + hit,) + picks

        chosen.append(lax.fori_loop(0, piece_count, pick, (jnp.int32(0),) * (capacity + 1))[1:])

    def wait_recv(dst, sem):
        pltpu.make_async_remote_copy(
            src_ref=dst, dst_ref=dst, send_sem=sem, recv_sem=sem,
            device_id=(x, sibling), device_id_type=MESH,
        ).wait_recv()

    def split_other(step, h):
        ref = rows_ref.at[part(h)] if step == 0 else zbuf.at[step - 1, part(h)]
        value = ref[...]
        hi = value.astype(jnp.bfloat16)
        zsplit[step, h, :half] = hi
        zsplit[step, h, half:] = (value - hi.astype(jnp.float32)).astype(jnp.bfloat16)

    def take_other(step, h):
        wait_recv(zbuf.at[step - 1, part(h)], zr.at[step - 1, h])
        if step < half_x:
            zcopy(step + 1, h)

    split_other(0, 0)
    split_other(0, 1)
    split(rows_ref[...], chi, clo, y)

    def take_cross(number, owner, halves):
        for h in halves:
            wait_recv(block(owner, h), sr.at[number, h])

    one = functools.partial(
        lax.dot_general,
        dimension_numbers=(((1,), (1,)), ((), ())),
        preferred_element_type=jnp.float32,
    )
    width = rows_ref.shape[1]
    row_inside = core * rows + lax.broadcasted_iota(jnp.int32, (half, 2 * rows), 0)
    col_inside = lax.broadcasted_iota(jnp.int32, (half, 2 * rows), 1)

    def one_piece_of(h):
        above = jnp.where(row_inside + h * half < col_inside, 1, 0)

        def one_piece(i, step, first, col):
            b_hi = chi[pl.ds(2 * col, 2)].reshape(2 * rows, width)
            b_lo = clo[pl.ds(2 * col, 2)].reshape(2 * rows, width)
            both = one(zsplit[step, h], b_hi)
            full = both[:half] + (both[half:] + one(zsplit[step, h, :half], b_lo))
            if step == 0:
                full = jnp.where(above * jnp.where(i == 0, 1, 0) == 1, 0.0, full)
            pieces[h, first + i, 0] = full[:, :rows]
            pieces[h, first + i, 1] = full[:, rows:]

        return one_piece

    farthest = chip_at(lax.rem(place + reach, chips), chips)
    soon = min(reach, half_x) if reach > 1 else 0

    def multiply(h, mode):
        one_piece = one_piece_of(h)
        for step, first, count in lists:
            if mode == "early" and step >= soon:
                continue

            def make(i, carry, step=step, first=first):
                col, _, _, _ = piece(x, chip, step, i, nx, half_tiles, half_x)
                if mode == "all" or step >= soon:
                    one_piece(i, step, first, col)
                else:
                    wanted = (col != farthest) if mode == "early" else (col == farthest)
                    pl.when(wanted)(lambda: one_piece(i, step, first, col))
                return carry
            lax.fori_loop(0, count, make, 0)

    pending = [(0, sibling, (0, 1))]
    for distance in range(1, reach + 1):
        if distance == reach:
            for number, owner, halves in pending[1:]:
                take_cross(number, owner, halves)
                split(gath[owner], chi, clo, owner)
            multiply(0, "early")
        if distance <= half_x:
            for h in (0, 1):
                if (distance, h) != (half_x, 1):
                    take_other(distance, h)
                if h in halves_of(1, distance):
                    owner = at(place - distance)
                    wait_recv(block(owner, h), gr_r.at[distance - 1, h])
                    if distance < reach and h in halves_of(1, distance + 1):
                        ring(1, distance + 1, h)
                    cross(2 * distance - 1, owner, h)
                g = 1 - h
                if g in halves_of(-1, distance):
                    owner = at(place + distance)
                    wait_recv(block(owner, g), gr_l.at[distance - 1, g])
                    if distance < reach and g in halves_of(-1, distance + 1):
                        ring(-1, distance + 1, g)
                    cross(2 * distance, owner, g)
            split_other(distance, 0)
            if distance < half_x:
                split_other(distance, 1)
        behind, ahead = at(place - distance), at(place + distance)
        pending.append((2 * distance - 1, behind + 1 - 2 * core, halves_of(1, distance)))
        pending.append((2 * distance, ahead + 1 - 2 * core, halves_of(-1, distance)))
        split(gath[behind], chi, clo, behind)
        if distance < reach:
            split(gath[ahead], chi, clo, ahead)
        for number, owner, halves in pending[: (1 if distance == 1 else 0)]:
            take_cross(number, owner, halves)
            split(gath[owner], chi, clo, owner)
    for number, owner, halves in pending[-2:]:
        take_cross(number, owner, halves)
    split(gath[pending[-1][1]], chi, clo, pending[-1][1])
    for step in range(reach + 1, half_x + 1):
        for h in (0, 1):
            if (step, h) != (half_x, 1):
                take_other(step, h)
                split_other(step, h)

    def arrival(offset):
        return pl.ds(offset * capacity * 2, capacity * 2)

    def exchange(h, offset):
        send(
            outgoing.at[h, offset], incoming.at[h, arrival(offset)],
            xs.at[h, offset], xr.at[h, offset], (x, lax.rem(y + offset, ny)),
        )

    for h in (0, 1):
        if h == 1:
            take_other(half_x, 1)
            split_other(half_x, 1)
        multiply(h, "all" if h == 1 else "late")
        for offset in range(1, ny):
            for k in range(capacity):
                outgoing[h, offset, 2 * k:2 * k + 2] = pieces[h, chosen[offset][k]]
            if offset > 1:
                exchange(h, offset - 1)
        for k in range(capacity):
            incoming[h, 2 * k:2 * k + 2] = pieces[h, chosen[0][k]]
        exchange(h, ny - 1)
    for h in (0, 1):
        for offset in range(1, ny):
            wait_recv(incoming.at[h, arrival(offset)], xr.at[h, offset])

    for s in range(slots):
        code = found[s]
        there = code >= 0
        safe = jnp.maximum(code, 0)
        rowwise = lax.rem(safe, 2) == 1
        rank = lax.rem(safe // 2, capacity)
        first_source = 2 * (safe // (2 * capacity))
        bases = [
            (lax.rem(y - first_source - h + ny, ny) * capacity + rank) * 2 for h in (0, 1)
        ]
        for i in (0, 1):
            for j in (0, 1):
                place_of = jnp.where(rowwise, bases[i] + j, bases[j] + i)
                value = jnp.concatenate([incoming[0, place_of], incoming[1, place_of]], axis=0)
                value = jnp.where(rowwise, value, value.T)
                out_ref[s, i * rows:(i + 1) * rows, j * rows:(j + 1) * rows] = jnp.where(
                    there, value, 0.0
                )
    for copy in started:
        copy.wait_send()


def plane_kernel(
    dims, rows_hbm, owner_hbm, slot_hbm, out_ref,
    gath, zfar, parts, far_parts, far, extra, owner_ref, slot_ref, todo,
    ins, ss, rs, entered,
):
    nx, ny, half_tiles, slots = dims
    rows, width = zfar.shape
    half = rows // 2
    cuts = (0, width // 2, width * 7 // 8, width)
    x = lax.axis_index("gx")
    y = lax.axis_index("gy")
    core = lax.rem(y, 2)
    chip = lax.div(y, 2)
    twin = 1 - core
    right, left = (lax.rem(x + 1, nx), y), (lax.rem(x + nx - 1, nx), y)
    sibling = (x, y + 1 - 2 * core)
    across = (x, y + 2 - 4 * lax.rem(chip, 2))
    along = (x, lax.rem(y + 4, ny))

    odd, high, ends = lax.rem(chip, 2), lax.div(chip, 2), jnp.where(x == nx - 1, 1, 0)
    earlier = (core, odd, high, jnp.where(x > 0, 1, 0))
    later = (1 - core, 1 - odd, 1 - high, 1 - ends)
    barrier = pltpu.get_barrier_semaphore()

    def signal_if(flag, semaphore, target):
        @pl.when(flag == 1)
        def _():
            pl.semaphore_signal(semaphore, inc=1, device_id=target, device_id_type=MESH)

    for flag, target in zip(later, (sibling, across, along, right)):
        signal_if(flag, barrier, target)
    signal_if(jnp.where(x == 0, 1, 0), barrier, left)
    loads = [
        pltpu.make_async_copy(rows_hbm, gath.at[0, core], ins.at[0]),
        pltpu.make_async_copy(owner_hbm, owner_ref, ins.at[1]),
        pltpu.make_async_copy(slot_hbm, slot_ref, ins.at[2]),
    ]
    for copy in loads:
        copy.start()
    expected = sum(earlier) + ends

    @pl.when(expected > 0)
    def _():
        pl.semaphore_wait(barrier, expected)

    for n, target in enumerate((sibling, across, along, left)):
        signal_if(earlier[n], entered.at[n], target)
    loads[0].wait()

    started, numbers = [], {}

    def number(name):
        return numbers.setdefault(name, len(numbers))

    def ready(name, src, dst, target):
        i = number(name)
        copy = pltpu.make_async_remote_copy(
            src_ref=src, dst_ref=dst, send_sem=ss.at[i], recv_sem=rs.at[i],
            device_id=target, device_id_type=MESH,
        )
        started.append(copy)
        return copy

    def send(*args):
        ready(*args).start()

    def got(name, dst):
        i = number(name)
        pltpu.make_async_remote_copy(
            src_ref=dst, dst_ref=dst, send_sem=rs.at[i], recv_sem=rs.at[i],
            device_id=sibling, device_id_type=MESH,
        ).wait_recv()

    def block(where, side, h):
        return gath.at[where, side, pl.ds(h * half, half)]

    def cross(where, h):
        send(("cross", where, h), block(where, core, h), block(where, core, h), sibling)

    def strip(where, side, c):
        return gath.at[where, side, :, pl.ds(cuts[c], cuts[c + 1] - cuts[c])]

    def crossed(where, h):
        got(("cross", where, h), block(where, twin, h))
        split(where, twin, h)

    def split_at(where, side, part):
        value = gath[where, side, part[0], part[1]]
        hi = value.astype(jnp.bfloat16)
        parts[where, 0, side, part[0], part[1]] = hi
        parts[where, 1, side, part[0], part[1]] = (
            value - hi.astype(jnp.float32)
        ).astype(jnp.bfloat16)

    def split(where, side, h):
        split_at(where, side, (slice(h * half, (h + 1) * half), slice(None)))

    def split_strip(side, c):
        split_at(7, side, (slice(None), slice(cuts[c], cuts[c + 1])))

    first = [
        [ready(("cross", 0, h), block(0, core, h), block(0, core, h), sibling) for h in (0, 1)],
        [ready(("x", 0, h), block(0, core, h), block(1, core, h), across) for h in (0, 1)],
        [ready(("y", 0, h), block(0, core, h), block(2, core, h), along) for h in (1, 0)],
        [ready(("z", 0, h), block(0, core, h), block(4, core, h), right) for h in (0, 1)],
    ]

    def open_way(n, early):
        @pl.when(later[n] == (0 if early else 1))
        def _():
            if not early:
                pl.semaphore_wait(entered.at[n], 1)
            for copy in first[n]:
                copy.start()

    for n in (3, 1, 2, 0):
        open_way(n, True)
    for n in (1, 2, 0):
        open_way(n, False)
    for h in (0, 1):
        split(0, core, h)
    open_way(3, False)
    for copy in loads[1:]:
        copy.wait()

    me = x * ny + y

    def look(tile, state):
        i_tile, j_tile = state[0], state[1]
        a, i = lax.div(i_tile, half_tiles), lax.rem(i_tile, half_tiles)
        b, j = lax.div(j_tile, half_tiles), lax.rem(j_tile, half_tiles)
        i_chip, j_chip = jnp.bitwise_xor(i, chip), jnp.bitwise_xor(j, chip)
        i_near, j_near = jnp.where(a == x, 0, half_tiles), jnp.where(b == x, 0, half_tiles)
        same = jnp.where(i_tile == j_tile, 256, 0)
        last = jnp.where((i_near + i_chip == 7) | (j_near + j_chip == 7), 64, 0)
        near = i_near + i_chip + 8 * (j_near + j_chip) + same + last
        far_code = 128 + jnp.where(
            a == x, j_chip + 8 * lax.div(i, 2), i_chip + 8 * lax.div(j, 2)
        )
        code = jnp.where(a - b == nx // 2, far_code, near)
        key = jnp.where(owner_ref[tile] == me, slot_ref[tile], slots)
        found = tuple(jnp.where(key == s, code, state[2 + s]) for s in range(slots))
        wrap = j_tile == i_tile
        return (
            jnp.where(wrap, i_tile + 1, i_tile), jnp.where(wrap, 0, j_tile + 1)
        ) + found

    codes = lax.fori_loop(
        0, owner_ref.shape[0], look, (jnp.int32(0),) * 2 + (jnp.int32(-1),) * slots
    )[2:]
    seen, picks, ranks = jnp.int32(0), [jnp.int32(0)] * 2, []
    kinds = []
    for s in range(slots):
        code = codes[s]
        kind = jnp.where(code < 0, 3, lax.rem(lax.div(code, 64), 4))
        kinds.append(kind)
        todo[s] = jnp.where(kind == 0, code, 0)
        is_last = jnp.where(kind == 1, 1, 0)
        ranks.append(seen)
        picks = [
            jnp.where(is_last * jnp.where(seen == k, 1, 0) == 1, code, picks[k])
            for k in range(2)
        ]
        seen = seen + is_last
    for k in range(2):
        todo[slots + k] = picks[k]

    one = functools.partial(
        lax.dot_general,
        dimension_numbers=(((1,), (1,)), ((), ())),
        preferred_element_type=jnp.float32,
    )

    def product(code, lo, hi):
        lhs, rhs = lax.rem(code, 8), lax.rem(lax.div(code, 8), 8)
        deep = hi - lo

        def part(n):
            return parts[rhs, n, :, :, lo:hi].reshape(2 * rows, deep)

        both = one(parts[lhs, :, :, :, lo:hi].reshape(4 * rows, deep), part(0))
        return both[:2 * rows] + (
            both[2 * rows:]
            + one(parts[lhs, 0, :, :, lo:hi].reshape(2 * rows, deep), part(1))
        )

    got(("x", 0, 0), block(1, core, 0))
    send(("y", 3, 0), block(1, core, 0), block(3, core, 0), along)
    got(("y", 0, 1), block(2, core, 1))
    send(("x", 3, 1), block(2, core, 1), block(3, core, 1), across)
    cross(1, 0)
    cross(2, 1)
    got(("z", 0, 0), block(4, core, 0))
    send(("z", 1, 0), block(4, core, 0), zfar.at[pl.ds(0, half)], right)
    cross(4, 0)
    split(1, core, 0)
    split(2, core, 1)
    split(4, core, 0)
    crossed(0, 0)
    crossed(0, 1)
    crossed(1, 0)
    crossed(2, 1)
    crossed(4, 0)
    got(("x", 0, 1), block(1, core, 1))
    cross(1, 1)
    got(("y", 0, 0), block(2, core, 0))
    cross(2, 0)
    got(("z", 0, 1), block(4, core, 1))
    send(("z", 1, 1), block(4, core, 1), zfar.at[pl.ds(half, half)], right)
    for h in (0, 1):
        send(("x", 4, h), block(4, core, h), block(5, core, h), across)
        send(("y", 4, 1 - h), block(4, core, 1 - h), block(6, core, 1 - h), along)
    cross(4, 1)
    split(1, core, 1)
    split(2, core, 0)
    split(4, core, 1)
    crossed(1, 1)
    crossed(2, 0)
    crossed(4, 1)
    got(("y", 3, 0), block(3, core, 0))
    cross(3, 0)
    got(("x", 3, 1), block(3, core, 1))
    cross(3, 1)
    for c in (0, 1):
        send(("z", 3, c), strip(3, core, c), strip(7, core, c), right)
    split(3, core, 0)
    split(3, core, 1)
    crossed(3, 0)
    crossed(3, 1)

    def corner(where, side, h):
        return gath.at[where, side, pl.ds(h * half, half), pl.ds(cuts[2], width - cuts[2])]

    got(("x", 4, 0), block(5, core, 0))
    send(("y", 7), corner(5, core, 0), corner(7, core, 0), along)
    got(("y", 4, 1), block(6, core, 1))
    send(("x", 7), corner(6, core, 1), corner(7, core, 1), across)
    cross(5, 0)
    cross(6, 1)
    split(5, core, 0)
    split(6, core, 1)
    crossed(5, 0)
    crossed(6, 1)

    def split_far(h):
        part = slice(h * half, (h + 1) * half)
        value = zfar[part]
        hi = value.astype(jnp.bfloat16)
        far_parts[0, part] = hi
        far_parts[1, part] = (value - hi.astype(jnp.float32)).astype(jnp.bfloat16)

    flag = jnp.where(x >= nx // 2, 1, 0)
    got(("z", 1, 0), zfar.at[pl.ds(0, half)])
    split_far(0)
    got(("z", 1, 1), zfar.at[pl.ds(half, half)])
    split_far(1)
    for t in (0, 1):
        col = flag + 2 * lax.rem(t + lax.div(chip, 2), 2)
        both = one(
            far_parts[...].reshape(2 * rows, width), parts[col, 0].reshape(2 * rows, width)
        )
        full = both[:rows] + (
            both[rows:] + one(far_parts[0], parts[col, 1].reshape(2 * rows, width))
        )
        for k in (0, 1):
            piece_k = full[:, k * rows:(k + 1) * rows]
            far[0, core, t, k] = jnp.where(flag == 0, piece_k, piece_k.T)

    def far_at(where, side, t):
        return far.at[where, side, t]

    def far_cross(where, t):
        send(("fcross", where, t), far_at(where, core, t), far_at(where, core, t), sibling)

    for t in (0, 1):
        send(("fx", 0, t), far_at(0, core, t), far_at(1, core, t), across)
        send(("fy", 0, 1 - t), far_at(0, core, 1 - t), far_at(2, core, 1 - t), along)
    for t in (0, 1):
        far_cross(0, t)

    got(("x", 4, 1), block(5, core, 1))
    cross(5, 1)
    got(("y", 4, 0), block(6, core, 0))
    cross(6, 0)
    split(5, core, 1)
    split(6, core, 0)
    got(("y", 7), corner(7, core, 0))
    got(("x", 7), corner(7, core, 1))
    send(("cross", 7, 2), strip(7, core, 2), strip(7, core, 2), sibling)
    split_strip(core, 2)
    crossed(5, 1)
    crossed(6, 0)

    above = jnp.where(
        lax.broadcasted_iota(jnp.int32, (2 * rows, 2 * rows), 0)
        < lax.broadcasted_iota(jnp.int32, (2 * rows, 2 * rows), 1), 1, 0,
    )

    def local(s, carry):
        code = todo[s]
        masked = jnp.where(code >= 256, 1, 0)
        out_ref[s] = jnp.where(above * masked == 1, 0.0, product(code, 0, width))
        return carry

    def take_strip(c):
        got(("z", 3, c), strip(7, core, c))
        send(("cross", 7, c), strip(7, core, c), strip(7, core, c), sibling)
        split_strip(core, c)

    def twin_strip(c):
        got(("cross", 7, c), strip(7, twin, c))
        split_strip(twin, c)

    middle = slots // 2
    lax.fori_loop(0, middle, local, 0)
    got(("fx", 0, 0), far_at(1, core, 0))
    send(("fy", 3, 0), far_at(1, core, 0), far_at(3, core, 0), along)
    got(("fy", 0, 1), far_at(2, core, 1))
    send(("fx", 3, 1), far_at(2, core, 1), far_at(3, core, 1), across)
    far_cross(1, 0)
    far_cross(2, 1)
    take_strip(0)
    lax.fori_loop(middle, slots, local, 0)
    twin_strip(2)
    twin_strip(0)

    def behind(k, carry):
        extra[k] = product(todo[slots + k], 0, cuts[1])
        return carry

    lax.fori_loop(0, 2, behind, 0)
    got(("fx", 0, 1), far_at(1, core, 1))
    far_cross(1, 1)
    got(("fy", 0, 0), far_at(2, core, 0))
    far_cross(2, 0)
    take_strip(1)
    twin_strip(1)

    def behind_more(k, carry):
        extra[k] = extra[k] + product(todo[slots + k], cuts[1], width)
        return carry

    lax.fori_loop(0, 2, behind_more, 0)
    got(("fy", 3, 0), far_at(3, core, 0))
    far_cross(3, 0)
    got(("fx", 3, 1), far_at(3, core, 1))
    far_cross(3, 1)
    for where in range(4):
        for t in (0, 1):
            got(("fcross", where, t), far_at(where, twin, t))

    for s in range(slots):
        kind, code = kinds[s], jnp.maximum(codes[s], 0)
        where = lax.rem(code, 4)
        t = lax.rem(lax.div(code, 8), 2)
        rank = jnp.minimum(ranks[s], 1)
        for i in (0, 1):
            for j in (0, 1):
                side, k = jnp.where(flag == 0, i, j), jnp.where(flag == 0, j, i)
                at = (s, slice(i * rows, (i + 1) * rows), slice(j * rows, (j + 1) * rows))
                value = jnp.where(kind == 1, extra[rank, at[1], at[2]], out_ref[at])
                value = jnp.where(kind == 2, far[where, side, t, k], value)
                out_ref[at] = jnp.where(kind == 3, 0.0, value)
    for copy in started:
        copy.wait_send()


def plane_call(dims, *arrays):
    nx, ny, half_tiles, slots = dims
    matrix_rows, tile_owner, tile_slot = arrays
    rows, width = matrix_rows.shape
    f32, bf16 = jnp.float32, jnp.bfloat16
    dma = pltpu.SemaphoreType.DMA
    hbm = pl.BlockSpec(memory_space=pltpu.HBM)
    return pl.pallas_call(
        functools.partial(plane_kernel, dims),
        out_shape=jax.ShapeDtypeStruct((slots, 2 * rows, 2 * rows), f32),
        in_specs=[hbm, hbm, hbm],
        out_specs=pl.BlockSpec(memory_space=pltpu.VMEM),
        scratch_shapes=[
            pltpu.VMEM((8, 2, rows, width), f32),
            pltpu.VMEM((rows, width), f32),
            pltpu.VMEM((8, 2, 2, rows, width), bf16),
            pltpu.VMEM((2, rows, width), bf16),
            pltpu.VMEM((4, 2, 2, 2, rows, rows), f32),
            pltpu.VMEM((2, 2 * rows, 2 * rows), f32),
            pltpu.SMEM(tile_owner.shape, jnp.int32),
            pltpu.SMEM(tile_slot.shape, jnp.int32),
            pltpu.SMEM((slots + 2,), jnp.int32),
            dma((3,)), dma((64,)), dma((64,)), pltpu.SemaphoreType.REGULAR((4,)),
        ],
        compiler_params=pltpu.CompilerParams(
            collective_id=0, has_side_effects=True,
            vmem_limit_bytes=44 * 1024 * 1024,
        ),
    )(*(pltpu.with_memory_space_constraint(a, pltpu.HBM) for a in arrays))


def copy_out(in_ref, out_ref, sem):
    copy = pltpu.make_async_copy(in_ref, out_ref, sem)
    copy.start()
    copy.wait()


def ring_call(mesh_shape, matrix_rows, tile_owner, tile_slot):
    nx, ny = mesh_shape
    rows, width = matrix_rows.shape
    half_tiles, half_x = ny // 2, nx // 2
    capacity = nx // 4 + 1
    slots = -(-tile_owner.shape[0] // (nx * ny))
    _, piece_count = piece_lists(half_tiles, half_x)
    reach = max(ny // 4, 1)
    f32, bf16 = jnp.float32, jnp.bfloat16
    dma = pltpu.SemaphoreType.DMA
    return pl.pallas_call(
        functools.partial(kernel, (nx, ny, half_tiles, half_x, capacity, slots)),
        out_shape=jax.ShapeDtypeStruct((slots, 2 * rows, 2 * rows), f32),
        in_specs=[
            pl.BlockSpec(memory_space=pltpu.VMEM),
            pl.BlockSpec(memory_space=pltpu.SMEM),
            pl.BlockSpec(memory_space=pltpu.SMEM),
        ],
        out_specs=pl.BlockSpec(memory_space=pltpu.VMEM),
        scratch_shapes=[
            pltpu.VMEM((ny, rows, width), f32),
            pltpu.VMEM((half_x, rows, width), f32),
            pltpu.VMEM((ny, rows, width), bf16),
            pltpu.VMEM((ny, rows, width), bf16),
            pltpu.VMEM((half_x + 1, 2, rows, width), bf16),
            pltpu.VMEM((2, piece_count, 2, rows // 2, rows), f32),
            pltpu.VMEM((2, ny, 2 * capacity, rows // 2, rows), f32),
            pltpu.VMEM((2, ny * 2 * capacity, rows // 2, rows), f32),
            pltpu.SMEM((piece_count,), jnp.int32),
            dma((reach, 2)), dma((reach, 2)), dma((reach, 2)), dma((reach, 2)),
            dma((2 * reach + 1, 2)), dma((2 * reach + 1, 2)),
            dma((half_x, 2)), dma((half_x, 2)),
            dma((2, ny)), dma((2, ny)),
        ],
        compiler_params=pltpu.CompilerParams(
            collective_id=0, has_side_effects=True, vmem_limit_bytes=44 * 1024 * 1024
        ),
    )(matrix_rows, tile_owner, tile_slot)


def per_device(mesh_shape, matrix_rows, tile_owner, tile_slot):
    nx, ny = mesh_shape
    if ny // 2 == 4 and nx == 4:
        slots = -(-tile_owner.shape[0] // (nx * ny))
        packed = plane_call((nx, ny, ny // 2, slots), matrix_rows, tile_owner, tile_slot)
    else:
        packed = ring_call(mesh_shape, matrix_rows, tile_owner, tile_slot)
    return pl.pallas_call(
        copy_out,
        out_shape=jax.ShapeDtypeStruct(packed.shape, packed.dtype),
        in_specs=[pl.BlockSpec(memory_space=pltpu.VMEM)],
        out_specs=pl.BlockSpec(memory_space=pl.ANY),
        scratch_shapes=[pltpu.SemaphoreType.DMA(())],
        compiler_params=pltpu.CompilerParams(vmem_limit_bytes=4 * 1024 * 1024),
    )(packed)


def solution(mesh):
    placed = (P(("gx", "gy"), None), P(), P())
    return jax.shard_map(
        functools.partial(per_device, (mesh.shape["gx"], mesh.shape["gy"])),
        mesh=mesh,
        in_specs=placed,
        out_specs=P(("gx", "gy"), None, None),
        check_vma=False,
    )
```

```python
import functools

import jax
import jax.numpy as jnp
from jax import lax
from jax.experimental import pallas as pl
from jax.experimental.pallas import tpu as pltpu
from jax.sharding import PartitionSpec as P

MESH = pl.DeviceIdType.MESH


def chip_position(chip, chips):
    row, col = lax.div(chip, 2), lax.rem(chip, 2)
    return col * (1 + row) + (1 - col) * lax.rem(chips - row, chips)


def chip_at(position, chips):
    behind = lax.rem(position + chips - 1, chips)
    far = lax.div(behind, chips // 2)
    return (1 - far) * (2 * behind + 1) + far * 2 * (chips - 1 - behind)


def piece_lists(half_tiles, half_x):
    lists, start = [], 0
    for step in range(half_x + 1):
        if step == 0:
            count = half_tiles // 2 + 1
        elif step < half_x:
            count = half_tiles
        else:
            count = half_tiles // 2
        lists.append((step, start, count))
        start += count
    return lists, start


def piece(x, r, step, i, nx, half_tiles, half_x):
    source = lax.rem(x - step + nx, nx)
    if step == 0:
        col = lax.rem(r - i + half_tiles, half_tiles)
        valid = jnp.logical_or(i < half_tiles // 2, r < half_tiles // 2)
        rowwise = col <= r
    elif step < half_x:
        col = i
        valid = i >= 0
        rowwise = source > x
    else:
        flag = jnp.where(x >= half_x, 1, 0)
        col = 2 * i + lax.rem(r + flag, 2)
        valid = i >= 0
        rowwise = source > x
    other, mine = source * half_tiles + r, x * half_tiles + col
    row_tile = jnp.where(rowwise, other, mine)
    col_tile = jnp.where(rowwise, mine, other)
    tile = jnp.where(valid, row_tile * (row_tile + 1) // 2 + col_tile, 0)
    return col, valid, rowwise, tile


def kernel(
    dims, rows_ref, owner_ref, slot_ref, out_ref,
    gath, zbuf, chi, clo, zsplit, pieces, outgoing, incoming, targets,
    gs_r, gr_r, gs_l, gr_l, ss, sr, zs, zr, xs, xr,
):
    nx, ny, half_tiles, half_x, capacity, slots = dims
    rows = rows_ref.shape[0]
    half = rows // 2
    chips = ny // 2
    reach = chips // 2
    x = lax.axis_index("gx")
    y = lax.axis_index("gy")
    core = lax.rem(y, 2)
    chip = lax.div(y, 2)
    right_x, left_x = lax.rem(x + 1, nx), lax.rem(x + nx - 1, nx)
    sibling = y + 1 - 2 * core
    place = chip_position(chip, chips)

    def at(position):
        return 2 * chip_at(lax.rem(position + chips, chips), chips) + core

    next_y, prev_y = at(place + 1), at(place - 1)
    lists, piece_count = piece_lists(half_tiles, half_x)

    barrier = pltpu.get_barrier_semaphore()
    for other in (right_x, left_x):
        pl.semaphore_signal(barrier, inc=1, device_id=(other, y), device_id_type=MESH)
    for offset in range(1, ny):
        pl.semaphore_signal(
            barrier, inc=1, device_id=(x, lax.rem(y + offset, ny)), device_id_type=MESH
        )
    pl.semaphore_wait(barrier, ny + 1)

    started = []

    def send(src, dst, send_sem, recv_sem, target):
        copy = pltpu.make_async_remote_copy(
            src_ref=src, dst_ref=dst, send_sem=send_sem, recv_sem=recv_sem,
            device_id=target, device_id_type=MESH,
        )
        copy.start()
        started.append(copy)

    def part(h):
        return pl.ds(h * half, half)

    def zcopy(step, h):
        src = rows_ref.at[part(h)] if step == 1 else zbuf.at[step - 2, part(h)]
        send(src, zbuf.at[step - 1, part(h)], zs.at[step - 1, h], zr.at[step - 1, h], (right_x, y))

    def block(owner, h):
        return gath.at[owner, part(h)]

    def ring(direction, distance, h):
        owner = at(place - direction * (distance - 1))
        src = rows_ref.at[part(h)] if distance == 1 else block(owner, h)
        s, r = (gs_r, gr_r) if direction == 1 else (gs_l, gr_l)
        target = next_y if direction == 1 else prev_y
        send(src, block(owner, h), s.at[distance - 1, h], r.at[distance - 1, h], (x, target))

    def cross(number, owner, h):
        src = rows_ref.at[part(h)] if number == 0 else block(owner, h)
        send(src, block(owner, h), ss.at[number, h], sr.at[number, h], (x, sibling))

    def halves_of(direction, distance):
        if distance < reach:
            return (0, 1) if direction == 1 else (1, 0)
        return (0,) if direction == 1 else (1,)

    def split(value, hi_ref, lo_ref, index):
        hi = value.astype(jnp.bfloat16)
        hi_ref[index] = hi
        lo_ref[index] = (value - hi.astype(jnp.float32)).astype(jnp.bfloat16)

    zcopy(1, 0)
    ring(1, 1, 0)
    if reach > 1:
        ring(-1, 1, 1)
        zcopy(1, 1)
        ring(1, 1, 1)
        ring(-1, 1, 0)
    else:
        ring(-1, 1, 1)
        zcopy(1, 1)
    cross(0, y, 0)
    cross(0, y, 1)

    for step, first, count in lists:
        def fill(i, carry, step=step, first=first):
            _, valid, _, tile = piece(x, chip, step, i, nx, half_tiles, half_x)
            targets[first + i] = jnp.where(valid, lax.rem(owner_ref[tile], ny), ny)
            return carry
        lax.fori_loop(0, count, fill, 0)

    me = x * ny + y

    def class_loop(r, carry):
        state = (jnp.int32(0),) + carry
        for step, first, count in lists:
            def look(i, state, step=step):
                seen, found = state[0], state[1:]
                _, valid, rowwise, tile = piece(x, r, step, i, nx, half_tiles, half_x)
                mine = jnp.where(valid, jnp.where(owner_ref[tile] == me, 1, 0), 0)
                slot = slot_ref[tile]
                code = 2 * (r * capacity + jnp.minimum(seen, capacity - 1))
                code = code + jnp.where(rowwise, 1, 0)
                key = jnp.where(mine == 1, slot, slots)
                found = tuple(jnp.where(key == s, code, found[s]) for s in range(slots))
                return (seen + mine,) + found
            state = lax.fori_loop(0, count, look, state)
        return state[1:]

    found = lax.fori_loop(0, half_tiles, class_loop, (jnp.int32(-1),) * slots)

    chosen = []
    for offset in range(ny):
        dest = lax.rem(y + offset, ny)

        def pick(p, state, dest=dest):
            hit = jnp.where(targets[p] == dest, 1, 0)
            seen = state[0]
            key = jnp.where(hit == 1, seen, capacity)
            picks = tuple(jnp.where(key == k, p, state[1 + k]) for k in range(capacity))
            return (seen + hit,) + picks

        chosen.append(lax.fori_loop(0, piece_count, pick, (jnp.int32(0),) * (capacity + 1))[1:])

    def wait_recv(dst, sem):
        pltpu.make_async_remote_copy(
            src_ref=dst, dst_ref=dst, send_sem=sem, recv_sem=sem,
            device_id=(x, sibling), device_id_type=MESH,
        ).wait_recv()

    def split_other(step, h):
        ref = rows_ref.at[part(h)] if step == 0 else zbuf.at[step - 1, part(h)]
        value = ref[...]
        hi = value.astype(jnp.bfloat16)
        zsplit[step, h, :half] = hi
        zsplit[step, h, half:] = (value - hi.astype(jnp.float32)).astype(jnp.bfloat16)

    def take_other(step, h):
        wait_recv(zbuf.at[step - 1, part(h)], zr.at[step - 1, h])
        if step < half_x:
            zcopy(step + 1, h)

    split_other(0, 0)
    split_other(0, 1)
    split(rows_ref[...], chi, clo, y)

    def take_cross(number, owner, halves):
        for h in halves:
            wait_recv(block(owner, h), sr.at[number, h])

    one = functools.partial(
        lax.dot_general,
        dimension_numbers=(((1,), (1,)), ((), ())),
        preferred_element_type=jnp.float32,
    )
    width = rows_ref.shape[1]
    row_inside = core * rows + lax.broadcasted_iota(jnp.int32, (half, 2 * rows), 0)
    col_inside = lax.broadcasted_iota(jnp.int32, (half, 2 * rows), 1)

    def one_piece_of(h):
        above = jnp.where(row_inside + h * half < col_inside, 1, 0)

        def one_piece(i, step, first, col):
            b_hi = chi[pl.ds(2 * col, 2)].reshape(2 * rows, width)
            b_lo = clo[pl.ds(2 * col, 2)].reshape(2 * rows, width)
            both = one(zsplit[step, h], b_hi)
            full = both[:half] + (both[half:] + one(zsplit[step, h, :half], b_lo))
            if step == 0:
                full = jnp.where(above * jnp.where(i == 0, 1, 0) == 1, 0.0, full)
            pieces[h, first + i, 0] = full[:, :rows]
            pieces[h, first + i, 1] = full[:, rows:]

        return one_piece

    farthest = chip_at(lax.rem(place + reach, chips), chips)
    soon = min(reach, half_x) if reach > 1 else 0

    def multiply(h, mode):
        one_piece = one_piece_of(h)
        for step, first, count in lists:
            if mode == "early" and step >= soon:
                continue

            def make(i, carry, step=step, first=first):
                col, _, _, _ = piece(x, chip, step, i, nx, half_tiles, half_x)
                if mode == "all" or step >= soon:
                    one_piece(i, step, first, col)
                else:
                    wanted = (col != farthest) if mode == "early" else (col == farthest)
                    pl.when(wanted)(lambda: one_piece(i, step, first, col))
                return carry
            lax.fori_loop(0, count, make, 0)

    pending = [(0, sibling, (0, 1))]
    for distance in range(1, reach + 1):
        if distance == reach:
            for number, owner, halves in pending[1:]:
                take_cross(number, owner, halves)
                split(gath[owner], chi, clo, owner)
            multiply(0, "early")
        if distance <= half_x:
            for h in (0, 1):
                if (distance, h) != (half_x, 1):
                    take_other(distance, h)
                if h in halves_of(1, distance):
                    owner = at(place - distance)
                    wait_recv(block(owner, h), gr_r.at[distance - 1, h])
                    if distance < reach and h in halves_of(1, distance + 1):
                        ring(1, distance + 1, h)
                    cross(2 * distance - 1, owner, h)
                g = 1 - h
                if g in halves_of(-1, distance):
                    owner = at(place + distance)
                    wait_recv(block(owner, g), gr_l.at[distance - 1, g])
                    if distance < reach and g in halves_of(-1, distance + 1):
                        ring(-1, distance + 1, g)
                    cross(2 * distance, owner, g)
            split_other(distance, 0)
            if distance < half_x:
                split_other(distance, 1)
        behind, ahead = at(place - distance), at(place + distance)
        pending.append((2 * distance - 1, behind + 1 - 2 * core, halves_of(1, distance)))
        pending.append((2 * distance, ahead + 1 - 2 * core, halves_of(-1, distance)))
        split(gath[behind], chi, clo, behind)
        if distance < reach:
            split(gath[ahead], chi, clo, ahead)
        for number, owner, halves in pending[: (1 if distance == 1 else 0)]:
            take_cross(number, owner, halves)
            split(gath[owner], chi, clo, owner)
    for number, owner, halves in pending[-2:]:
        take_cross(number, owner, halves)
    split(gath[pending[-1][1]], chi, clo, pending[-1][1])
    for step in range(reach + 1, half_x + 1):
        for h in (0, 1):
            if (step, h) != (half_x, 1):
                take_other(step, h)
                split_other(step, h)

    def arrival(offset):
        return pl.ds(offset * capacity * 2, capacity * 2)

    def exchange(h, offset):
        send(
            outgoing.at[h, offset], incoming.at[h, arrival(offset)],
            xs.at[h, offset], xr.at[h, offset], (x, lax.rem(y + offset, ny)),
        )

    for h in (0, 1):
        if h == 1:
            take_other(half_x, 1)
            split_other(half_x, 1)
        multiply(h, "all" if h == 1 else "late")
        for offset in range(1, ny):
            for k in range(capacity):
                outgoing[h, offset, 2 * k:2 * k + 2] = pieces[h, chosen[offset][k]]
            if offset > 1:
                exchange(h, offset - 1)
        for k in range(capacity):
            incoming[h, 2 * k:2 * k + 2] = pieces[h, chosen[0][k]]
        exchange(h, ny - 1)
    for h in (0, 1):
        for offset in range(1, ny):
            wait_recv(incoming.at[h, arrival(offset)], xr.at[h, offset])

    for s in range(slots):
        code = found[s]
        there = code >= 0
        safe = jnp.maximum(code, 0)
        rowwise = lax.rem(safe, 2) == 1
        rank = lax.rem(safe // 2, capacity)
        first_source = 2 * (safe // (2 * capacity))
        bases = [
            (lax.rem(y - first_source - h + ny, ny) * capacity + rank) * 2 for h in (0, 1)
        ]
        for i in (0, 1):
            for j in (0, 1):
                place_of = jnp.where(rowwise, bases[i] + j, bases[j] + i)
                value = jnp.concatenate([incoming[0, place_of], incoming[1, place_of]], axis=0)
                value = jnp.where(rowwise, value, value.T)
                out_ref[s, i * rows:(i + 1) * rows, j * rows:(j + 1) * rows] = jnp.where(
                    there, value, 0.0
                )
    for copy in started:
        copy.wait_send()


def plane_kernel(
    dims, rows_hbm, owner_hbm, slot_hbm, out_ref,
    gath, zfar, parts, far_parts, far, extra, owner_ref, slot_ref, todo,
    ins, ss, rs, entered,
):
    nx, ny, half_tiles, slots = dims
    rows, width = zfar.shape
    half = rows // 2
    cuts = (0, width // 2, width)
    x = lax.axis_index("gx")
    y = lax.axis_index("gy")
    core = lax.rem(y, 2)
    chip = lax.div(y, 2)
    twin = 1 - core
    right, left = (lax.rem(x + 1, nx), y), (lax.rem(x + nx - 1, nx), y)
    sibling = (x, y + 1 - 2 * core)
    across = (x, y + 2 - 4 * lax.rem(chip, 2))
    along = (x, lax.rem(y + 4, ny))

    odd, high, ends = lax.rem(chip, 2), lax.div(chip, 2), jnp.where(x == nx - 1, 1, 0)
    earlier = (core, odd, high, jnp.where(x > 0, 1, 0))
    later = (1 - core, 1 - odd, 1 - high, 1 - ends)
    barrier = pltpu.get_barrier_semaphore()

    def signal_if(flag, semaphore, target):
        @pl.when(flag == 1)
        def _():
            pl.semaphore_signal(semaphore, inc=1, device_id=target, device_id_type=MESH)

    for flag, target in zip(later, (sibling, across, along, right)):
        signal_if(flag, barrier, target)
    signal_if(jnp.where(x == 0, 1, 0), barrier, left)
    loads = [
        pltpu.make_async_copy(
            rows_hbm.at[pl.ds(h * half, half)], gath.at[0, core, pl.ds(h * half, half)],
            ins.at[h],
        )
        for h in (0, 1)
    ] + [
        pltpu.make_async_copy(owner_hbm, owner_ref, ins.at[2]),
        pltpu.make_async_copy(slot_hbm, slot_ref, ins.at[3]),
    ]
    for copy in loads:
        copy.start()
    expected = sum(earlier) + ends

    @pl.when(expected > 0)
    def _():
        pl.semaphore_wait(barrier, expected)

    for n, target in enumerate((sibling, across, along, left)):
        signal_if(earlier[n], entered.at[n], target)
    loads[0].wait()
    loads[1].wait()

    numbers, flying, issued = {}, {}, {}
    ways = {"x": (across, 0), "y": (along, 4), "z": (right, 8), "c": (sibling, 12)}

    def number(name):
        return numbers.setdefault(name, len(numbers))

    def ready(way, name, src, dst):
        target, base = ways[way]
        turn = issued.get(way, 0)
        issued[way] = turn + 1
        i, j = number(name), base + turn % 4
        if j in flying:
            flying[j].wait_send()
        copy = pltpu.make_async_remote_copy(
            src_ref=src, dst_ref=dst, send_sem=ss.at[j], recv_sem=rs.at[i],
            device_id=target, device_id_type=MESH,
        )
        flying[j] = copy
        return copy

    def send(*args):
        ready(*args).start()

    def got(name, dst):
        i = number(name)
        pltpu.make_async_remote_copy(
            src_ref=dst, dst_ref=dst, send_sem=rs.at[i], recv_sem=rs.at[i],
            device_id=sibling, device_id_type=MESH,
        ).wait_recv()

    def block(where, side, h):
        return gath.at[where, side, pl.ds(h * half, half)]

    def cross(where, h, name):
        send("c", ("cross", name), block(where, core, h), block(where, core, h))

    def crossed(where, h, name):
        got(("cross", name), block(where, twin, h))
        split(where, twin, h)

    def both_crossed(where):
        got(("cross", where), gath.at[where, twin])
        split(where, twin, 0)
        split(where, twin, 1)

    def strip(where, side, c):
        return gath.at[where, side, :, pl.ds(cuts[c], cuts[c + 1] - cuts[c])]

    def split_at(where, side, part):
        value = gath[where, side, part[0], part[1]]
        hi = value.astype(jnp.bfloat16)
        parts[where, 0, side, part[0], part[1]] = hi
        parts[where, 1, side, part[0], part[1]] = (
            value - hi.astype(jnp.float32)
        ).astype(jnp.bfloat16)

    def split(where, side, h):
        split_at(where, side, (slice(h * half, (h + 1) * half), slice(None)))

    def split_strip(side, c):
        split_at(7, side, (slice(None), slice(cuts[c], cuts[c + 1])))

    first = [
        [ready("c", ("cross", 0), block(0, core, h), block(0, core, h)) for h in (0, 1)],
        [ready("x", ("x", 0, h), block(0, core, h), block(1, core, h)) for h in (0, 1)],
        [ready("y", ("y", 0, h), block(0, core, h), block(2, core, h)) for h in (1, 0)],
        [ready("z", ("z", 0, h), block(0, core, h), block(4, core, h)) for h in (0, 1)],
    ]

    def open_way(n, early):
        @pl.when(later[n] == (0 if early else 1))
        def _():
            if not early:
                pl.semaphore_wait(entered.at[n], 1)
            for copy in first[n]:
                copy.start()

    for n in (3, 1, 2, 0):
        open_way(n, True)
    for n in (1, 2, 0):
        open_way(n, False)
    for h in (0, 1):
        split(0, core, h)
    open_way(3, False)
    for copy in loads[2:]:
        copy.wait()

    me = x * ny + y

    def look(tile, state):
        i_tile, j_tile = state[0], state[1]
        a, i = lax.div(i_tile, half_tiles), lax.rem(i_tile, half_tiles)
        b, j = lax.div(j_tile, half_tiles), lax.rem(j_tile, half_tiles)
        i_chip, j_chip = jnp.bitwise_xor(i, chip), jnp.bitwise_xor(j, chip)
        i_near, j_near = jnp.where(a == x, 0, half_tiles), jnp.where(b == x, 0, half_tiles)
        same = jnp.where(i_tile == j_tile, 256, 0)
        last = jnp.where((i_near + i_chip == 7) | (j_near + j_chip == 7), 64, 0)
        near = i_near + i_chip + 8 * (j_near + j_chip) + same + last
        far_code = 128 + jnp.where(
            a == x, j_chip + 8 * lax.div(i, 2), i_chip + 8 * lax.div(j, 2)
        )
        code = jnp.where(a - b == nx // 2, far_code, near)
        key = jnp.where(owner_ref[tile] == me, slot_ref[tile], slots)
        found = tuple(jnp.where(key == s, code, state[2 + s]) for s in range(slots))
        wrap = j_tile == i_tile
        return (
            jnp.where(wrap, i_tile + 1, i_tile), jnp.where(wrap, 0, j_tile + 1)
        ) + found

    codes = lax.fori_loop(
        0, owner_ref.shape[0], look, (jnp.int32(0),) * 2 + (jnp.int32(-1),) * slots
    )[2:]
    seen, picks, ranks = jnp.int32(0), [jnp.int32(0)] * 2, []
    kinds = []
    for s in range(slots):
        code = codes[s]
        kind = jnp.where(code < 0, 3, lax.rem(lax.div(code, 64), 4))
        kinds.append(kind)
        todo[s] = jnp.where(kind == 0, code, 0)
        is_last = jnp.where(kind == 1, 1, 0)
        ranks.append(seen)
        picks = [
            jnp.where(is_last * jnp.where(seen == k, 1, 0) == 1, code, picks[k])
            for k in range(2)
        ]
        seen = seen + is_last
    for k in range(2):
        todo[slots + k] = picks[k]

    one = functools.partial(
        lax.dot_general,
        dimension_numbers=(((1,), (1,)), ((), ())),
        preferred_element_type=jnp.float32,
    )

    def product(code, lo, hi):
        lhs, rhs = lax.rem(code, 8), lax.rem(lax.div(code, 8), 8)
        deep = hi - lo

        def part(n):
            return parts[rhs, n, :, :, lo:hi].reshape(2 * rows, deep)

        both = one(parts[lhs, :, :, :, lo:hi].reshape(4 * rows, deep), part(0))
        return both[:2 * rows] + (
            both[2 * rows:]
            + one(parts[lhs, 0, :, :, lo:hi].reshape(2 * rows, deep), part(1))
        )

    def to_zfar(h):
        send("z", ("z", 1), block(4, core, h), zfar.at[pl.ds(h * half, half)])

    got(("x", 0, 0), block(1, core, 0))
    send("y", ("near", 3), block(1, core, 0), block(3, core, 0))
    got(("y", 0, 1), block(2, core, 1))
    send("x", ("near", 3), block(2, core, 1), block(3, core, 1))
    cross(1, 0, (1, 0))
    cross(2, 1, (2, 1))
    got(("z", 0, 0), block(4, core, 0))
    to_zfar(0)
    cross(4, 0, (4, 0))
    split(1, core, 0)
    split(2, core, 1)
    split(4, core, 0)
    both_crossed(0)
    crossed(1, 0, (1, 0))
    crossed(2, 1, (2, 1))
    crossed(4, 0, (4, 0))
    got(("x", 0, 1), block(1, core, 1))
    cross(1, 1, (1, 1))
    got(("y", 0, 0), block(2, core, 0))
    cross(2, 0, (2, 0))
    got(("z", 0, 1), block(4, core, 1))
    to_zfar(1)
    for h in (0, 1):
        send("x", ("next", h), block(4, core, h), block(5, core, h))
        send("y", ("next", h), block(4, core, h), block(6, core, h))
    cross(4, 1, (4, 1))
    split(1, core, 1)
    split(2, core, 0)
    split(4, core, 1)
    crossed(1, 1, (1, 1))
    crossed(2, 0, (2, 0))
    crossed(4, 1, (4, 1))
    got(("near", 3), gath.at[3, core])
    for c in (0, 1):
        send("z", ("z", 3, c), strip(3, core, c), strip(7, core, c))
    for h in (0, 1):
        cross(3, h, 3)
    split(3, core, 0)
    split(3, core, 1)
    both_crossed(3)

    def pair(side, h):
        return gath.at[pl.ds(5, 2), side, pl.ds(h * half, half)]

    def take_next(h):
        got(("next", h), pair(core, h))
        cross(5, h, ("next", h))
        cross(6, h, ("next", h))
        split(5, core, h)
        split(6, core, h)

    def twin_next(h):
        got(("cross", ("next", h)), pair(twin, h))
        split(5, twin, h)
        split(6, twin, h)

    take_next(0)
    twin_next(0)

    def split_far(h):
        part = slice(h * half, (h + 1) * half)
        value = zfar[part]
        hi = value.astype(jnp.bfloat16)
        far_parts[0, part] = hi
        far_parts[1, part] = (value - hi.astype(jnp.float32)).astype(jnp.bfloat16)

    def far_at(where, side, t):
        return far.at[where, side, t]

    def far_cross(where, t):
        send("c", ("far",), far_at(where, core, t), far_at(where, core, t))

    flag = jnp.where(x >= nx // 2, 1, 0)
    got(("z", 1), zfar)
    split_far(0)
    split_far(1)
    for t in (0, 1):
        col = flag + 2 * lax.rem(t + lax.div(chip, 2), 2)
        both = one(
            far_parts[...].reshape(2 * rows, width), parts[col, 0].reshape(2 * rows, width)
        )
        full = both[:rows] + (
            both[rows:] + one(far_parts[0], parts[col, 1].reshape(2 * rows, width))
        )
        for k in (0, 1):
            piece_k = full[:, k * rows:(k + 1) * rows]
            far[0, core, t, k] = jnp.where(flag == 0, piece_k, piece_k.T)
        if t == 0:
            send("x", ("fx", 0), far_at(0, core, 0), far_at(1, core, 0))
    send("y", ("fy", 1), far_at(0, core, 1), far_at(2, core, 1))
    send("x", ("fx", 1), far_at(0, core, 1), far_at(1, core, 1))
    send("y", ("fy", 0), far_at(0, core, 0), far_at(2, core, 0))
    for t in (0, 1):
        far_cross(0, t)

    take_next(1)
    twin_next(1)

    above = jnp.where(
        lax.broadcasted_iota(jnp.int32, (2 * rows, 2 * rows), 0)
        < lax.broadcasted_iota(jnp.int32, (2 * rows, 2 * rows), 1), 1, 0,
    )

    def local(s, carry):
        code = todo[s]
        masked = jnp.where(code >= 256, 1, 0)
        out_ref[s] = jnp.where(above * masked == 1, 0.0, product(code, 0, width))
        return carry

    def take_strip(c):
        got(("z", 3, c), strip(7, core, c))
        send("c", ("cross", (7, c)), strip(7, core, c), strip(7, core, c))
        split_strip(core, c)

    def twin_strip(c):
        got(("cross", (7, c)), strip(7, twin, c))
        split_strip(twin, c)

    def behind(k, carry):
        extra[k] = product(todo[slots + k], 0, cuts[1])
        return carry

    def behind_more(k, carry):
        extra[k] = extra[k] + product(todo[slots + k], cuts[1], width)
        return carry

    middle = slots // 2
    lax.fori_loop(0, middle, local, 0)
    got(("fx", 0), far_at(1, core, 0))
    send("y", ("far", 3), far_at(1, core, 0), far_at(3, core, 0))
    got(("fy", 1), far_at(2, core, 1))
    send("x", ("far", 3), far_at(2, core, 1), far_at(3, core, 1))
    far_cross(1, 0)
    far_cross(2, 1)
    take_strip(0)
    lax.fori_loop(middle, slots, local, 0)
    twin_strip(0)
    lax.fori_loop(0, 2, behind, 0)
    got(("fx", 1), far_at(1, core, 1))
    far_cross(1, 1)
    got(("fy", 0), far_at(2, core, 0))
    far_cross(2, 0)
    take_strip(1)
    got(("far", 3), far.at[3, core])
    far_cross(3, 0)
    far_cross(3, 1)
    twin_strip(1)
    lax.fori_loop(0, 2, behind_more, 0)
    got(("far",), far.at[:, twin])

    for s in range(slots):
        kind, code = kinds[s], jnp.maximum(codes[s], 0)
        where = lax.rem(code, 4)
        t = lax.rem(lax.div(code, 8), 2)
        rank = jnp.minimum(ranks[s], 1)
        for i in (0, 1):
            for j in (0, 1):
                side, k = jnp.where(flag == 0, i, j), jnp.where(flag == 0, j, i)
                at = (s, slice(i * rows, (i + 1) * rows), slice(j * rows, (j + 1) * rows))
                value = jnp.where(kind == 1, extra[rank, at[1], at[2]], out_ref[at])
                value = jnp.where(kind == 2, far[where, side, t, k], value)
                out_ref[at] = jnp.where(kind == 3, 0.0, value)
    for copy in flying.values():
        copy.wait_send()


def plane_call(dims, *arrays):
    nx, ny, half_tiles, slots = dims
    matrix_rows, tile_owner, tile_slot = arrays
    rows, width = matrix_rows.shape
    f32, bf16 = jnp.float32, jnp.bfloat16
    dma = pltpu.SemaphoreType.DMA
    hbm = pl.BlockSpec(memory_space=pltpu.HBM)
    return pl.pallas_call(
        functools.partial(plane_kernel, dims),
        out_shape=jax.ShapeDtypeStruct((slots, 2 * rows, 2 * rows), f32),
        in_specs=[hbm, hbm, hbm],
        out_specs=pl.BlockSpec(memory_space=pltpu.VMEM),
        scratch_shapes=[
            pltpu.VMEM((8, 2, rows, width), f32),
            pltpu.VMEM((rows, width), f32),
            pltpu.VMEM((8, 2, 2, rows, width), bf16),
            pltpu.VMEM((2, rows, width), bf16),
            pltpu.VMEM((4, 2, 2, 2, rows, rows), f32),
            pltpu.VMEM((2, 2 * rows, 2 * rows), f32),
            pltpu.SMEM(tile_owner.shape, jnp.int32),
            pltpu.SMEM(tile_slot.shape, jnp.int32),
            pltpu.SMEM((slots + 2,), jnp.int32),
            dma((4,)), dma((16,)), dma((30,)), pltpu.SemaphoreType.REGULAR((4,)),
        ],
        compiler_params=pltpu.CompilerParams(
            collective_id=0, has_side_effects=True,
            vmem_limit_bytes=44 * 1024 * 1024,
        ),
    )(*(pltpu.with_memory_space_constraint(a, pltpu.HBM) for a in arrays))


def copy_out(in_ref, out_ref, sem):
    copy = pltpu.make_async_copy(in_ref, out_ref, sem)
    copy.start()
    copy.wait()


def ring_call(mesh_shape, matrix_rows, tile_owner, tile_slot):
    nx, ny = mesh_shape
    rows, width = matrix_rows.shape
    half_tiles, half_x = ny // 2, nx // 2
    capacity = nx // 4 + 1
    slots = -(-tile_owner.shape[0] // (nx * ny))
    _, piece_count = piece_lists(half_tiles, half_x)
    reach = max(ny // 4, 1)
    f32, bf16 = jnp.float32, jnp.bfloat16
    dma = pltpu.SemaphoreType.DMA
    return pl.pallas_call(
        functools.partial(kernel, (nx, ny, half_tiles, half_x, capacity, slots)),
        out_shape=jax.ShapeDtypeStruct((slots, 2 * rows, 2 * rows), f32),
        in_specs=[
            pl.BlockSpec(memory_space=pltpu.VMEM),
            pl.BlockSpec(memory_space=pltpu.SMEM),
            pl.BlockSpec(memory_space=pltpu.SMEM),
        ],
        out_specs=pl.BlockSpec(memory_space=pltpu.VMEM),
        scratch_shapes=[
            pltpu.VMEM((ny, rows, width), f32),
            pltpu.VMEM((half_x, rows, width), f32),
            pltpu.VMEM((ny, rows, width), bf16),
            pltpu.VMEM((ny, rows, width), bf16),
            pltpu.VMEM((half_x + 1, 2, rows, width), bf16),
            pltpu.VMEM((2, piece_count, 2, rows // 2, rows), f32),
            pltpu.VMEM((2, ny, 2 * capacity, rows // 2, rows), f32),
            pltpu.VMEM((2, ny * 2 * capacity, rows // 2, rows), f32),
            pltpu.SMEM((piece_count,), jnp.int32),
            dma((reach, 2)), dma((reach, 2)), dma((reach, 2)), dma((reach, 2)),
            dma((2 * reach + 1, 2)), dma((2 * reach + 1, 2)),
            dma((half_x, 2)), dma((half_x, 2)),
            dma((2, ny)), dma((2, ny)),
        ],
        compiler_params=pltpu.CompilerParams(
            collective_id=0, has_side_effects=True, vmem_limit_bytes=44 * 1024 * 1024
        ),
    )(matrix_rows, tile_owner, tile_slot)


def per_device(mesh_shape, matrix_rows, tile_owner, tile_slot):
    nx, ny = mesh_shape
    if ny // 2 == 4 and nx == 4:
        slots = -(-tile_owner.shape[0] // (nx * ny))
        packed = plane_call((nx, ny, ny // 2, slots), matrix_rows, tile_owner, tile_slot)
    else:
        packed = ring_call(mesh_shape, matrix_rows, tile_owner, tile_slot)
    return pl.pallas_call(
        copy_out,
        out_shape=jax.ShapeDtypeStruct(packed.shape, packed.dtype),
        in_specs=[pl.BlockSpec(memory_space=pltpu.VMEM)],
        out_specs=pl.BlockSpec(memory_space=pl.ANY),
        scratch_shapes=[pltpu.SemaphoreType.DMA(())],
        compiler_params=pltpu.CompilerParams(vmem_limit_bytes=4 * 1024 * 1024),
    )(packed)


def solution(mesh):
    placed = (P(("gx", "gy"), None), P(), P())
    return jax.shard_map(
        functools.partial(per_device, (mesh.shape["gx"], mesh.shape["gy"])),
        mesh=mesh,
        in_specs=placed,
        out_specs=P(("gx", "gy"), None, None),
        check_vma=False,
    )
```

```python
import functools

import jax
import jax.numpy as jnp
from jax import lax
from jax.experimental import pallas as pl
from jax.experimental.pallas import tpu as pltpu
from jax.sharding import PartitionSpec as P

MESH = pl.DeviceIdType.MESH


def chip_position(chip, chips):
    row, col = lax.div(chip, 2), lax.rem(chip, 2)
    return col * (1 + row) + (1 - col) * lax.rem(chips - row, chips)


def chip_at(position, chips):
    behind = lax.rem(position + chips - 1, chips)
    far = lax.div(behind, chips // 2)
    return (1 - far) * (2 * behind + 1) + far * 2 * (chips - 1 - behind)


def piece_lists(half_tiles, half_x):
    lists, start = [], 0
    for step in range(half_x + 1):
        if step == 0:
            count = half_tiles // 2 + 1
        elif step < half_x:
            count = half_tiles
        else:
            count = half_tiles // 2
        lists.append((step, start, count))
        start += count
    return lists, start


def piece(x, r, step, i, nx, half_tiles, half_x):
    source = lax.rem(x - step + nx, nx)
    if step == 0:
        col = lax.rem(r - i + half_tiles, half_tiles)
        valid = jnp.logical_or(i < half_tiles // 2, r < half_tiles // 2)
        rowwise = col <= r
    elif step < half_x:
        col = i
        valid = i >= 0
        rowwise = source > x
    else:
        flag = jnp.where(x >= half_x, 1, 0)
        col = 2 * i + lax.rem(r + flag, 2)
        valid = i >= 0
        rowwise = source > x
    other, mine = source * half_tiles + r, x * half_tiles + col
    row_tile = jnp.where(rowwise, other, mine)
    col_tile = jnp.where(rowwise, mine, other)
    tile = jnp.where(valid, row_tile * (row_tile + 1) // 2 + col_tile, 0)
    return col, valid, rowwise, tile


def kernel(
    dims, rows_ref, owner_ref, slot_ref, out_ref,
    gath, zbuf, chi, clo, zsplit, pieces, outgoing, incoming, targets,
    gs_r, gr_r, gs_l, gr_l, ss, sr, zs, zr, xs, xr,
):
    nx, ny, half_tiles, half_x, capacity, slots = dims
    rows = rows_ref.shape[0]
    half = rows // 2
    chips = ny // 2
    reach = chips // 2
    x = lax.axis_index("gx")
    y = lax.axis_index("gy")
    core = lax.rem(y, 2)
    chip = lax.div(y, 2)
    right_x, left_x = lax.rem(x + 1, nx), lax.rem(x + nx - 1, nx)
    sibling = y + 1 - 2 * core
    place = chip_position(chip, chips)

    def at(position):
        return 2 * chip_at(lax.rem(position + chips, chips), chips) + core

    next_y, prev_y = at(place + 1), at(place - 1)
    lists, piece_count = piece_lists(half_tiles, half_x)

    barrier = pltpu.get_barrier_semaphore()
    for other in (right_x, left_x):
        pl.semaphore_signal(barrier, inc=1, device_id=(other, y), device_id_type=MESH)
    for offset in range(1, ny):
        pl.semaphore_signal(
            barrier, inc=1, device_id=(x, lax.rem(y + offset, ny)), device_id_type=MESH
        )
    pl.semaphore_wait(barrier, ny + 1)

    started = []

    def send(src, dst, send_sem, recv_sem, target):
        copy = pltpu.make_async_remote_copy(
            src_ref=src, dst_ref=dst, send_sem=send_sem, recv_sem=recv_sem,
            device_id=target, device_id_type=MESH,
        )
        copy.start()
        started.append(copy)

    def part(h):
        return pl.ds(h * half, half)

    def zcopy(step, h):
        src = rows_ref.at[part(h)] if step == 1 else zbuf.at[step - 2, part(h)]
        send(src, zbuf.at[step - 1, part(h)], zs.at[step - 1, h], zr.at[step - 1, h], (right_x, y))

    def block(owner, h):
        return gath.at[owner, part(h)]

    def ring(direction, distance, h):
        owner = at(place - direction * (distance - 1))
        src = rows_ref.at[part(h)] if distance == 1 else block(owner, h)
        s, r = (gs_r, gr_r) if direction == 1 else (gs_l, gr_l)
        target = next_y if direction == 1 else prev_y
        send(src, block(owner, h), s.at[distance - 1, h], r.at[distance - 1, h], (x, target))

    def cross(number, owner, h):
        src = rows_ref.at[part(h)] if number == 0 else block(owner, h)
        send(src, block(owner, h), ss.at[number, h], sr.at[number, h], (x, sibling))

    def halves_of(direction, distance):
        if distance < reach:
            return (0, 1) if direction == 1 else (1, 0)
        return (0,) if direction == 1 else (1,)

    def split(value, hi_ref, lo_ref, index):
        hi = value.astype(jnp.bfloat16)
        hi_ref[index] = hi
        lo_ref[index] = (value - hi.astype(jnp.float32)).astype(jnp.bfloat16)

    zcopy(1, 0)
    ring(1, 1, 0)
    if reach > 1:
        ring(-1, 1, 1)
        zcopy(1, 1)
        ring(1, 1, 1)
        ring(-1, 1, 0)
    else:
        ring(-1, 1, 1)
        zcopy(1, 1)
    cross(0, y, 0)
    cross(0, y, 1)

    for step, first, count in lists:
        def fill(i, carry, step=step, first=first):
            _, valid, _, tile = piece(x, chip, step, i, nx, half_tiles, half_x)
            targets[first + i] = jnp.where(valid, lax.rem(owner_ref[tile], ny), ny)
            return carry
        lax.fori_loop(0, count, fill, 0)

    me = x * ny + y

    def class_loop(r, carry):
        state = (jnp.int32(0),) + carry
        for step, first, count in lists:
            def look(i, state, step=step):
                seen, found = state[0], state[1:]
                _, valid, rowwise, tile = piece(x, r, step, i, nx, half_tiles, half_x)
                mine = jnp.where(valid, jnp.where(owner_ref[tile] == me, 1, 0), 0)
                slot = slot_ref[tile]
                code = 2 * (r * capacity + jnp.minimum(seen, capacity - 1))
                code = code + jnp.where(rowwise, 1, 0)
                key = jnp.where(mine == 1, slot, slots)
                found = tuple(jnp.where(key == s, code, found[s]) for s in range(slots))
                return (seen + mine,) + found
            state = lax.fori_loop(0, count, look, state)
        return state[1:]

    found = lax.fori_loop(0, half_tiles, class_loop, (jnp.int32(-1),) * slots)

    chosen = []
    for offset in range(ny):
        dest = lax.rem(y + offset, ny)

        def pick(p, state, dest=dest):
            hit = jnp.where(targets[p] == dest, 1, 0)
            seen = state[0]
            key = jnp.where(hit == 1, seen, capacity)
            picks = tuple(jnp.where(key == k, p, state[1 + k]) for k in range(capacity))
            return (seen + hit,) + picks

        chosen.append(lax.fori_loop(0, piece_count, pick, (jnp.int32(0),) * (capacity + 1))[1:])

    def wait_recv(dst, sem):
        pltpu.make_async_remote_copy(
            src_ref=dst, dst_ref=dst, send_sem=sem, recv_sem=sem,
            device_id=(x, sibling), device_id_type=MESH,
        ).wait_recv()

    def split_other(step, h):
        ref = rows_ref.at[part(h)] if step == 0 else zbuf.at[step - 1, part(h)]
        value = ref[...]
        hi = value.astype(jnp.bfloat16)
        zsplit[step, h, :half] = hi
        zsplit[step, h, half:] = (value - hi.astype(jnp.float32)).astype(jnp.bfloat16)

    def take_other(step, h):
        wait_recv(zbuf.at[step - 1, part(h)], zr.at[step - 1, h])
        if step < half_x:
            zcopy(step + 1, h)

    split_other(0, 0)
    split_other(0, 1)
    split(rows_ref[...], chi, clo, y)

    def take_cross(number, owner, halves):
        for h in halves:
            wait_recv(block(owner, h), sr.at[number, h])

    one = functools.partial(
        lax.dot_general,
        dimension_numbers=(((1,), (1,)), ((), ())),
        preferred_element_type=jnp.float32,
    )
    width = rows_ref.shape[1]
    row_inside = core * rows + lax.broadcasted_iota(jnp.int32, (half, 2 * rows), 0)
    col_inside = lax.broadcasted_iota(jnp.int32, (half, 2 * rows), 1)

    def one_piece_of(h):
        above = jnp.where(row_inside + h * half < col_inside, 1, 0)

        def one_piece(i, step, first, col):
            b_hi = chi[pl.ds(2 * col, 2)].reshape(2 * rows, width)
            b_lo = clo[pl.ds(2 * col, 2)].reshape(2 * rows, width)
            both = one(zsplit[step, h], b_hi)
            full = both[:half] + (both[half:] + one(zsplit[step, h, :half], b_lo))
            if step == 0:
                full = jnp.where(above * jnp.where(i == 0, 1, 0) == 1, 0.0, full)
            pieces[h, first + i, 0] = full[:, :rows]
            pieces[h, first + i, 1] = full[:, rows:]

        return one_piece

    farthest = chip_at(lax.rem(place + reach, chips), chips)
    soon = min(reach, half_x) if reach > 1 else 0

    def multiply(h, mode):
        one_piece = one_piece_of(h)
        for step, first, count in lists:
            if mode == "early" and step >= soon:
                continue

            def make(i, carry, step=step, first=first):
                col, _, _, _ = piece(x, chip, step, i, nx, half_tiles, half_x)
                if mode == "all" or step >= soon:
                    one_piece(i, step, first, col)
                else:
                    wanted = (col != farthest) if mode == "early" else (col == farthest)
                    pl.when(wanted)(lambda: one_piece(i, step, first, col))
                return carry
            lax.fori_loop(0, count, make, 0)

    pending = [(0, sibling, (0, 1))]
    for distance in range(1, reach + 1):
        if distance == reach:
            for number, owner, halves in pending[1:]:
                take_cross(number, owner, halves)
                split(gath[owner], chi, clo, owner)
            multiply(0, "early")
        if distance <= half_x:
            for h in (0, 1):
                if (distance, h) != (half_x, 1):
                    take_other(distance, h)
                if h in halves_of(1, distance):
                    owner = at(place - distance)
                    wait_recv(block(owner, h), gr_r.at[distance - 1, h])
                    if distance < reach and h in halves_of(1, distance + 1):
                        ring(1, distance + 1, h)
                    cross(2 * distance - 1, owner, h)
                g = 1 - h
                if g in halves_of(-1, distance):
                    owner = at(place + distance)
                    wait_recv(block(owner, g), gr_l.at[distance - 1, g])
                    if distance < reach and g in halves_of(-1, distance + 1):
                        ring(-1, distance + 1, g)
                    cross(2 * distance, owner, g)
            split_other(distance, 0)
            if distance < half_x:
                split_other(distance, 1)
        behind, ahead = at(place - distance), at(place + distance)
        pending.append((2 * distance - 1, behind + 1 - 2 * core, halves_of(1, distance)))
        pending.append((2 * distance, ahead + 1 - 2 * core, halves_of(-1, distance)))
        split(gath[behind], chi, clo, behind)
        if distance < reach:
            split(gath[ahead], chi, clo, ahead)
        for number, owner, halves in pending[: (1 if distance == 1 else 0)]:
            take_cross(number, owner, halves)
            split(gath[owner], chi, clo, owner)
    for number, owner, halves in pending[-2:]:
        take_cross(number, owner, halves)
    split(gath[pending[-1][1]], chi, clo, pending[-1][1])
    for step in range(reach + 1, half_x + 1):
        for h in (0, 1):
            if (step, h) != (half_x, 1):
                take_other(step, h)
                split_other(step, h)

    def arrival(offset):
        return pl.ds(offset * capacity * 2, capacity * 2)

    def exchange(h, offset):
        send(
            outgoing.at[h, offset], incoming.at[h, arrival(offset)],
            xs.at[h, offset], xr.at[h, offset], (x, lax.rem(y + offset, ny)),
        )

    for h in (0, 1):
        if h == 1:
            take_other(half_x, 1)
            split_other(half_x, 1)
        multiply(h, "all" if h == 1 else "late")
        for offset in range(1, ny):
            for k in range(capacity):
                outgoing[h, offset, 2 * k:2 * k + 2] = pieces[h, chosen[offset][k]]
            if offset > 1:
                exchange(h, offset - 1)
        for k in range(capacity):
            incoming[h, 2 * k:2 * k + 2] = pieces[h, chosen[0][k]]
        exchange(h, ny - 1)
    for h in (0, 1):
        for offset in range(1, ny):
            wait_recv(incoming.at[h, arrival(offset)], xr.at[h, offset])

    for s in range(slots):
        code = found[s]
        there = code >= 0
        safe = jnp.maximum(code, 0)
        rowwise = lax.rem(safe, 2) == 1
        rank = lax.rem(safe // 2, capacity)
        first_source = 2 * (safe // (2 * capacity))
        bases = [
            (lax.rem(y - first_source - h + ny, ny) * capacity + rank) * 2 for h in (0, 1)
        ]
        for i in (0, 1):
            for j in (0, 1):
                place_of = jnp.where(rowwise, bases[i] + j, bases[j] + i)
                value = jnp.concatenate([incoming[0, place_of], incoming[1, place_of]], axis=0)
                value = jnp.where(rowwise, value, value.T)
                out_ref[s, i * rows:(i + 1) * rows, j * rows:(j + 1) * rows] = jnp.where(
                    there, value, 0.0
                )
    for copy in started:
        copy.wait_send()


def plane_kernel(
    dims, rows_hbm, owner_hbm, slot_hbm, out_ref,
    gath, zfar, parts, far_parts, far, extra, owner_ref, slot_ref, todo,
    ins, ss, rs, entered,
):
    nx, ny, half_tiles, slots = dims
    rows, width = zfar.shape
    half = rows // 2
    cuts = (0, width // 2, width)
    x = lax.axis_index("gx")
    y = lax.axis_index("gy")
    core = lax.rem(y, 2)
    chip = lax.div(y, 2)
    twin = 1 - core
    right, left = (lax.rem(x + 1, nx), y), (lax.rem(x + nx - 1, nx), y)
    sibling = (x, y + 1 - 2 * core)
    across = (x, y + 2 - 4 * lax.rem(chip, 2))
    along = (x, lax.rem(y + 4, ny))

    odd, high, ends = lax.rem(chip, 2), lax.div(chip, 2), jnp.where(x == nx - 1, 1, 0)
    earlier = (1 - core, odd, high, jnp.where(x > 0, 1, 0))
    later = (core, 1 - odd, 1 - high, 1 - ends)
    barrier = pltpu.get_barrier_semaphore()

    def signal_if(flag, semaphore, target):
        @pl.when(flag == 1)
        def _():
            pl.semaphore_signal(semaphore, inc=1, device_id=target, device_id_type=MESH)

    for flag, target in zip(later, (sibling, across, along, right)):
        signal_if(flag, barrier, target)
    signal_if(jnp.where(x == 0, 1, 0), barrier, left)
    loads = [
        pltpu.make_async_copy(
            rows_hbm.at[pl.ds(h * half, half)], gath.at[0, core, pl.ds(h * half, half)],
            ins.at[h],
        )
        for h in (0, 1)
    ] + [
        pltpu.make_async_copy(owner_hbm, owner_ref, ins.at[2]),
        pltpu.make_async_copy(slot_hbm, slot_ref, ins.at[3]),
    ]
    for copy in loads:
        copy.start()
    expected = sum(earlier) + ends

    @pl.when(expected > 0)
    def _():
        pl.semaphore_wait(barrier, expected)

    for n, target in enumerate((sibling, across, along, left)):
        signal_if(earlier[n], entered.at[n], target)

    numbers, flying, issued = {}, {}, {}
    ways = {"x": (across, 0), "y": (along, 4), "z": (right, 8), "c": (sibling, 12)}

    def number(name):
        return numbers.setdefault(name, len(numbers))

    def ready(way, name, src, dst, other=None):
        target, base = ways[way]
        turn = issued.get(way, 0)
        issued[way] = turn + 1
        i, j = number(name), base + turn % 4
        if j in flying:
            flying[j].wait_send()
        copy = pltpu.make_async_remote_copy(
            src_ref=src, dst_ref=dst, send_sem=ss.at[j], recv_sem=rs.at[i],
            device_id=target, device_id_type=MESH,
        )
        flying[j] = copy
        if other is None:
            return copy
        return copy, pltpu.make_async_remote_copy(
            src_ref=other, dst_ref=dst, send_sem=ss.at[j], recv_sem=rs.at[i],
            device_id=target, device_id_type=MESH,
        )

    def send(*args):
        ready(*args).start()

    def got(name, dst):
        i = number(name)
        pltpu.make_async_remote_copy(
            src_ref=dst, dst_ref=dst, send_sem=rs.at[i], recv_sem=rs.at[i],
            device_id=sibling, device_id_type=MESH,
        ).wait_recv()

    def block(where, side, h):
        return gath.at[where, side, pl.ds(h * half, half)]

    def cross(where, h, name):
        send("c", ("cross", name), block(where, core, h), block(where, core, h))

    def crossed(where, h, name):
        got(("cross", name), block(where, twin, h))
        split(where, twin, h)

    def both_crossed(where):
        got(("cross", where), gath.at[where, twin])
        split(where, twin, 0)
        split(where, twin, 1)

    def strip(where, side, c):
        return gath.at[where, side, :, pl.ds(cuts[c], cuts[c + 1] - cuts[c])]

    def split_at(where, side, part):
        value = gath[where, side, part[0], part[1]]
        hi = value.astype(jnp.bfloat16)
        parts[where, 0, side, part[0], part[1]] = hi
        parts[where, 1, side, part[0], part[1]] = (
            value - hi.astype(jnp.float32)
        ).astype(jnp.bfloat16)

    def split(where, side, h):
        split_at(where, side, (slice(h * half, (h + 1) * half), slice(None)))

    def split_strip(side, c):
        split_at(7, side, (slice(None), slice(cuts[c], cuts[c + 1])))

    own = [rows_hbm.at[pl.ds(h * half, half)] for h in (0, 1)]
    first = [
        [ready("x", ("x", 0, h), block(0, core, h), block(1, core, h), own[h]) for h in (0, 1)],
        [ready("y", ("y", 0, h), block(0, core, h), block(2, core, h), own[h]) for h in (1, 0)],
        [ready("z", ("z", 0, h), block(0, core, h), block(4, core, h), own[h]) for h in (0, 1)],
    ]

    def open_way(n, early):
        @pl.when(later[n] == (0 if early else 1))
        def _():
            if not early:
                pl.semaphore_wait(entered.at[n], 1)
            for copies in first[n - 1]:
                copies[1 if early else 0].start()

    for n in (1, 2, 3):
        open_way(n, True)
    loads[0].wait()
    loads[1].wait()
    for n in (1, 2):
        open_way(n, False)

    @pl.when(later[0] == 1)
    def _():
        pl.semaphore_wait(entered.at[0], 1)

    for h in (0, 1):
        cross(0, h, 0)
    for h in (0, 1):
        split(0, core, h)
    open_way(3, False)
    for copy in loads[2:]:
        copy.wait()

    me = x * ny + y

    def look(tile, state):
        i_tile, j_tile = state[0], state[1]
        a, i = lax.div(i_tile, half_tiles), lax.rem(i_tile, half_tiles)
        b, j = lax.div(j_tile, half_tiles), lax.rem(j_tile, half_tiles)
        i_chip, j_chip = jnp.bitwise_xor(i, chip), jnp.bitwise_xor(j, chip)
        i_near, j_near = jnp.where(a == x, 0, half_tiles), jnp.where(b == x, 0, half_tiles)
        same = jnp.where(i_tile == j_tile, 256, 0)
        last = jnp.where((i_near + i_chip == 7) | (j_near + j_chip == 7), 64, 0)
        near = i_near + i_chip + 8 * (j_near + j_chip) + same + last
        far_code = 128 + jnp.where(
            a == x, j_chip + 8 * lax.div(i, 2), i_chip + 8 * lax.div(j, 2)
        )
        code = jnp.where(a - b == nx // 2, far_code, near)
        key = jnp.where(owner_ref[tile] == me, slot_ref[tile], slots)
        found = tuple(jnp.where(key == s, code, state[2 + s]) for s in range(slots))
        wrap = j_tile == i_tile
        return (
            jnp.where(wrap, i_tile + 1, i_tile), jnp.where(wrap, 0, j_tile + 1)
        ) + found

    codes = lax.fori_loop(
        0, owner_ref.shape[0], look, (jnp.int32(0),) * 2 + (jnp.int32(-1),) * slots
    )[2:]
    seen, picks, ranks = jnp.int32(0), [jnp.int32(0)] * 2, []
    kinds = []
    for s in range(slots):
        code = codes[s]
        kind = jnp.where(code < 0, 3, lax.rem(lax.div(code, 64), 4))
        kinds.append(kind)
        todo[s] = jnp.where(kind == 0, code, 0)
        is_last = jnp.where(kind == 1, 1, 0)
        ranks.append(seen)
        picks = [
            jnp.where(is_last * jnp.where(seen == k, 1, 0) == 1, code, picks[k])
            for k in range(2)
        ]
        seen = seen + is_last
    for k in range(2):
        todo[slots + k] = picks[k]

    one = functools.partial(
        lax.dot_general,
        dimension_numbers=(((1,), (1,)), ((), ())),
        preferred_element_type=jnp.float32,
    )

    def product(code, lo, hi):
        lhs, rhs = lax.rem(code, 8), lax.rem(lax.div(code, 8), 8)
        deep = hi - lo

        def part(n):
            return parts[rhs, n, :, :, lo:hi].reshape(2 * rows, deep)

        both = one(parts[lhs, :, :, :, lo:hi].reshape(4 * rows, deep), part(0))
        return both[:2 * rows] + (
            both[2 * rows:]
            + one(parts[lhs, 0, :, :, lo:hi].reshape(2 * rows, deep), part(1))
        )

    def to_zfar(h):
        send("z", ("z", 1), block(4, core, h), zfar.at[pl.ds(h * half, half)])

    got(("x", 0, 0), block(1, core, 0))
    send("y", ("near", 3), block(1, core, 0), block(3, core, 0))
    got(("y", 0, 1), block(2, core, 1))
    send("x", ("near", 3), block(2, core, 1), block(3, core, 1))
    cross(1, 0, (1, 0))
    cross(2, 1, (2, 1))
    got(("z", 0, 0), block(4, core, 0))
    to_zfar(0)
    cross(4, 0, (4, 0))
    split(1, core, 0)
    split(2, core, 1)
    split(4, core, 0)
    both_crossed(0)
    crossed(1, 0, (1, 0))
    crossed(2, 1, (2, 1))
    crossed(4, 0, (4, 0))
    got(("x", 0, 1), block(1, core, 1))
    cross(1, 1, (1, 1))
    got(("y", 0, 0), block(2, core, 0))
    cross(2, 0, (2, 0))
    got(("z", 0, 1), block(4, core, 1))
    to_zfar(1)
    for h in (0, 1):
        send("x", ("next", h), block(4, core, h), block(5, core, h))
        send("y", ("next", h), block(4, core, h), block(6, core, h))
    cross(4, 1, (4, 1))
    split(1, core, 1)
    split(2, core, 0)
    split(4, core, 1)
    crossed(1, 1, (1, 1))
    crossed(2, 0, (2, 0))
    crossed(4, 1, (4, 1))
    got(("near", 3), gath.at[3, core])
    for c in (0, 1):
        send("z", ("z", 3, c), strip(3, core, c), strip(7, core, c))
    for h in (0, 1):
        cross(3, h, 3)
    split(3, core, 0)
    split(3, core, 1)
    both_crossed(3)

    def pair(side, h):
        return gath.at[pl.ds(5, 2), side, pl.ds(h * half, half)]

    def take_next(h):
        got(("next", h), pair(core, h))
        cross(5, h, ("next", h))
        cross(6, h, ("next", h))
        split(5, core, h)
        split(6, core, h)

    def twin_next(h):
        got(("cross", ("next", h)), pair(twin, h))
        split(5, twin, h)
        split(6, twin, h)

    take_next(0)
    twin_next(0)

    def split_far(h):
        part = slice(h * half, (h + 1) * half)
        value = zfar[part]
        hi = value.astype(jnp.bfloat16)
        far_parts[0, part] = hi
        far_parts[1, part] = (value - hi.astype(jnp.float32)).astype(jnp.bfloat16)

    def far_at(where, side, t):
        return far.at[where, side, t]

    def far_cross(where, t):
        send("c", ("far",), far_at(where, core, t), far_at(where, core, t))

    flag = jnp.where(x >= nx // 2, 1, 0)
    got(("z", 1), zfar)
    split_far(0)
    split_far(1)
    for t in (0, 1):
        col = flag + 2 * lax.rem(t + lax.div(chip, 2), 2)
        both = one(
            far_parts[...].reshape(2 * rows, width), parts[col, 0].reshape(2 * rows, width)
        )
        full = both[:rows] + (
            both[rows:] + one(far_parts[0], parts[col, 1].reshape(2 * rows, width))
        )
        for k in (0, 1):
            piece_k = full[:, k * rows:(k + 1) * rows]
            far[0, core, t, k] = jnp.where(flag == 0, piece_k, piece_k.T)
        if t == 0:
            send("x", ("fx", 0), far_at(0, core, 0), far_at(1, core, 0))
    send("y", ("fy", 1), far_at(0, core, 1), far_at(2, core, 1))
    send("x", ("fx", 1), far_at(0, core, 1), far_at(1, core, 1))
    send("y", ("fy", 0), far_at(0, core, 0), far_at(2, core, 0))
    for t in (0, 1):
        far_cross(0, t)

    take_next(1)
    twin_next(1)

    above = jnp.where(
        lax.broadcasted_iota(jnp.int32, (2 * rows, 2 * rows), 0)
        < lax.broadcasted_iota(jnp.int32, (2 * rows, 2 * rows), 1), 1, 0,
    )

    def local(s, carry):
        code = todo[s]
        masked = jnp.where(code >= 256, 1, 0)
        out_ref[s] = jnp.where(above * masked == 1, 0.0, product(code, 0, width))
        return carry

    def take_strip(c):
        got(("z", 3, c), strip(7, core, c))
        send("c", ("cross", (7, c)), strip(7, core, c), strip(7, core, c))
        split_strip(core, c)

    def twin_strip(c):
        got(("cross", (7, c)), strip(7, twin, c))
        split_strip(twin, c)

    def behind(k, carry):
        extra[k] = product(todo[slots + k], 0, cuts[1])
        return carry

    def behind_more(k, carry):
        extra[k] = extra[k] + product(todo[slots + k], cuts[1], width)
        return carry

    middle = slots // 2
    lax.fori_loop(0, middle, local, 0)
    got(("fx", 0), far_at(1, core, 0))
    send("y", ("far", 3), far_at(1, core, 0), far_at(3, core, 0))
    got(("fy", 1), far_at(2, core, 1))
    send("x", ("far", 3), far_at(2, core, 1), far_at(3, core, 1))
    far_cross(1, 0)
    far_cross(2, 1)
    take_strip(0)
    lax.fori_loop(middle, slots, local, 0)
    twin_strip(0)
    lax.fori_loop(0, 2, behind, 0)
    got(("fx", 1), far_at(1, core, 1))
    far_cross(1, 1)
    got(("fy", 0), far_at(2, core, 0))
    far_cross(2, 0)
    take_strip(1)
    got(("far", 3), far.at[3, core])
    far_cross(3, 0)
    far_cross(3, 1)
    twin_strip(1)
    lax.fori_loop(0, 2, behind_more, 0)
    got(("far",), far.at[:, twin])

    for s in range(slots):
        kind, code = kinds[s], jnp.maximum(codes[s], 0)
        where = lax.rem(code, 4)
        t = lax.rem(lax.div(code, 8), 2)
        rank = jnp.minimum(ranks[s], 1)
        for i in (0, 1):
            for j in (0, 1):
                side, k = jnp.where(flag == 0, i, j), jnp.where(flag == 0, j, i)
                at = (s, slice(i * rows, (i + 1) * rows), slice(j * rows, (j + 1) * rows))
                value = jnp.where(kind == 1, extra[rank, at[1], at[2]], out_ref[at])
                value = jnp.where(kind == 2, far[where, side, t, k], value)
                out_ref[at] = jnp.where(kind == 3, 0.0, value)
    for copy in flying.values():
        copy.wait_send()


def plane_call(dims, *arrays):
    nx, ny, half_tiles, slots = dims
    matrix_rows, tile_owner, tile_slot = arrays
    rows, width = matrix_rows.shape
    f32, bf16 = jnp.float32, jnp.bfloat16
    dma = pltpu.SemaphoreType.DMA
    hbm = pl.BlockSpec(memory_space=pltpu.HBM)
    return pl.pallas_call(
        functools.partial(plane_kernel, dims),
        out_shape=jax.ShapeDtypeStruct((slots, 2 * rows, 2 * rows), f32),
        in_specs=[hbm, hbm, hbm],
        out_specs=pl.BlockSpec(memory_space=pltpu.VMEM),
        scratch_shapes=[
            pltpu.VMEM((8, 2, rows, width), f32),
            pltpu.VMEM((rows, width), f32),
            pltpu.VMEM((8, 2, 2, rows, width), bf16),
            pltpu.VMEM((2, rows, width), bf16),
            pltpu.VMEM((4, 2, 2, 2, rows, rows), f32),
            pltpu.VMEM((2, 2 * rows, 2 * rows), f32),
            pltpu.SMEM(tile_owner.shape, jnp.int32),
            pltpu.SMEM(tile_slot.shape, jnp.int32),
            pltpu.SMEM((slots + 2,), jnp.int32),
            dma((4,)), dma((16,)), dma((30,)), pltpu.SemaphoreType.REGULAR((4,)),
        ],
        compiler_params=pltpu.CompilerParams(
            collective_id=0, has_side_effects=True,
            vmem_limit_bytes=44 * 1024 * 1024,
        ),
    )(*(pltpu.with_memory_space_constraint(a, pltpu.HBM) for a in arrays))


def copy_out(in_ref, out_ref, sem):
    copy = pltpu.make_async_copy(in_ref, out_ref, sem)
    copy.start()
    copy.wait()


def ring_call(mesh_shape, matrix_rows, tile_owner, tile_slot):
    nx, ny = mesh_shape
    rows, width = matrix_rows.shape
    half_tiles, half_x = ny // 2, nx // 2
    capacity = nx // 4 + 1
    slots = -(-tile_owner.shape[0] // (nx * ny))
    _, piece_count = piece_lists(half_tiles, half_x)
    reach = max(ny // 4, 1)
    f32, bf16 = jnp.float32, jnp.bfloat16
    dma = pltpu.SemaphoreType.DMA
    return pl.pallas_call(
        functools.partial(kernel, (nx, ny, half_tiles, half_x, capacity, slots)),
        out_shape=jax.ShapeDtypeStruct((slots, 2 * rows, 2 * rows), f32),
        in_specs=[
            pl.BlockSpec(memory_space=pltpu.VMEM),
            pl.BlockSpec(memory_space=pltpu.SMEM),
            pl.BlockSpec(memory_space=pltpu.SMEM),
        ],
        out_specs=pl.BlockSpec(memory_space=pltpu.VMEM),
        scratch_shapes=[
            pltpu.VMEM((ny, rows, width), f32),
            pltpu.VMEM((half_x, rows, width), f32),
            pltpu.VMEM((ny, rows, width), bf16),
            pltpu.VMEM((ny, rows, width), bf16),
            pltpu.VMEM((half_x + 1, 2, rows, width), bf16),
            pltpu.VMEM((2, piece_count, 2, rows // 2, rows), f32),
            pltpu.VMEM((2, ny, 2 * capacity, rows // 2, rows), f32),
            pltpu.VMEM((2, ny * 2 * capacity, rows // 2, rows), f32),
            pltpu.SMEM((piece_count,), jnp.int32),
            dma((reach, 2)), dma((reach, 2)), dma((reach, 2)), dma((reach, 2)),
            dma((2 * reach + 1, 2)), dma((2 * reach + 1, 2)),
            dma((half_x, 2)), dma((half_x, 2)),
            dma((2, ny)), dma((2, ny)),
        ],
        compiler_params=pltpu.CompilerParams(
            collective_id=0, has_side_effects=True, vmem_limit_bytes=44 * 1024 * 1024
        ),
    )(matrix_rows, tile_owner, tile_slot)


def per_device(mesh_shape, matrix_rows, tile_owner, tile_slot):
    nx, ny = mesh_shape
    if ny // 2 == 4 and nx == 4:
        slots = -(-tile_owner.shape[0] // (nx * ny))
        packed = plane_call((nx, ny, ny // 2, slots), matrix_rows, tile_owner, tile_slot)
    else:
        packed = ring_call(mesh_shape, matrix_rows, tile_owner, tile_slot)
    return pl.pallas_call(
        copy_out,
        out_shape=jax.ShapeDtypeStruct(packed.shape, packed.dtype),
        in_specs=[pl.BlockSpec(memory_space=pltpu.VMEM)],
        out_specs=pl.BlockSpec(memory_space=pl.ANY),
        scratch_shapes=[pltpu.SemaphoreType.DMA(())],
        compiler_params=pltpu.CompilerParams(vmem_limit_bytes=4 * 1024 * 1024),
    )(packed)


def solution(mesh):
    placed = (P(("gx", "gy"), None), P(), P())
    return jax.shard_map(
        functools.partial(per_device, (mesh.shape["gx"], mesh.shape["gy"])),
        mesh=mesh,
        in_specs=placed,
        out_specs=P(("gx", "gy"), None, None),
        check_vma=False,
    )
```

```python
import functools

import jax
import jax.numpy as jnp
from jax import lax
from jax.experimental import pallas as pl
from jax.experimental.pallas import tpu as pltpu
from jax.sharding import PartitionSpec as P

MESH = pl.DeviceIdType.MESH


def chip_position(chip, chips):
    row, col = lax.div(chip, 2), lax.rem(chip, 2)
    return col * (1 + row) + (1 - col) * lax.rem(chips - row, chips)


def chip_at(position, chips):
    behind = lax.rem(position + chips - 1, chips)
    far = lax.div(behind, chips // 2)
    return (1 - far) * (2 * behind + 1) + far * 2 * (chips - 1 - behind)


def piece_lists(half_tiles, half_x):
    lists, start = [], 0
    for step in range(half_x + 1):
        if step == 0:
            count = half_tiles // 2 + 1
        elif step < half_x:
            count = half_tiles
        else:
            count = half_tiles // 2
        lists.append((step, start, count))
        start += count
    return lists, start


def piece(x, r, step, i, nx, half_tiles, half_x):
    source = lax.rem(x - step + nx, nx)
    if step == 0:
        col = lax.rem(r - i + half_tiles, half_tiles)
        valid = jnp.logical_or(i < half_tiles // 2, r < half_tiles // 2)
        rowwise = col <= r
    elif step < half_x:
        col = i
        valid = i >= 0
        rowwise = source > x
    else:
        flag = jnp.where(x >= half_x, 1, 0)
        col = 2 * i + lax.rem(r + flag, 2)
        valid = i >= 0
        rowwise = source > x
    other, mine = source * half_tiles + r, x * half_tiles + col
    row_tile = jnp.where(rowwise, other, mine)
    col_tile = jnp.where(rowwise, mine, other)
    tile = jnp.where(valid, row_tile * (row_tile + 1) // 2 + col_tile, 0)
    return col, valid, rowwise, tile


def kernel(
    dims, rows_ref, owner_ref, slot_ref, out_ref,
    gath, zbuf, chi, clo, zsplit, pieces, outgoing, incoming, targets,
    gs_r, gr_r, gs_l, gr_l, ss, sr, zs, zr, xs, xr,
):
    nx, ny, half_tiles, half_x, capacity, slots = dims
    rows = rows_ref.shape[0]
    half = rows // 2
    chips = ny // 2
    reach = chips // 2
    x = lax.axis_index("gx")
    y = lax.axis_index("gy")
    core = lax.rem(y, 2)
    chip = lax.div(y, 2)
    right_x, left_x = lax.rem(x + 1, nx), lax.rem(x + nx - 1, nx)
    sibling = y + 1 - 2 * core
    place = chip_position(chip, chips)

    def at(position):
        return 2 * chip_at(lax.rem(position + chips, chips), chips) + core

    next_y, prev_y = at(place + 1), at(place - 1)
    lists, piece_count = piece_lists(half_tiles, half_x)

    barrier = pltpu.get_barrier_semaphore()
    for other in (right_x, left_x):
        pl.semaphore_signal(barrier, inc=1, device_id=(other, y), device_id_type=MESH)
    for offset in range(1, ny):
        pl.semaphore_signal(
            barrier, inc=1, device_id=(x, lax.rem(y + offset, ny)), device_id_type=MESH
        )
    pl.semaphore_wait(barrier, ny + 1)

    started = []

    def send(src, dst, send_sem, recv_sem, target):
        copy = pltpu.make_async_remote_copy(
            src_ref=src, dst_ref=dst, send_sem=send_sem, recv_sem=recv_sem,
            device_id=target, device_id_type=MESH,
        )
        copy.start()
        started.append(copy)

    def part(h):
        return pl.ds(h * half, half)

    def zcopy(step, h):
        src = rows_ref.at[part(h)] if step == 1 else zbuf.at[step - 2, part(h)]
        send(src, zbuf.at[step - 1, part(h)], zs.at[step - 1, h], zr.at[step - 1, h], (right_x, y))

    def block(owner, h):
        return gath.at[owner, part(h)]

    def ring(direction, distance, h):
        owner = at(place - direction * (distance - 1))
        src = rows_ref.at[part(h)] if distance == 1 else block(owner, h)
        s, r = (gs_r, gr_r) if direction == 1 else (gs_l, gr_l)
        target = next_y if direction == 1 else prev_y
        send(src, block(owner, h), s.at[distance - 1, h], r.at[distance - 1, h], (x, target))

    def cross(number, owner, h):
        src = rows_ref.at[part(h)] if number == 0 else block(owner, h)
        send(src, block(owner, h), ss.at[number, h], sr.at[number, h], (x, sibling))

    def halves_of(direction, distance):
        if distance < reach:
            return (0, 1) if direction == 1 else (1, 0)
        return (0,) if direction == 1 else (1,)

    def split(value, hi_ref, lo_ref, index):
        hi = value.astype(jnp.bfloat16)
        hi_ref[index] = hi
        lo_ref[index] = (value - hi.astype(jnp.float32)).astype(jnp.bfloat16)

    zcopy(1, 0)
    ring(1, 1, 0)
    if reach > 1:
        ring(-1, 1, 1)
        zcopy(1, 1)
        ring(1, 1, 1)
        ring(-1, 1, 0)
    else:
        ring(-1, 1, 1)
        zcopy(1, 1)
    cross(0, y, 0)
    cross(0, y, 1)

    for step, first, count in lists:
        def fill(i, carry, step=step, first=first):
            _, valid, _, tile = piece(x, chip, step, i, nx, half_tiles, half_x)
            targets[first + i] = jnp.where(valid, lax.rem(owner_ref[tile], ny), ny)
            return carry
        lax.fori_loop(0, count, fill, 0)

    me = x * ny + y

    def class_loop(r, carry):
        state = (jnp.int32(0),) + carry
        for step, first, count in lists:
            def look(i, state, step=step):
                seen, found = state[0], state[1:]
                _, valid, rowwise, tile = piece(x, r, step, i, nx, half_tiles, half_x)
                mine = jnp.where(valid, jnp.where(owner_ref[tile] == me, 1, 0), 0)
                slot = slot_ref[tile]
                code = 2 * (r * capacity + jnp.minimum(seen, capacity - 1))
                code = code + jnp.where(rowwise, 1, 0)
                key = jnp.where(mine == 1, slot, slots)
                found = tuple(jnp.where(key == s, code, found[s]) for s in range(slots))
                return (seen + mine,) + found
            state = lax.fori_loop(0, count, look, state)
        return state[1:]

    found = lax.fori_loop(0, half_tiles, class_loop, (jnp.int32(-1),) * slots)

    chosen = []
    for offset in range(ny):
        dest = lax.rem(y + offset, ny)

        def pick(p, state, dest=dest):
            hit = jnp.where(targets[p] == dest, 1, 0)
            seen = state[0]
            key = jnp.where(hit == 1, seen, capacity)
            picks = tuple(jnp.where(key == k, p, state[1 + k]) for k in range(capacity))
            return (seen + hit,) + picks

        chosen.append(lax.fori_loop(0, piece_count, pick, (jnp.int32(0),) * (capacity + 1))[1:])

    def wait_recv(dst, sem):
        pltpu.make_async_remote_copy(
            src_ref=dst, dst_ref=dst, send_sem=sem, recv_sem=sem,
            device_id=(x, sibling), device_id_type=MESH,
        ).wait_recv()

    def split_other(step, h):
        ref = rows_ref.at[part(h)] if step == 0 else zbuf.at[step - 1, part(h)]
        value = ref[...]
        hi = value.astype(jnp.bfloat16)
        zsplit[step, h, :half] = hi
        zsplit[step, h, half:] = (value - hi.astype(jnp.float32)).astype(jnp.bfloat16)

    def take_other(step, h):
        wait_recv(zbuf.at[step - 1, part(h)], zr.at[step - 1, h])
        if step < half_x:
            zcopy(step + 1, h)

    split_other(0, 0)
    split_other(0, 1)
    split(rows_ref[...], chi, clo, y)

    def take_cross(number, owner, halves):
        for h in halves:
            wait_recv(block(owner, h), sr.at[number, h])

    one = functools.partial(
        lax.dot_general,
        dimension_numbers=(((1,), (1,)), ((), ())),
        preferred_element_type=jnp.float32,
    )
    width = rows_ref.shape[1]
    row_inside = core * rows + lax.broadcasted_iota(jnp.int32, (half, 2 * rows), 0)
    col_inside = lax.broadcasted_iota(jnp.int32, (half, 2 * rows), 1)

    def one_piece_of(h):
        above = jnp.where(row_inside + h * half < col_inside, 1, 0)

        def one_piece(i, step, first, col):
            b_hi = chi[pl.ds(2 * col, 2)].reshape(2 * rows, width)
            b_lo = clo[pl.ds(2 * col, 2)].reshape(2 * rows, width)
            both = one(zsplit[step, h], b_hi)
            full = both[:half] + (both[half:] + one(zsplit[step, h, :half], b_lo))
            if step == 0:
                full = jnp.where(above * jnp.where(i == 0, 1, 0) == 1, 0.0, full)
            pieces[h, first + i, 0] = full[:, :rows]
            pieces[h, first + i, 1] = full[:, rows:]

        return one_piece

    farthest = chip_at(lax.rem(place + reach, chips), chips)
    soon = min(reach, half_x) if reach > 1 else 0

    def multiply(h, mode):
        one_piece = one_piece_of(h)
        for step, first, count in lists:
            if mode == "early" and step >= soon:
                continue

            def make(i, carry, step=step, first=first):
                col, _, _, _ = piece(x, chip, step, i, nx, half_tiles, half_x)
                if mode == "all" or step >= soon:
                    one_piece(i, step, first, col)
                else:
                    wanted = (col != farthest) if mode == "early" else (col == farthest)
                    pl.when(wanted)(lambda: one_piece(i, step, first, col))
                return carry
            lax.fori_loop(0, count, make, 0)

    pending = [(0, sibling, (0, 1))]
    for distance in range(1, reach + 1):
        if distance == reach:
            for number, owner, halves in pending[1:]:
                take_cross(number, owner, halves)
                split(gath[owner], chi, clo, owner)
            multiply(0, "early")
        if distance <= half_x:
            for h in (0, 1):
                if (distance, h) != (half_x, 1):
                    take_other(distance, h)
                if h in halves_of(1, distance):
                    owner = at(place - distance)
                    wait_recv(block(owner, h), gr_r.at[distance - 1, h])
                    if distance < reach and h in halves_of(1, distance + 1):
                        ring(1, distance + 1, h)
                    cross(2 * distance - 1, owner, h)
                g = 1 - h
                if g in halves_of(-1, distance):
                    owner = at(place + distance)
                    wait_recv(block(owner, g), gr_l.at[distance - 1, g])
                    if distance < reach and g in halves_of(-1, distance + 1):
                        ring(-1, distance + 1, g)
                    cross(2 * distance, owner, g)
            split_other(distance, 0)
            if distance < half_x:
                split_other(distance, 1)
        behind, ahead = at(place - distance), at(place + distance)
        pending.append((2 * distance - 1, behind + 1 - 2 * core, halves_of(1, distance)))
        pending.append((2 * distance, ahead + 1 - 2 * core, halves_of(-1, distance)))
        split(gath[behind], chi, clo, behind)
        if distance < reach:
            split(gath[ahead], chi, clo, ahead)
        for number, owner, halves in pending[: (1 if distance == 1 else 0)]:
            take_cross(number, owner, halves)
            split(gath[owner], chi, clo, owner)
    for number, owner, halves in pending[-2:]:
        take_cross(number, owner, halves)
    split(gath[pending[-1][1]], chi, clo, pending[-1][1])
    for step in range(reach + 1, half_x + 1):
        for h in (0, 1):
            if (step, h) != (half_x, 1):
                take_other(step, h)
                split_other(step, h)

    def arrival(offset):
        return pl.ds(offset * capacity * 2, capacity * 2)

    def exchange(h, offset):
        send(
            outgoing.at[h, offset], incoming.at[h, arrival(offset)],
            xs.at[h, offset], xr.at[h, offset], (x, lax.rem(y + offset, ny)),
        )

    for h in (0, 1):
        if h == 1:
            take_other(half_x, 1)
            split_other(half_x, 1)
        multiply(h, "all" if h == 1 else "late")
        for offset in range(1, ny):
            for k in range(capacity):
                outgoing[h, offset, 2 * k:2 * k + 2] = pieces[h, chosen[offset][k]]
            if offset > 1:
                exchange(h, offset - 1)
        for k in range(capacity):
            incoming[h, 2 * k:2 * k + 2] = pieces[h, chosen[0][k]]
        exchange(h, ny - 1)
    for h in (0, 1):
        for offset in range(1, ny):
            wait_recv(incoming.at[h, arrival(offset)], xr.at[h, offset])

    for s in range(slots):
        code = found[s]
        there = code >= 0
        safe = jnp.maximum(code, 0)
        rowwise = lax.rem(safe, 2) == 1
        rank = lax.rem(safe // 2, capacity)
        first_source = 2 * (safe // (2 * capacity))
        bases = [
            (lax.rem(y - first_source - h + ny, ny) * capacity + rank) * 2 for h in (0, 1)
        ]
        for i in (0, 1):
            for j in (0, 1):
                place_of = jnp.where(rowwise, bases[i] + j, bases[j] + i)
                value = jnp.concatenate([incoming[0, place_of], incoming[1, place_of]], axis=0)
                value = jnp.where(rowwise, value, value.T)
                out_ref[s, i * rows:(i + 1) * rows, j * rows:(j + 1) * rows] = jnp.where(
                    there, value, 0.0
                )
    for copy in started:
        copy.wait_send()


def plane_kernel(
    dims, rows_hbm, owner_hbm, slot_hbm, out_ref,
    gath, zfar, parts, far_parts, far, extra, owner_ref, slot_ref, todo,
    ins, ss, rs, entered,
):
    nx, ny, half_tiles, slots = dims
    rows, width = zfar.shape
    half = rows // 2
    cuts = (0, width // 2, width)
    x = lax.axis_index("gx")
    y = lax.axis_index("gy")
    core = lax.rem(y, 2)
    chip = lax.div(y, 2)
    twin = 1 - core
    right, left = (lax.rem(x + 1, nx), y), (lax.rem(x + nx - 1, nx), y)
    sibling = (x, y + 1 - 2 * core)
    across = (x, y + 2 - 4 * lax.rem(chip, 2))
    along = (x, lax.rem(y + 4, ny))

    odd, high, ends = lax.rem(chip, 2), lax.div(chip, 2), jnp.where(x == nx - 1, 1, 0)
    earlier = (1 - core, odd, high, jnp.where(x > 0, 1, 0))
    later = (core, 1 - odd, 1 - high, 1 - ends)
    barrier = pltpu.get_barrier_semaphore()

    def signal_if(flag, semaphore, target):
        @pl.when(flag == 1)
        def _():
            pl.semaphore_signal(semaphore, inc=1, device_id=target, device_id_type=MESH)

    for flag, target in zip(later, (sibling, across, along, right)):
        signal_if(flag, barrier, target)
    signal_if(jnp.where(x == 0, 1, 0), barrier, left)
    loads = [
        pltpu.make_async_copy(
            rows_hbm.at[pl.ds(h * half, half)], gath.at[0, core, pl.ds(h * half, half)],
            ins.at[h],
        )
        for h in (0, 1)
    ] + [
        pltpu.make_async_copy(owner_hbm, owner_ref, ins.at[2]),
        pltpu.make_async_copy(slot_hbm, slot_ref, ins.at[3]),
    ]
    for copy in loads:
        copy.start()
    expected = sum(earlier) + ends

    @pl.when(expected > 0)
    def _():
        pl.semaphore_wait(barrier, expected)

    for n, target in enumerate((sibling, across, along, left)):
        signal_if(earlier[n], entered.at[n], target)

    numbers, flying, issued = {}, {}, {}
    ways = {"x": (across, 0), "y": (along, 5), "z": (right, 10), "c": (sibling, 15)}

    def number(name):
        return numbers.setdefault(name, len(numbers))

    def ready(way, name, src, dst, other=None):
        target, base = ways[way]
        turn = issued.get(way, 0)
        issued[way] = turn + 1
        i, j = number(name), base + turn % 5
        if j in flying:
            flying[j].wait_send()
        copy = pltpu.make_async_remote_copy(
            src_ref=src, dst_ref=dst, send_sem=ss.at[j], recv_sem=rs.at[i],
            device_id=target, device_id_type=MESH,
        )
        flying[j] = copy
        if other is None:
            return copy
        return copy, pltpu.make_async_remote_copy(
            src_ref=other, dst_ref=dst, send_sem=ss.at[j], recv_sem=rs.at[i],
            device_id=target, device_id_type=MESH,
        )

    def send(*args):
        ready(*args).start()

    def got(name, dst):
        i = number(name)
        pltpu.make_async_remote_copy(
            src_ref=dst, dst_ref=dst, send_sem=rs.at[i], recv_sem=rs.at[i],
            device_id=sibling, device_id_type=MESH,
        ).wait_recv()

    def block(where, side, h):
        return gath.at[where, side, pl.ds(h * half, half)]

    def cross(where, h, name):
        send("c", ("cross", name), block(where, core, h), block(where, core, h))

    def crossed(where, h, name):
        got(("cross", name), block(where, twin, h))
        split(where, twin, h)

    def both_crossed(where):
        got(("cross", where), gath.at[where, twin])
        split(where, twin, 0)
        split(where, twin, 1)

    def strip(where, side, c):
        return gath.at[where, side, :, pl.ds(cuts[c], cuts[c + 1] - cuts[c])]

    def split_at(where, side, part):
        value = gath[where, side, part[0], part[1]]
        hi = value.astype(jnp.bfloat16)
        parts[where, 0, side, part[0], part[1]] = hi
        parts[where, 1, side, part[0], part[1]] = (
            value - hi.astype(jnp.float32)
        ).astype(jnp.bfloat16)

    def split(where, side, h):
        split_at(where, side, (slice(h * half, (h + 1) * half), slice(None)))

    def split_strip(side, c):
        split_at(7, side, (slice(None), slice(cuts[c], cuts[c + 1])))

    own = [rows_hbm.at[pl.ds(h * half, half)] for h in (0, 1)]
    first = [
        [ready("x", ("x", 0, h), block(0, core, h), block(1, core, h), own[h]) for h in (0, 1)],
        [ready("y", ("y", 0, h), block(0, core, h), block(2, core, h), own[h]) for h in (1, 0)],
        [ready("z", ("z", 0, h), block(0, core, h), block(4, core, h), own[h]) for h in (0, 1)],
    ]

    def open_way(n, early):
        @pl.when(later[n] == (0 if early else 1))
        def _():
            if not early:
                pl.semaphore_wait(entered.at[n], 1)
            for copies in first[n - 1]:
                copies[1 if early else 0].start()

    for n in (1, 2, 3):
        open_way(n, True)
    loads[0].wait()
    loads[1].wait()
    for n in (1, 2):
        open_way(n, False)

    @pl.when(later[0] == 1)
    def _():
        pl.semaphore_wait(entered.at[0], 1)

    for h in (0, 1):
        cross(0, h, 0)
    for h in (0, 1):
        split(0, core, h)
    open_way(3, False)
    for copy in loads[2:]:
        copy.wait()

    me = x * ny + y

    def look(tile, state):
        i_tile, j_tile = state[0], state[1]
        a, i = lax.div(i_tile, half_tiles), lax.rem(i_tile, half_tiles)
        b, j = lax.div(j_tile, half_tiles), lax.rem(j_tile, half_tiles)
        i_chip, j_chip = jnp.bitwise_xor(i, chip), jnp.bitwise_xor(j, chip)
        i_near, j_near = jnp.where(a == x, 0, half_tiles), jnp.where(b == x, 0, half_tiles)
        same = jnp.where(i_tile == j_tile, 256, 0)
        last = jnp.where((i_near + i_chip == 7) | (j_near + j_chip == 7), 64, 0)
        near = i_near + i_chip + 8 * (j_near + j_chip) + same + last
        far_code = 128 + jnp.where(
            a == x, j_chip + 8 * lax.div(i, 2), i_chip + 8 * lax.div(j, 2)
        )
        code = jnp.where(a - b == nx // 2, far_code, near)
        key = jnp.where(owner_ref[tile] == me, slot_ref[tile], slots)
        found = tuple(jnp.where(key == s, code, state[2 + s]) for s in range(slots))
        wrap = j_tile == i_tile
        return (
            jnp.where(wrap, i_tile + 1, i_tile), jnp.where(wrap, 0, j_tile + 1)
        ) + found

    codes = lax.fori_loop(
        0, owner_ref.shape[0], look, (jnp.int32(0),) * 2 + (jnp.int32(-1),) * slots
    )[2:]
    seen, picks, ranks = jnp.int32(0), [jnp.int32(0)] * 2, []
    kinds = []
    for s in range(slots):
        code = codes[s]
        kind = jnp.where(code < 0, 3, lax.rem(lax.div(code, 64), 4))
        kinds.append(kind)
        todo[s] = jnp.where(kind == 0, code, 0)
        is_last = jnp.where(kind == 1, 1, 0)
        ranks.append(seen)
        picks = [
            jnp.where(is_last * jnp.where(seen == k, 1, 0) == 1, code, picks[k])
            for k in range(2)
        ]
        seen = seen + is_last
    for k in range(2):
        todo[slots + k] = picks[k]

    one = functools.partial(
        lax.dot_general,
        dimension_numbers=(((1,), (1,)), ((), ())),
        preferred_element_type=jnp.float32,
    )

    def product(code, lo, hi):
        lhs, rhs = lax.rem(code, 8), lax.rem(lax.div(code, 8), 8)
        deep = hi - lo

        def part(n):
            return parts[rhs, n, :, :, lo:hi].reshape(2 * rows, deep)

        both = one(parts[lhs, :, :, :, lo:hi].reshape(4 * rows, deep), part(0))
        return both[:2 * rows] + (
            both[2 * rows:]
            + one(parts[lhs, 0, :, :, lo:hi].reshape(2 * rows, deep), part(1))
        )

    def to_zfar(h):
        send("z", ("z", 1, h), block(4, core, h), zfar.at[pl.ds(h * half, half)])

    got(("x", 0, 0), block(1, core, 0))
    send("y", ("near", 3), block(1, core, 0), block(3, core, 0))
    got(("y", 0, 1), block(2, core, 1))
    send("x", ("near", 3), block(2, core, 1), block(3, core, 1))
    cross(1, 0, (1, 0))
    cross(2, 1, (2, 1))
    got(("z", 0, 0), block(4, core, 0))
    to_zfar(0)
    cross(4, 0, (4, 0))
    split(1, core, 0)
    split(2, core, 1)
    split(4, core, 0)
    both_crossed(0)
    crossed(1, 0, (1, 0))
    crossed(2, 1, (2, 1))
    crossed(4, 0, (4, 0))
    got(("x", 0, 1), block(1, core, 1))
    cross(1, 1, (1, 1))
    got(("y", 0, 0), block(2, core, 0))
    cross(2, 0, (2, 0))
    got(("z", 0, 1), block(4, core, 1))
    to_zfar(1)
    for h in (0, 1):
        send("x", ("next", h), block(4, core, h), block(5, core, h))
        send("y", ("next", h), block(4, core, h), block(6, core, h))
    cross(4, 1, (4, 1))
    split(1, core, 1)
    split(2, core, 0)
    split(4, core, 1)
    crossed(1, 1, (1, 1))
    crossed(2, 0, (2, 0))
    crossed(4, 1, (4, 1))
    got(("near", 3), gath.at[3, core])
    for c in (0, 1):
        send("z", ("z", 3, c), strip(3, core, c), strip(7, core, c))
    for h in (0, 1):
        cross(3, h, 3)
    split(3, core, 0)
    split(3, core, 1)
    both_crossed(3)

    def pair(side, h):
        return gath.at[pl.ds(5, 2), side, pl.ds(h * half, half)]

    def take_next(h):
        got(("next", h), pair(core, h))
        cross(5, h, ("next", h))
        cross(6, h, ("next", h))
        split(5, core, h)
        split(6, core, h)

    def twin_next(h):
        got(("cross", ("next", h)), pair(twin, h))
        split(5, twin, h)
        split(6, twin, h)

    take_next(0)
    twin_next(0)

    def split_far(h):
        part = slice(h * half, (h + 1) * half)
        value = zfar[part]
        hi = value.astype(jnp.bfloat16)
        far_parts[0, part] = hi
        far_parts[1, part] = (value - hi.astype(jnp.float32)).astype(jnp.bfloat16)

    def far_at(where, side, t):
        return far.at[where, side, t]

    def far_cross(where, t):
        send("c", ("far",), far_at(where, core, t), far_at(where, core, t))

    flag = jnp.where(x >= nx // 2, 1, 0)
    def far_tile(t, lo, hi):
        count = hi - lo
        col = flag + 2 * lax.rem(t + lax.div(chip, 2), 2)
        both = one(
            far_parts[:, lo:hi].reshape(2 * count, width),
            parts[col, 0].reshape(2 * rows, width),
        )
        return both[:count] + (
            both[count:] + one(far_parts[0, lo:hi], parts[col, 1].reshape(2 * rows, width))
        )

    def far_rows(t, h):
        full = far_tile(t, h * half, (h + 1) * half)
        for k in (0, 1):
            far[0, core, t, k, h * half:(h + 1) * half] = full[:, k * rows:(k + 1) * rows]

    def far_turned(t):
        full = far_tile(t, 0, rows)
        for k in (0, 1):
            far[0, core, t, k] = full[:, k * rows:(k + 1) * rows].T

    def far_piece(where, t, h):
        return far.at[where, core, t, :, pl.ds(h * half, half)]

    def far_ready(h):
        return [
            ready("x", ("fx", 0, h), far_piece(0, 0, h), far_piece(1, 0, h)),
            ready("y", ("fy", 1, h), far_piece(0, 1, h), far_piece(2, 1, h)),
            ready("x", ("fx", 1), far_piece(0, 1, h), far_piece(1, 1, h)),
            ready("y", ("fy", 0), far_piece(0, 0, h), far_piece(2, 0, h)),
        ]

    got(("z", 1, 0), zfar.at[pl.ds(0, half)])
    split_far(0)
    upper = far_ready(0)

    @pl.when(flag == 0)
    def _():
        far_rows(0, 0)
        far_rows(1, 0)
        for copy in upper:
            copy.start()

    got(("z", 1, 1), zfar.at[pl.ds(half, half)])
    split_far(1)
    lower = far_ready(1)

    @pl.when(flag == 0)
    def _():
        far_rows(0, 1)
        lower[0].start()
        far_rows(1, 1)
        for copy in lower[1:]:
            copy.start()

    @pl.when(flag == 1)
    def _():
        far_turned(0)
        far_turned(1)
        for pair_of in zip(upper, lower):
            for copy in pair_of:
                copy.start()

    for t in (0, 1):
        far_cross(0, t)

    take_next(1)
    twin_next(1)

    above = jnp.where(
        lax.broadcasted_iota(jnp.int32, (2 * rows, 2 * rows), 0)
        < lax.broadcasted_iota(jnp.int32, (2 * rows, 2 * rows), 1), 1, 0,
    )

    def local(s, carry):
        code = todo[s]
        masked = jnp.where(code >= 256, 1, 0)
        out_ref[s] = jnp.where(above * masked == 1, 0.0, product(code, 0, width))
        return carry

    def take_strip(c):
        got(("z", 3, c), strip(7, core, c))
        send("c", ("cross", (7, c)), strip(7, core, c), strip(7, core, c))
        split_strip(core, c)

    def twin_strip(c):
        got(("cross", (7, c)), strip(7, twin, c))
        split_strip(twin, c)

    def behind(k, carry):
        extra[k] = product(todo[slots + k], 0, cuts[1])
        return carry

    def behind_more(k, carry):
        extra[k] = extra[k] + product(todo[slots + k], cuts[1], width)
        return carry

    middle = slots // 2
    lax.fori_loop(0, middle, local, 0)
    for h in (0, 1):
        got(("fx", 0, h), far_piece(1, 0, h))
        send("y", ("far", 3), far_piece(1, 0, h), far_piece(3, 0, h))
        got(("fy", 1, h), far_piece(2, 1, h))
        send("x", ("far", 3), far_piece(2, 1, h), far_piece(3, 1, h))
    far_cross(1, 0)
    far_cross(2, 1)
    take_strip(0)
    lax.fori_loop(middle, slots, local, 0)
    twin_strip(0)
    lax.fori_loop(0, 2, behind, 0)
    got(("fx", 1), far_at(1, core, 1))
    far_cross(1, 1)
    got(("fy", 0), far_at(2, core, 0))
    far_cross(2, 0)
    take_strip(1)
    got(("far", 3), far.at[3, core])
    far_cross(3, 0)
    far_cross(3, 1)
    twin_strip(1)
    lax.fori_loop(0, 2, behind_more, 0)
    got(("far",), far.at[:, twin])

    for s in range(slots):
        kind, code = kinds[s], jnp.maximum(codes[s], 0)
        where = lax.rem(code, 4)
        t = lax.rem(lax.div(code, 8), 2)
        rank = jnp.minimum(ranks[s], 1)
        for i in (0, 1):
            for j in (0, 1):
                side, k = jnp.where(flag == 0, i, j), jnp.where(flag == 0, j, i)
                at = (s, slice(i * rows, (i + 1) * rows), slice(j * rows, (j + 1) * rows))
                value = jnp.where(kind == 1, extra[rank, at[1], at[2]], out_ref[at])
                value = jnp.where(kind == 2, far[where, side, t, k], value)
                out_ref[at] = jnp.where(kind == 3, 0.0, value)
    for copy in flying.values():
        copy.wait_send()


def plane_call(dims, *arrays):
    nx, ny, half_tiles, slots = dims
    matrix_rows, tile_owner, tile_slot = arrays
    rows, width = matrix_rows.shape
    f32, bf16 = jnp.float32, jnp.bfloat16
    dma = pltpu.SemaphoreType.DMA
    hbm = pl.BlockSpec(memory_space=pltpu.HBM)
    return pl.pallas_call(
        functools.partial(plane_kernel, dims),
        out_shape=jax.ShapeDtypeStruct((slots, 2 * rows, 2 * rows), f32),
        in_specs=[hbm, hbm, hbm],
        out_specs=pl.BlockSpec(memory_space=pltpu.VMEM),
        scratch_shapes=[
            pltpu.VMEM((8, 2, rows, width), f32),
            pltpu.VMEM((rows, width), f32),
            pltpu.VMEM((8, 2, 2, rows, width), bf16),
            pltpu.VMEM((2, rows, width), bf16),
            pltpu.VMEM((4, 2, 2, 2, rows, rows), f32),
            pltpu.VMEM((2, 2 * rows, 2 * rows), f32),
            pltpu.SMEM(tile_owner.shape, jnp.int32),
            pltpu.SMEM(tile_slot.shape, jnp.int32),
            pltpu.SMEM((slots + 2,), jnp.int32),
            dma((4,)), dma((20,)), dma((33,)), pltpu.SemaphoreType.REGULAR((4,)),
        ],
        compiler_params=pltpu.CompilerParams(
            collective_id=0, has_side_effects=True,
            vmem_limit_bytes=44 * 1024 * 1024,
        ),
    )(*(pltpu.with_memory_space_constraint(a, pltpu.HBM) for a in arrays))


def copy_out(in_ref, out_ref, sem):
    copy = pltpu.make_async_copy(in_ref, out_ref, sem)
    copy.start()
    copy.wait()


def ring_call(mesh_shape, matrix_rows, tile_owner, tile_slot):
    nx, ny = mesh_shape
    rows, width = matrix_rows.shape
    half_tiles, half_x = ny // 2, nx // 2
    capacity = nx // 4 + 1
    slots = -(-tile_owner.shape[0] // (nx * ny))
    _, piece_count = piece_lists(half_tiles, half_x)
    reach = max(ny // 4, 1)
    f32, bf16 = jnp.float32, jnp.bfloat16
    dma = pltpu.SemaphoreType.DMA
    return pl.pallas_call(
        functools.partial(kernel, (nx, ny, half_tiles, half_x, capacity, slots)),
        out_shape=jax.ShapeDtypeStruct((slots, 2 * rows, 2 * rows), f32),
        in_specs=[
            pl.BlockSpec(memory_space=pltpu.VMEM),
            pl.BlockSpec(memory_space=pltpu.SMEM),
            pl.BlockSpec(memory_space=pltpu.SMEM),
        ],
        out_specs=pl.BlockSpec(memory_space=pltpu.VMEM),
        scratch_shapes=[
            pltpu.VMEM((ny, rows, width), f32),
            pltpu.VMEM((half_x, rows, width), f32),
            pltpu.VMEM((ny, rows, width), bf16),
            pltpu.VMEM((ny, rows, width), bf16),
            pltpu.VMEM((half_x + 1, 2, rows, width), bf16),
            pltpu.VMEM((2, piece_count, 2, rows // 2, rows), f32),
            pltpu.VMEM((2, ny, 2 * capacity, rows // 2, rows), f32),
            pltpu.VMEM((2, ny * 2 * capacity, rows // 2, rows), f32),
            pltpu.SMEM((piece_count,), jnp.int32),
            dma((reach, 2)), dma((reach, 2)), dma((reach, 2)), dma((reach, 2)),
            dma((2 * reach + 1, 2)), dma((2 * reach + 1, 2)),
            dma((half_x, 2)), dma((half_x, 2)),
            dma((2, ny)), dma((2, ny)),
        ],
        compiler_params=pltpu.CompilerParams(
            collective_id=0, has_side_effects=True, vmem_limit_bytes=44 * 1024 * 1024
        ),
    )(matrix_rows, tile_owner, tile_slot)


def per_device(mesh_shape, matrix_rows, tile_owner, tile_slot):
    nx, ny = mesh_shape
    if ny // 2 == 4 and nx == 4:
        slots = -(-tile_owner.shape[0] // (nx * ny))
        packed = plane_call((nx, ny, ny // 2, slots), matrix_rows, tile_owner, tile_slot)
    else:
        packed = ring_call(mesh_shape, matrix_rows, tile_owner, tile_slot)
    return pl.pallas_call(
        copy_out,
        out_shape=jax.ShapeDtypeStruct(packed.shape, packed.dtype),
        in_specs=[pl.BlockSpec(memory_space=pltpu.VMEM)],
        out_specs=pl.BlockSpec(memory_space=pl.ANY),
        scratch_shapes=[pltpu.SemaphoreType.DMA(())],
        compiler_params=pltpu.CompilerParams(vmem_limit_bytes=4 * 1024 * 1024),
    )(packed)


def solution(mesh):
    placed = (P(("gx", "gy"), None), P(), P())
    return jax.shard_map(
        functools.partial(per_device, (mesh.shape["gx"], mesh.shape["gy"])),
        mesh=mesh,
        in_specs=placed,
        out_specs=P(("gx", "gy"), None, None),
        check_vma=False,
    )
```

```python
import functools

import jax
import jax.numpy as jnp
from jax import lax
from jax.experimental import pallas as pl
from jax.experimental.pallas import tpu as pltpu
from jax.sharding import PartitionSpec as P

MESH = pl.DeviceIdType.MESH


def chip_position(chip, chips):
    row, col = lax.div(chip, 2), lax.rem(chip, 2)
    return col * (1 + row) + (1 - col) * lax.rem(chips - row, chips)


def chip_at(position, chips):
    behind = lax.rem(position + chips - 1, chips)
    far = lax.div(behind, chips // 2)
    return (1 - far) * (2 * behind + 1) + far * 2 * (chips - 1 - behind)


def piece_lists(half_tiles, half_x):
    lists, start = [], 0
    for step in range(half_x + 1):
        if step == 0:
            count = half_tiles // 2 + 1
        elif step < half_x:
            count = half_tiles
        else:
            count = half_tiles // 2
        lists.append((step, start, count))
        start += count
    return lists, start


def piece(x, r, step, i, nx, half_tiles, half_x):
    source = lax.rem(x - step + nx, nx)
    if step == 0:
        col = lax.rem(r - i + half_tiles, half_tiles)
        valid = jnp.logical_or(i < half_tiles // 2, r < half_tiles // 2)
        rowwise = col <= r
    elif step < half_x:
        col = i
        valid = i >= 0
        rowwise = source > x
    else:
        flag = jnp.where(x >= half_x, 1, 0)
        col = 2 * i + lax.rem(r + flag, 2)
        valid = i >= 0
        rowwise = source > x
    other, mine = source * half_tiles + r, x * half_tiles + col
    row_tile = jnp.where(rowwise, other, mine)
    col_tile = jnp.where(rowwise, mine, other)
    tile = jnp.where(valid, row_tile * (row_tile + 1) // 2 + col_tile, 0)
    return col, valid, rowwise, tile


def kernel(
    dims, rows_ref, owner_ref, slot_ref, out_ref,
    gath, zbuf, chi, clo, zsplit, pieces, outgoing, incoming, targets,
    gs_r, gr_r, gs_l, gr_l, ss, sr, zs, zr, xs, xr,
):
    nx, ny, half_tiles, half_x, capacity, slots = dims
    rows = rows_ref.shape[0]
    half = rows // 2
    chips = ny // 2
    reach = chips // 2
    x = lax.axis_index("gx")
    y = lax.axis_index("gy")
    core = lax.rem(y, 2)
    chip = lax.div(y, 2)
    right_x, left_x = lax.rem(x + 1, nx), lax.rem(x + nx - 1, nx)
    sibling = y + 1 - 2 * core
    place = chip_position(chip, chips)

    def at(position):
        return 2 * chip_at(lax.rem(position + chips, chips), chips) + core

    next_y, prev_y = at(place + 1), at(place - 1)
    lists, piece_count = piece_lists(half_tiles, half_x)

    barrier = pltpu.get_barrier_semaphore()
    for other in (right_x, left_x):
        pl.semaphore_signal(barrier, inc=1, device_id=(other, y), device_id_type=MESH)
    for offset in range(1, ny):
        pl.semaphore_signal(
            barrier, inc=1, device_id=(x, lax.rem(y + offset, ny)), device_id_type=MESH
        )
    pl.semaphore_wait(barrier, ny + 1)

    started = []

    def send(src, dst, send_sem, recv_sem, target):
        copy = pltpu.make_async_remote_copy(
            src_ref=src, dst_ref=dst, send_sem=send_sem, recv_sem=recv_sem,
            device_id=target, device_id_type=MESH,
        )
        copy.start()
        started.append(copy)

    def part(h):
        return pl.ds(h * half, half)

    def zcopy(step, h):
        src = rows_ref.at[part(h)] if step == 1 else zbuf.at[step - 2, part(h)]
        send(src, zbuf.at[step - 1, part(h)], zs.at[step - 1, h], zr.at[step - 1, h], (right_x, y))

    def block(owner, h):
        return gath.at[owner, part(h)]

    def ring(direction, distance, h):
        owner = at(place - direction * (distance - 1))
        src = rows_ref.at[part(h)] if distance == 1 else block(owner, h)
        s, r = (gs_r, gr_r) if direction == 1 else (gs_l, gr_l)
        target = next_y if direction == 1 else prev_y
        send(src, block(owner, h), s.at[distance - 1, h], r.at[distance - 1, h], (x, target))

    def cross(number, owner, h):
        src = rows_ref.at[part(h)] if number == 0 else block(owner, h)
        send(src, block(owner, h), ss.at[number, h], sr.at[number, h], (x, sibling))

    def halves_of(direction, distance):
        if distance < reach:
            return (0, 1) if direction == 1 else (1, 0)
        return (0,) if direction == 1 else (1,)

    def split(value, hi_ref, lo_ref, index):
        hi = value.astype(jnp.bfloat16)
        hi_ref[index] = hi
        lo_ref[index] = (value - hi.astype(jnp.float32)).astype(jnp.bfloat16)

    zcopy(1, 0)
    ring(1, 1, 0)
    if reach > 1:
        ring(-1, 1, 1)
        zcopy(1, 1)
        ring(1, 1, 1)
        ring(-1, 1, 0)
    else:
        ring(-1, 1, 1)
        zcopy(1, 1)
    cross(0, y, 0)
    cross(0, y, 1)

    for step, first, count in lists:
        def fill(i, carry, step=step, first=first):
            _, valid, _, tile = piece(x, chip, step, i, nx, half_tiles, half_x)
            targets[first + i] = jnp.where(valid, lax.rem(owner_ref[tile], ny), ny)
            return carry
        lax.fori_loop(0, count, fill, 0)

    me = x * ny + y

    def class_loop(r, carry):
        state = (jnp.int32(0),) + carry
        for step, first, count in lists:
            def look(i, state, step=step):
                seen, found = state[0], state[1:]
                _, valid, rowwise, tile = piece(x, r, step, i, nx, half_tiles, half_x)
                mine = jnp.where(valid, jnp.where(owner_ref[tile] == me, 1, 0), 0)
                slot = slot_ref[tile]
                code = 2 * (r * capacity + jnp.minimum(seen, capacity - 1))
                code = code + jnp.where(rowwise, 1, 0)
                key = jnp.where(mine == 1, slot, slots)
                found = tuple(jnp.where(key == s, code, found[s]) for s in range(slots))
                return (seen + mine,) + found
            state = lax.fori_loop(0, count, look, state)
        return state[1:]

    found = lax.fori_loop(0, half_tiles, class_loop, (jnp.int32(-1),) * slots)

    chosen = []
    for offset in range(ny):
        dest = lax.rem(y + offset, ny)

        def pick(p, state, dest=dest):
            hit = jnp.where(targets[p] == dest, 1, 0)
            seen = state[0]
            key = jnp.where(hit == 1, seen, capacity)
            picks = tuple(jnp.where(key == k, p, state[1 + k]) for k in range(capacity))
            return (seen + hit,) + picks

        chosen.append(lax.fori_loop(0, piece_count, pick, (jnp.int32(0),) * (capacity + 1))[1:])

    def wait_recv(dst, sem):
        pltpu.make_async_remote_copy(
            src_ref=dst, dst_ref=dst, send_sem=sem, recv_sem=sem,
            device_id=(x, sibling), device_id_type=MESH,
        ).wait_recv()

    def split_other(step, h):
        ref = rows_ref.at[part(h)] if step == 0 else zbuf.at[step - 1, part(h)]
        value = ref[...]
        hi = value.astype(jnp.bfloat16)
        zsplit[step, h, :half] = hi
        zsplit[step, h, half:] = (value - hi.astype(jnp.float32)).astype(jnp.bfloat16)

    def take_other(step, h):
        wait_recv(zbuf.at[step - 1, part(h)], zr.at[step - 1, h])
        if step < half_x:
            zcopy(step + 1, h)

    split_other(0, 0)
    split_other(0, 1)
    split(rows_ref[...], chi, clo, y)

    def take_cross(number, owner, halves):
        for h in halves:
            wait_recv(block(owner, h), sr.at[number, h])

    one = functools.partial(
        lax.dot_general,
        dimension_numbers=(((1,), (1,)), ((), ())),
        preferred_element_type=jnp.float32,
    )
    width = rows_ref.shape[1]
    row_inside = core * rows + lax.broadcasted_iota(jnp.int32, (half, 2 * rows), 0)
    col_inside = lax.broadcasted_iota(jnp.int32, (half, 2 * rows), 1)

    def one_piece_of(h):
        above = jnp.where(row_inside + h * half < col_inside, 1, 0)

        def one_piece(i, step, first, col):
            b_hi = chi[pl.ds(2 * col, 2)].reshape(2 * rows, width)
            b_lo = clo[pl.ds(2 * col, 2)].reshape(2 * rows, width)
            both = one(zsplit[step, h], b_hi)
            full = both[:half] + (both[half:] + one(zsplit[step, h, :half], b_lo))
            if step == 0:
                full = jnp.where(above * jnp.where(i == 0, 1, 0) == 1, 0.0, full)
            pieces[h, first + i, 0] = full[:, :rows]
            pieces[h, first + i, 1] = full[:, rows:]

        return one_piece

    farthest = chip_at(lax.rem(place + reach, chips), chips)
    soon = min(reach, half_x) if reach > 1 else 0

    def multiply(h, mode):
        one_piece = one_piece_of(h)
        for step, first, count in lists:
            if mode == "early" and step >= soon:
                continue

            def make(i, carry, step=step, first=first):
                col, _, _, _ = piece(x, chip, step, i, nx, half_tiles, half_x)
                if mode == "all" or step >= soon:
                    one_piece(i, step, first, col)
                else:
                    wanted = (col != farthest) if mode == "early" else (col == farthest)
                    pl.when(wanted)(lambda: one_piece(i, step, first, col))
                return carry
            lax.fori_loop(0, count, make, 0)

    pending = [(0, sibling, (0, 1))]
    for distance in range(1, reach + 1):
        if distance == reach:
            for number, owner, halves in pending[1:]:
                take_cross(number, owner, halves)
                split(gath[owner], chi, clo, owner)
            multiply(0, "early")
        if distance <= half_x:
            for h in (0, 1):
                if (distance, h) != (half_x, 1):
                    take_other(distance, h)
                if h in halves_of(1, distance):
                    owner = at(place - distance)
                    wait_recv(block(owner, h), gr_r.at[distance - 1, h])
                    if distance < reach and h in halves_of(1, distance + 1):
                        ring(1, distance + 1, h)
                    cross(2 * distance - 1, owner, h)
                g = 1 - h
                if g in halves_of(-1, distance):
                    owner = at(place + distance)
                    wait_recv(block(owner, g), gr_l.at[distance - 1, g])
                    if distance < reach and g in halves_of(-1, distance + 1):
                        ring(-1, distance + 1, g)
                    cross(2 * distance, owner, g)
            split_other(distance, 0)
            if distance < half_x:
                split_other(distance, 1)
        behind, ahead = at(place - distance), at(place + distance)
        pending.append((2 * distance - 1, behind + 1 - 2 * core, halves_of(1, distance)))
        pending.append((2 * distance, ahead + 1 - 2 * core, halves_of(-1, distance)))
        split(gath[behind], chi, clo, behind)
        if distance < reach:
            split(gath[ahead], chi, clo, ahead)
        for number, owner, halves in pending[: (1 if distance == 1 else 0)]:
            take_cross(number, owner, halves)
            split(gath[owner], chi, clo, owner)
    for number, owner, halves in pending[-2:]:
        take_cross(number, owner, halves)
    split(gath[pending[-1][1]], chi, clo, pending[-1][1])
    for step in range(reach + 1, half_x + 1):
        for h in (0, 1):
            if (step, h) != (half_x, 1):
                take_other(step, h)
                split_other(step, h)

    def arrival(offset):
        return pl.ds(offset * capacity * 2, capacity * 2)

    def exchange(h, offset):
        send(
            outgoing.at[h, offset], incoming.at[h, arrival(offset)],
            xs.at[h, offset], xr.at[h, offset], (x, lax.rem(y + offset, ny)),
        )

    for h in (0, 1):
        if h == 1:
            take_other(half_x, 1)
            split_other(half_x, 1)
        multiply(h, "all" if h == 1 else "late")
        for offset in range(1, ny):
            for k in range(capacity):
                outgoing[h, offset, 2 * k:2 * k + 2] = pieces[h, chosen[offset][k]]
            if offset > 1:
                exchange(h, offset - 1)
        for k in range(capacity):
            incoming[h, 2 * k:2 * k + 2] = pieces[h, chosen[0][k]]
        exchange(h, ny - 1)
    for h in (0, 1):
        for offset in range(1, ny):
            wait_recv(incoming.at[h, arrival(offset)], xr.at[h, offset])

    for s in range(slots):
        code = found[s]
        there = code >= 0
        safe = jnp.maximum(code, 0)
        rowwise = lax.rem(safe, 2) == 1
        rank = lax.rem(safe // 2, capacity)
        first_source = 2 * (safe // (2 * capacity))
        bases = [
            (lax.rem(y - first_source - h + ny, ny) * capacity + rank) * 2 for h in (0, 1)
        ]
        for i in (0, 1):
            for j in (0, 1):
                place_of = jnp.where(rowwise, bases[i] + j, bases[j] + i)
                value = jnp.concatenate([incoming[0, place_of], incoming[1, place_of]], axis=0)
                value = jnp.where(rowwise, value, value.T)
                out_ref[s, i * rows:(i + 1) * rows, j * rows:(j + 1) * rows] = jnp.where(
                    there, value, 0.0
                )
    for copy in started:
        copy.wait_send()


def plane_kernel(
    dims, rows_hbm, owner_hbm, slot_hbm, out_ref,
    gath, zfar, parts, far_parts, far, extra, owner_ref, slot_ref, todo,
    ins, ss, rs, entered,
):
    nx, ny, half_tiles, slots = dims
    rows, width = zfar.shape
    half = rows // 2
    cuts = (0, width // 2, width)
    x = lax.axis_index("gx")
    y = lax.axis_index("gy")
    core = lax.rem(y, 2)
    chip = lax.div(y, 2)
    twin = 1 - core
    right, left = (lax.rem(x + 1, nx), y), (lax.rem(x + nx - 1, nx), y)
    sibling = (x, y + 1 - 2 * core)
    across = (x, y + 2 - 4 * lax.rem(chip, 2))
    along = (x, lax.rem(y + 4, ny))

    odd, high, ends = lax.rem(chip, 2), lax.div(chip, 2), jnp.where(x == nx - 1, 1, 0)
    earlier = (1 - core, odd, high, jnp.where(x > 0, 1, 0))
    later = (core, 1 - odd, 1 - high, 1 - ends)
    barrier = pltpu.get_barrier_semaphore()

    def signal_if(flag, semaphore, target):
        @pl.when(flag == 1)
        def _():
            pl.semaphore_signal(semaphore, inc=1, device_id=target, device_id_type=MESH)

    for flag, target in zip(later, (sibling, across, along, right)):
        signal_if(flag, barrier, target)
    signal_if(jnp.where(x == 0, 1, 0), barrier, left)
    loads = [
        pltpu.make_async_copy(rows_hbm, gath.at[0, core], ins.at[0]),
        pltpu.make_async_copy(owner_hbm, owner_ref, ins.at[1]),
        pltpu.make_async_copy(slot_hbm, slot_ref, ins.at[2]),
    ]
    for copy in loads:
        copy.start()
    expected = sum(earlier) + ends

    @pl.when(expected > 0)
    def _():
        pl.semaphore_wait(barrier, expected)

    for n, target in enumerate((sibling, across, along, left)):
        signal_if(earlier[n], entered.at[n], target)

    numbers, flying, issued = {}, {}, {}
    ways = {"x": (across, 0, 5), "y": (along, 5, 5), "z": (right, 10, 3), "c": (sibling, 13, 4)}

    def number(name):
        return numbers.setdefault(name, len(numbers))

    def ready(way, name, src, dst, other=None):
        target, base, pool = ways[way]
        turn = issued.get(way, 0)
        issued[way] = turn + 1
        i, j = number(name), base + turn % pool
        if j in flying:
            flying[j].wait_send()
        copy = pltpu.make_async_remote_copy(
            src_ref=src, dst_ref=dst, send_sem=ss.at[j], recv_sem=rs.at[i],
            device_id=target, device_id_type=MESH,
        )
        flying[j] = copy
        if other is None:
            return copy
        return copy, pltpu.make_async_remote_copy(
            src_ref=other, dst_ref=dst, send_sem=ss.at[j], recv_sem=rs.at[i],
            device_id=target, device_id_type=MESH,
        )

    def send(*args):
        ready(*args).start()

    def got(name, dst):
        i = number(name)
        pltpu.make_async_remote_copy(
            src_ref=dst, dst_ref=dst, send_sem=rs.at[i], recv_sem=rs.at[i],
            device_id=sibling, device_id_type=MESH,
        ).wait_recv()

    def block(where, side, h):
        return gath.at[where, side, pl.ds(h * half, half)]

    def cross(where, h, name):
        send("c", ("cross", name), block(where, core, h), block(where, core, h))

    def crossed(where, h, name):
        got(("cross", name), block(where, twin, h))
        split(where, twin, h)

    def both_crossed(where):
        got(("cross", where), gath.at[where, twin])
        split(where, twin, 0)
        split(where, twin, 1)

    def strip(where, side, c):
        return gath.at[where, side, :, pl.ds(cuts[c], cuts[c + 1] - cuts[c])]

    def split_at(where, side, part):
        value = gath[where, side, part[0], part[1]]
        hi = value.astype(jnp.bfloat16)
        parts[where, 0, side, part[0], part[1]] = hi
        parts[where, 1, side, part[0], part[1]] = (
            value - hi.astype(jnp.float32)
        ).astype(jnp.bfloat16)

    def split(where, side, h):
        split_at(where, side, (slice(h * half, (h + 1) * half), slice(None)))

    def split_strip(side, c):
        split_at(7, side, (slice(None), slice(cuts[c], cuts[c + 1])))

    own = [rows_hbm.at[pl.ds(h * half, half)] for h in (0, 1)]
    first = [
        [ready("x", ("x", 0, h), block(0, core, h), block(1, core, h), own[h]) for h in (0, 1)],
        [ready("y", ("y", 0, h), block(0, core, h), block(2, core, h), own[h]) for h in (1, 0)],
        [ready("z", ("z", 0, h), block(0, core, h), block(4, core, h), own[h]) for h in (0, 1)],
    ]

    def open_way(n, early):
        @pl.when(later[n] == (0 if early else 1))
        def _():
            if not early:
                pl.semaphore_wait(entered.at[n], 1)
            for copies in first[n - 1]:
                copies[1 if early else 0].start()

    for n in (1, 2, 3):
        open_way(n, True)
    loads[0].wait()
    for n in (1, 2):
        open_way(n, False)

    @pl.when(later[0] == 1)
    def _():
        pl.semaphore_wait(entered.at[0], 1)

    for h in (0, 1):
        cross(0, h, 0)
    for h in (0, 1):
        split(0, core, h)
    open_way(3, False)
    for copy in loads[1:]:
        copy.wait()

    me = x * ny + y

    def look(tile, state):
        i_tile, j_tile = state[0], state[1]
        a, i = lax.div(i_tile, half_tiles), lax.rem(i_tile, half_tiles)
        b, j = lax.div(j_tile, half_tiles), lax.rem(j_tile, half_tiles)
        i_chip, j_chip = jnp.bitwise_xor(i, chip), jnp.bitwise_xor(j, chip)
        i_near, j_near = jnp.where(a == x, 0, half_tiles), jnp.where(b == x, 0, half_tiles)
        same = jnp.where(i_tile == j_tile, 256, 0)
        last = jnp.where((i_near + i_chip == 7) | (j_near + j_chip == 7), 64, 0)
        near = i_near + i_chip + 8 * (j_near + j_chip) + same + last
        far_code = 128 + jnp.where(
            a == x, j_chip + 8 * lax.div(i, 2), i_chip + 8 * lax.div(j, 2)
        )
        code = jnp.where(a - b == nx // 2, far_code, near)
        key = jnp.where(owner_ref[tile] == me, slot_ref[tile], slots)
        found = tuple(jnp.where(key == s, code, state[2 + s]) for s in range(slots))
        wrap = j_tile == i_tile
        return (
            jnp.where(wrap, i_tile + 1, i_tile), jnp.where(wrap, 0, j_tile + 1)
        ) + found

    codes = lax.fori_loop(
        0, owner_ref.shape[0], look, (jnp.int32(0),) * 2 + (jnp.int32(-1),) * slots
    )[2:]
    seen, picks, ranks = jnp.int32(0), [jnp.int32(0)] * 2, []
    kinds = []
    for s in range(slots):
        code = codes[s]
        kind = jnp.where(code < 0, 3, lax.rem(lax.div(code, 64), 4))
        kinds.append(kind)
        todo[s] = jnp.where(kind == 0, code, 0)
        is_last = jnp.where(kind == 1, 1, 0)
        ranks.append(seen)
        picks = [
            jnp.where(is_last * jnp.where(seen == k, 1, 0) == 1, code, picks[k])
            for k in range(2)
        ]
        seen = seen + is_last
    for k in range(2):
        todo[slots + k] = picks[k]

    one = functools.partial(
        lax.dot_general,
        dimension_numbers=(((1,), (1,)), ((), ())),
        preferred_element_type=jnp.float32,
    )

    def product(code, lo, hi):
        lhs, rhs = lax.rem(code, 8), lax.rem(lax.div(code, 8), 8)
        deep = hi - lo

        def part(n):
            return parts[rhs, n, :, :, lo:hi].reshape(2 * rows, deep)

        both = one(parts[lhs, :, :, :, lo:hi].reshape(4 * rows, deep), part(0))
        return both[:2 * rows] + (
            both[2 * rows:]
            + one(parts[lhs, 0, :, :, lo:hi].reshape(2 * rows, deep), part(1))
        )

    def to_zfar(h):
        send("z", ("z", 1, h), block(4, core, h), zfar.at[pl.ds(h * half, half)])

    got(("x", 0, 0), block(1, core, 0))
    send("y", ("near", 3), block(1, core, 0), block(3, core, 0))
    got(("y", 0, 1), block(2, core, 1))
    send("x", ("near", 3), block(2, core, 1), block(3, core, 1))
    cross(1, 0, (1, 0))
    cross(2, 1, (2, 1))
    got(("z", 0, 0), block(4, core, 0))
    to_zfar(0)
    cross(4, 0, (4, 0))
    split(1, core, 0)
    split(2, core, 1)
    split(4, core, 0)
    both_crossed(0)
    crossed(1, 0, (1, 0))
    crossed(2, 1, (2, 1))
    crossed(4, 0, (4, 0))
    got(("x", 0, 1), block(1, core, 1))
    cross(1, 1, (1, 1))
    got(("y", 0, 0), block(2, core, 0))
    cross(2, 0, (2, 0))
    got(("z", 0, 1), block(4, core, 1))
    to_zfar(1)
    for h in (0, 1):
        send("x", ("next", h), block(4, core, h), block(5, core, h))
        send("y", ("next", h), block(4, core, h), block(6, core, h))
    cross(4, 1, (4, 1))
    split(1, core, 1)
    split(2, core, 0)
    split(4, core, 1)
    crossed(1, 1, (1, 1))
    crossed(2, 0, (2, 0))
    crossed(4, 1, (4, 1))
    got(("near", 3), gath.at[3, core])
    for c in (0, 1):
        send("z", ("z", 3, c), strip(3, core, c), strip(7, core, c))
    for h in (0, 1):
        cross(3, h, 3)
    split(3, core, 0)
    split(3, core, 1)
    both_crossed(3)

    def pair(side, h):
        return gath.at[pl.ds(5, 2), side, pl.ds(h * half, half)]

    def take_next(h):
        got(("next", h), pair(core, h))
        cross(5, h, ("next", h))
        cross(6, h, ("next", h))
        split(5, core, h)
        split(6, core, h)

    def twin_next(h):
        got(("cross", ("next", h)), pair(twin, h))
        split(5, twin, h)
        split(6, twin, h)

    take_next(0)
    twin_next(0)

    def split_far(h):
        part = slice(h * half, (h + 1) * half)
        value = zfar[part]
        hi = value.astype(jnp.bfloat16)
        far_parts[0, part] = hi
        far_parts[1, part] = (value - hi.astype(jnp.float32)).astype(jnp.bfloat16)

    def far_at(where, side, t):
        return far.at[where, side, t]

    def far_cross(where, t):
        send("c", ("far",), far_at(where, core, t), far_at(where, core, t))

    flag = jnp.where(x >= nx // 2, 1, 0)
    def far_tile(t, lo, hi):
        count = hi - lo
        col = flag + 2 * lax.rem(t + lax.div(chip, 2), 2)
        both = one(
            far_parts[:, lo:hi].reshape(2 * count, width),
            parts[col, 0].reshape(2 * rows, width),
        )
        return both[:count] + (
            both[count:] + one(far_parts[0, lo:hi], parts[col, 1].reshape(2 * rows, width))
        )

    def far_rows(t, h):
        full = far_tile(t, h * half, (h + 1) * half)
        for k in (0, 1):
            far[0, core, t, k, h * half:(h + 1) * half] = full[:, k * rows:(k + 1) * rows]

    def far_turned(t):
        full = far_tile(t, 0, rows)
        for k in (0, 1):
            far[0, core, t, k] = full[:, k * rows:(k + 1) * rows].T

    def far_piece(where, t, h):
        return far.at[where, core, t, :, pl.ds(h * half, half)]

    def far_ready(h):
        return [
            ready("x", ("fx", 0, h), far_piece(0, 0, h), far_piece(1, 0, h)),
            ready("y", ("fy", 1, h), far_piece(0, 1, h), far_piece(2, 1, h)),
            ready("x", ("f2",), far_piece(0, 1, h), far_piece(1, 1, h)),
            ready("y", ("f2",), far_piece(0, 0, h), far_piece(2, 0, h)),
        ]

    got(("z", 1, 0), zfar.at[pl.ds(0, half)])
    split_far(0)
    upper = far_ready(0)

    @pl.when(flag == 0)
    def _():
        far_rows(0, 0)
        far_rows(1, 0)
        for copy in upper:
            copy.start()

    got(("z", 1, 1), zfar.at[pl.ds(half, half)])
    split_far(1)
    lower = far_ready(1)

    @pl.when(flag == 0)
    def _():
        far_rows(0, 1)
        lower[0].start()
        far_rows(1, 1)
        for copy in lower[1:]:
            copy.start()

    @pl.when(flag == 1)
    def _():
        far_turned(0)
        far_turned(1)
        for pair_of in zip(upper, lower):
            for copy in pair_of:
                copy.start()

    for t in (0, 1):
        far_cross(0, t)

    take_next(1)
    twin_next(1)

    above = jnp.where(
        lax.broadcasted_iota(jnp.int32, (2 * rows, 2 * rows), 0)
        < lax.broadcasted_iota(jnp.int32, (2 * rows, 2 * rows), 1), 1, 0,
    )

    def local(s, carry):
        code = todo[s]
        masked = jnp.where(code >= 256, 1, 0)
        out_ref[s] = jnp.where(above * masked == 1, 0.0, product(code, 0, width))
        return carry

    def take_strip(c):
        got(("z", 3, c), strip(7, core, c))
        send("c", ("cross", (7, c)), strip(7, core, c), strip(7, core, c))
        split_strip(core, c)

    def twin_strip(c):
        got(("cross", (7, c)), strip(7, twin, c))
        split_strip(twin, c)

    def behind(k, carry):
        extra[k] = product(todo[slots + k], 0, cuts[1])
        return carry

    def behind_more(k, carry):
        extra[k] = extra[k] + product(todo[slots + k], cuts[1], width)
        return carry

    middle = slots // 2
    lax.fori_loop(0, middle, local, 0)
    for h in (0, 1):
        got(("fx", 0, h), far_piece(1, 0, h))
        send("y", ("far", 3, h), far_piece(1, 0, h), far_piece(3, 0, h))
        got(("fy", 1, h), far_piece(2, 1, h))
        send("x", ("far", 3, h), far_piece(2, 1, h), far_piece(3, 1, h))
    far_cross(1, 0)
    far_cross(2, 1)
    take_strip(0)
    lax.fori_loop(middle, slots, local, 0)
    twin_strip(0)
    lax.fori_loop(0, 2, behind, 0)
    got(("f2",), far.at[1, core])
    far_cross(1, 1)
    far_cross(2, 0)
    take_strip(1)
    for h in (0, 1):
        both_tiles = far.at[3, core, :, :, pl.ds(h * half, half)]
        got(("far", 3, h), both_tiles)
        send("c", ("far",), both_tiles, both_tiles)
    twin_strip(1)
    lax.fori_loop(0, 2, behind_more, 0)
    got(("far",), far.at[:, twin])

    for s in range(slots):
        kind, code = kinds[s], jnp.maximum(codes[s], 0)
        where = lax.rem(code, 4)
        t = lax.rem(lax.div(code, 8), 2)
        rank = jnp.minimum(ranks[s], 1)
        for i in (0, 1):
            for j in (0, 1):
                side, k = jnp.where(flag == 0, i, j), jnp.where(flag == 0, j, i)
                at = (s, slice(i * rows, (i + 1) * rows), slice(j * rows, (j + 1) * rows))
                value = jnp.where(kind == 1, extra[rank, at[1], at[2]], out_ref[at])
                value = jnp.where(kind == 2, far[where, side, t, k], value)
                out_ref[at] = jnp.where(kind == 3, 0.0, value)
    for copy in flying.values():
        copy.wait_send()


def plane_call(dims, *arrays):
    nx, ny, half_tiles, slots = dims
    matrix_rows, tile_owner, tile_slot = arrays
    rows, width = matrix_rows.shape
    f32, bf16 = jnp.float32, jnp.bfloat16
    dma = pltpu.SemaphoreType.DMA
    hbm = pl.BlockSpec(memory_space=pltpu.HBM)
    return pl.pallas_call(
        functools.partial(plane_kernel, dims),
        out_shape=jax.ShapeDtypeStruct((slots, 2 * rows, 2 * rows), f32),
        in_specs=[hbm, hbm, hbm],
        out_specs=pl.BlockSpec(memory_space=pltpu.VMEM),
        scratch_shapes=[
            pltpu.VMEM((8, 2, rows, width), f32),
            pltpu.VMEM((rows, width), f32),
            pltpu.VMEM((8, 2, 2, rows, width), bf16),
            pltpu.VMEM((2, rows, width), bf16),
            pltpu.VMEM((4, 2, 2, 2, rows, rows), f32),
            pltpu.VMEM((2, 2 * rows, 2 * rows), f32),
            pltpu.SMEM(tile_owner.shape, jnp.int32),
            pltpu.SMEM(tile_slot.shape, jnp.int32),
            pltpu.SMEM((slots + 2,), jnp.int32),
            dma((3,)), dma((17,)), dma((33,)), pltpu.SemaphoreType.REGULAR((4,)),
        ],
        compiler_params=pltpu.CompilerParams(
            collective_id=0, has_side_effects=True,
            vmem_limit_bytes=44 * 1024 * 1024,
        ),
    )(*(pltpu.with_memory_space_constraint(a, pltpu.HBM) for a in arrays))


def copy_out(in_ref, out_ref, sem):
    copy = pltpu.make_async_copy(in_ref, out_ref, sem)
    copy.start()
    copy.wait()


def ring_call(mesh_shape, matrix_rows, tile_owner, tile_slot):
    nx, ny = mesh_shape
    rows, width = matrix_rows.shape
    half_tiles, half_x = ny // 2, nx // 2
    capacity = nx // 4 + 1
    slots = -(-tile_owner.shape[0] // (nx * ny))
    _, piece_count = piece_lists(half_tiles, half_x)
    reach = max(ny // 4, 1)
    f32, bf16 = jnp.float32, jnp.bfloat16
    dma = pltpu.SemaphoreType.DMA
    return pl.pallas_call(
        functools.partial(kernel, (nx, ny, half_tiles, half_x, capacity, slots)),
        out_shape=jax.ShapeDtypeStruct((slots, 2 * rows, 2 * rows), f32),
        in_specs=[
            pl.BlockSpec(memory_space=pltpu.VMEM),
            pl.BlockSpec(memory_space=pltpu.SMEM),
            pl.BlockSpec(memory_space=pltpu.SMEM),
        ],
        out_specs=pl.BlockSpec(memory_space=pltpu.VMEM),
        scratch_shapes=[
            pltpu.VMEM((ny, rows, width), f32),
            pltpu.VMEM((half_x, rows, width), f32),
            pltpu.VMEM((ny, rows, width), bf16),
            pltpu.VMEM((ny, rows, width), bf16),
            pltpu.VMEM((half_x + 1, 2, rows, width), bf16),
            pltpu.VMEM((2, piece_count, 2, rows // 2, rows), f32),
            pltpu.VMEM((2, ny, 2 * capacity, rows // 2, rows), f32),
            pltpu.VMEM((2, ny * 2 * capacity, rows // 2, rows), f32),
            pltpu.SMEM((piece_count,), jnp.int32),
            dma((reach, 2)), dma((reach, 2)), dma((reach, 2)), dma((reach, 2)),
            dma((2 * reach + 1, 2)), dma((2 * reach + 1, 2)),
            dma((half_x, 2)), dma((half_x, 2)),
            dma((2, ny)), dma((2, ny)),
        ],
        compiler_params=pltpu.CompilerParams(
            collective_id=0, has_side_effects=True, vmem_limit_bytes=44 * 1024 * 1024
        ),
    )(matrix_rows, tile_owner, tile_slot)


def per_device(mesh_shape, matrix_rows, tile_owner, tile_slot):
    nx, ny = mesh_shape
    if ny // 2 == 4 and nx == 4:
        slots = -(-tile_owner.shape[0] // (nx * ny))
        packed = plane_call((nx, ny, ny // 2, slots), matrix_rows, tile_owner, tile_slot)
    else:
        packed = ring_call(mesh_shape, matrix_rows, tile_owner, tile_slot)
    return pl.pallas_call(
        copy_out,
        out_shape=jax.ShapeDtypeStruct(packed.shape, packed.dtype),
        in_specs=[pl.BlockSpec(memory_space=pltpu.VMEM)],
        out_specs=pl.BlockSpec(memory_space=pl.ANY),
        scratch_shapes=[pltpu.SemaphoreType.DMA(())],
        compiler_params=pltpu.CompilerParams(vmem_limit_bytes=4 * 1024 * 1024),
    )(packed)


def solution(mesh):
    placed = (P(("gx", "gy"), None), P(), P())
    return jax.shard_map(
        functools.partial(per_device, (mesh.shape["gx"], mesh.shape["gy"])),
        mesh=mesh,
        in_specs=placed,
        out_specs=P(("gx", "gy"), None, None),
        check_vma=False,
    )
```

```python
import functools

import jax
import jax.numpy as jnp
from jax import lax
from jax.experimental import pallas as pl
from jax.experimental.pallas import tpu as pltpu
from jax.sharding import PartitionSpec as P

MESH = pl.DeviceIdType.MESH


def chip_position(chip, chips):
    row, col = lax.div(chip, 2), lax.rem(chip, 2)
    return col * (1 + row) + (1 - col) * lax.rem(chips - row, chips)


def chip_at(position, chips):
    behind = lax.rem(position + chips - 1, chips)
    far = lax.div(behind, chips // 2)
    return (1 - far) * (2 * behind + 1) + far * 2 * (chips - 1 - behind)


def piece_lists(half_tiles, half_x):
    lists, start = [], 0
    for step in range(half_x + 1):
        if step == 0:
            count = half_tiles // 2 + 1
        elif step < half_x:
            count = half_tiles
        else:
            count = half_tiles // 2
        lists.append((step, start, count))
        start += count
    return lists, start


def piece(x, r, step, i, nx, half_tiles, half_x):
    source = lax.rem(x - step + nx, nx)
    if step == 0:
        col = lax.rem(r - i + half_tiles, half_tiles)
        valid = jnp.logical_or(i < half_tiles // 2, r < half_tiles // 2)
        rowwise = col <= r
    elif step < half_x:
        col = i
        valid = i >= 0
        rowwise = source > x
    else:
        flag = jnp.where(x >= half_x, 1, 0)
        col = 2 * i + lax.rem(r + flag, 2)
        valid = i >= 0
        rowwise = source > x
    other, mine = source * half_tiles + r, x * half_tiles + col
    row_tile = jnp.where(rowwise, other, mine)
    col_tile = jnp.where(rowwise, mine, other)
    tile = jnp.where(valid, row_tile * (row_tile + 1) // 2 + col_tile, 0)
    return col, valid, rowwise, tile


def kernel(
    dims, rows_ref, owner_ref, slot_ref, out_ref,
    gath, zbuf, chi, clo, zsplit, pieces, outgoing, incoming, targets,
    gs_r, gr_r, gs_l, gr_l, ss, sr, zs, zr, xs, xr,
):
    nx, ny, half_tiles, half_x, capacity, slots = dims
    rows = rows_ref.shape[0]
    half = rows // 2
    chips = ny // 2
    reach = chips // 2
    x = lax.axis_index("gx")
    y = lax.axis_index("gy")
    core = lax.rem(y, 2)
    chip = lax.div(y, 2)
    right_x, left_x = lax.rem(x + 1, nx), lax.rem(x + nx - 1, nx)
    sibling = y + 1 - 2 * core
    place = chip_position(chip, chips)

    def at(position):
        return 2 * chip_at(lax.rem(position + chips, chips), chips) + core

    next_y, prev_y = at(place + 1), at(place - 1)
    lists, piece_count = piece_lists(half_tiles, half_x)

    barrier = pltpu.get_barrier_semaphore()
    for other in (right_x, left_x):
        pl.semaphore_signal(barrier, inc=1, device_id=(other, y), device_id_type=MESH)
    for offset in range(1, ny):
        pl.semaphore_signal(
            barrier, inc=1, device_id=(x, lax.rem(y + offset, ny)), device_id_type=MESH
        )
    pl.semaphore_wait(barrier, ny + 1)

    started = []

    def send(src, dst, send_sem, recv_sem, target):
        copy = pltpu.make_async_remote_copy(
            src_ref=src, dst_ref=dst, send_sem=send_sem, recv_sem=recv_sem,
            device_id=target, device_id_type=MESH,
        )
        copy.start()
        started.append(copy)

    def part(h):
        return pl.ds(h * half, half)

    def zcopy(step, h):
        src = rows_ref.at[part(h)] if step == 1 else zbuf.at[step - 2, part(h)]
        send(src, zbuf.at[step - 1, part(h)], zs.at[step - 1, h], zr.at[step - 1, h], (right_x, y))

    def block(owner, h):
        return gath.at[owner, part(h)]

    def ring(direction, distance, h):
        owner = at(place - direction * (distance - 1))
        src = rows_ref.at[part(h)] if distance == 1 else block(owner, h)
        s, r = (gs_r, gr_r) if direction == 1 else (gs_l, gr_l)
        target = next_y if direction == 1 else prev_y
        send(src, block(owner, h), s.at[distance - 1, h], r.at[distance - 1, h], (x, target))

    def cross(number, owner, h):
        src = rows_ref.at[part(h)] if number == 0 else block(owner, h)
        send(src, block(owner, h), ss.at[number, h], sr.at[number, h], (x, sibling))

    def halves_of(direction, distance):
        if distance < reach:
            return (0, 1) if direction == 1 else (1, 0)
        return (0,) if direction == 1 else (1,)

    def split(value, hi_ref, lo_ref, index):
        hi = value.astype(jnp.bfloat16)
        hi_ref[index] = hi
        lo_ref[index] = (value - hi.astype(jnp.float32)).astype(jnp.bfloat16)

    zcopy(1, 0)
    ring(1, 1, 0)
    if reach > 1:
        ring(-1, 1, 1)
        zcopy(1, 1)
        ring(1, 1, 1)
        ring(-1, 1, 0)
    else:
        ring(-1, 1, 1)
        zcopy(1, 1)
    cross(0, y, 0)
    cross(0, y, 1)

    for step, first, count in lists:
        def fill(i, carry, step=step, first=first):
            _, valid, _, tile = piece(x, chip, step, i, nx, half_tiles, half_x)
            targets[first + i] = jnp.where(valid, lax.rem(owner_ref[tile], ny), ny)
            return carry
        lax.fori_loop(0, count, fill, 0)

    me = x * ny + y

    def class_loop(r, carry):
        state = (jnp.int32(0),) + carry
        for step, first, count in lists:
            def look(i, state, step=step):
                seen, found = state[0], state[1:]
                _, valid, rowwise, tile = piece(x, r, step, i, nx, half_tiles, half_x)
                mine = jnp.where(valid, jnp.where(owner_ref[tile] == me, 1, 0), 0)
                slot = slot_ref[tile]
                code = 2 * (r * capacity + jnp.minimum(seen, capacity - 1))
                code = code + jnp.where(rowwise, 1, 0)
                key = jnp.where(mine == 1, slot, slots)
                found = tuple(jnp.where(key == s, code, found[s]) for s in range(slots))
                return (seen + mine,) + found
            state = lax.fori_loop(0, count, look, state)
        return state[1:]

    found = lax.fori_loop(0, half_tiles, class_loop, (jnp.int32(-1),) * slots)

    chosen = []
    for offset in range(ny):
        dest = lax.rem(y + offset, ny)

        def pick(p, state, dest=dest):
            hit = jnp.where(targets[p] == dest, 1, 0)
            seen = state[0]
            key = jnp.where(hit == 1, seen, capacity)
            picks = tuple(jnp.where(key == k, p, state[1 + k]) for k in range(capacity))
            return (seen + hit,) + picks

        chosen.append(lax.fori_loop(0, piece_count, pick, (jnp.int32(0),) * (capacity + 1))[1:])

    def wait_recv(dst, sem):
        pltpu.make_async_remote_copy(
            src_ref=dst, dst_ref=dst, send_sem=sem, recv_sem=sem,
            device_id=(x, sibling), device_id_type=MESH,
        ).wait_recv()

    def split_other(step, h):
        ref = rows_ref.at[part(h)] if step == 0 else zbuf.at[step - 1, part(h)]
        value = ref[...]
        hi = value.astype(jnp.bfloat16)
        zsplit[step, h, :half] = hi
        zsplit[step, h, half:] = (value - hi.astype(jnp.float32)).astype(jnp.bfloat16)

    def take_other(step, h):
        wait_recv(zbuf.at[step - 1, part(h)], zr.at[step - 1, h])
        if step < half_x:
            zcopy(step + 1, h)

    split_other(0, 0)
    split_other(0, 1)
    split(rows_ref[...], chi, clo, y)

    def take_cross(number, owner, halves):
        for h in halves:
            wait_recv(block(owner, h), sr.at[number, h])

    one = functools.partial(
        lax.dot_general,
        dimension_numbers=(((1,), (1,)), ((), ())),
        preferred_element_type=jnp.float32,
    )
    width = rows_ref.shape[1]
    row_inside = core * rows + lax.broadcasted_iota(jnp.int32, (half, 2 * rows), 0)
    col_inside = lax.broadcasted_iota(jnp.int32, (half, 2 * rows), 1)

    def one_piece_of(h):
        above = jnp.where(row_inside + h * half < col_inside, 1, 0)

        def one_piece(i, step, first, col):
            b_hi = chi[pl.ds(2 * col, 2)].reshape(2 * rows, width)
            b_lo = clo[pl.ds(2 * col, 2)].reshape(2 * rows, width)
            both = one(zsplit[step, h], b_hi)
            full = both[:half] + (both[half:] + one(zsplit[step, h, :half], b_lo))
            if step == 0:
                full = jnp.where(above * jnp.where(i == 0, 1, 0) == 1, 0.0, full)
            pieces[h, first + i, 0] = full[:, :rows]
            pieces[h, first + i, 1] = full[:, rows:]

        return one_piece

    farthest = chip_at(lax.rem(place + reach, chips), chips)
    soon = min(reach, half_x) if reach > 1 else 0

    def multiply(h, mode):
        one_piece = one_piece_of(h)
        for step, first, count in lists:
            if mode == "early" and step >= soon:
                continue

            def make(i, carry, step=step, first=first):
                col, _, _, _ = piece(x, chip, step, i, nx, half_tiles, half_x)
                if mode == "all" or step >= soon:
                    one_piece(i, step, first, col)
                else:
                    wanted = (col != farthest) if mode == "early" else (col == farthest)
                    pl.when(wanted)(lambda: one_piece(i, step, first, col))
                return carry
            lax.fori_loop(0, count, make, 0)

    pending = [(0, sibling, (0, 1))]
    for distance in range(1, reach + 1):
        if distance == reach:
            for number, owner, halves in pending[1:]:
                take_cross(number, owner, halves)
                split(gath[owner], chi, clo, owner)
            multiply(0, "early")
        if distance <= half_x:
            for h in (0, 1):
                if (distance, h) != (half_x, 1):
                    take_other(distance, h)
                if h in halves_of(1, distance):
                    owner = at(place - distance)
                    wait_recv(block(owner, h), gr_r.at[distance - 1, h])
                    if distance < reach and h in halves_of(1, distance + 1):
                        ring(1, distance + 1, h)
                    cross(2 * distance - 1, owner, h)
                g = 1 - h
                if g in halves_of(-1, distance):
                    owner = at(place + distance)
                    wait_recv(block(owner, g), gr_l.at[distance - 1, g])
                    if distance < reach and g in halves_of(-1, distance + 1):
                        ring(-1, distance + 1, g)
                    cross(2 * distance, owner, g)
            split_other(distance, 0)
            if distance < half_x:
                split_other(distance, 1)
        behind, ahead = at(place - distance), at(place + distance)
        pending.append((2 * distance - 1, behind + 1 - 2 * core, halves_of(1, distance)))
        pending.append((2 * distance, ahead + 1 - 2 * core, halves_of(-1, distance)))
        split(gath[behind], chi, clo, behind)
        if distance < reach:
            split(gath[ahead], chi, clo, ahead)
        for number, owner, halves in pending[: (1 if distance == 1 else 0)]:
            take_cross(number, owner, halves)
            split(gath[owner], chi, clo, owner)
    for number, owner, halves in pending[-2:]:
        take_cross(number, owner, halves)
    split(gath[pending[-1][1]], chi, clo, pending[-1][1])
    for step in range(reach + 1, half_x + 1):
        for h in (0, 1):
            if (step, h) != (half_x, 1):
                take_other(step, h)
                split_other(step, h)

    def arrival(offset):
        return pl.ds(offset * capacity * 2, capacity * 2)

    def exchange(h, offset):
        send(
            outgoing.at[h, offset], incoming.at[h, arrival(offset)],
            xs.at[h, offset], xr.at[h, offset], (x, lax.rem(y + offset, ny)),
        )

    for h in (0, 1):
        if h == 1:
            take_other(half_x, 1)
            split_other(half_x, 1)
        multiply(h, "all" if h == 1 else "late")
        for offset in range(1, ny):
            for k in range(capacity):
                outgoing[h, offset, 2 * k:2 * k + 2] = pieces[h, chosen[offset][k]]
            if offset > 1:
                exchange(h, offset - 1)
        for k in range(capacity):
            incoming[h, 2 * k:2 * k + 2] = pieces[h, chosen[0][k]]
        exchange(h, ny - 1)
    for h in (0, 1):
        for offset in range(1, ny):
            wait_recv(incoming.at[h, arrival(offset)], xr.at[h, offset])

    for s in range(slots):
        code = found[s]
        there = code >= 0
        safe = jnp.maximum(code, 0)
        rowwise = lax.rem(safe, 2) == 1
        rank = lax.rem(safe // 2, capacity)
        first_source = 2 * (safe // (2 * capacity))
        bases = [
            (lax.rem(y - first_source - h + ny, ny) * capacity + rank) * 2 for h in (0, 1)
        ]
        for i in (0, 1):
            for j in (0, 1):
                place_of = jnp.where(rowwise, bases[i] + j, bases[j] + i)
                value = jnp.concatenate([incoming[0, place_of], incoming[1, place_of]], axis=0)
                value = jnp.where(rowwise, value, value.T)
                out_ref[s, i * rows:(i + 1) * rows, j * rows:(j + 1) * rows] = jnp.where(
                    there, value, 0.0
                )
    for copy in started:
        copy.wait_send()


def plane_kernel(
    dims, rows_hbm, owner_hbm, slot_hbm, out_ref,
    gath, zfar, parts, far_parts, far, extra, owner_ref, slot_ref, todo,
    ins, ss, rs, entered,
):
    nx, ny, half_tiles, slots = dims
    rows, width = zfar.shape
    half = rows // 2
    cuts = (0, width * 5 // 8, width)
    x = lax.axis_index("gx")
    y = lax.axis_index("gy")
    core = lax.rem(y, 2)
    chip = lax.div(y, 2)
    twin = 1 - core
    right, left = (lax.rem(x + 1, nx), y), (lax.rem(x + nx - 1, nx), y)
    sibling = (x, y + 1 - 2 * core)
    across = (x, y + 2 - 4 * lax.rem(chip, 2))
    along = (x, lax.rem(y + 4, ny))

    odd, high, ends = lax.rem(chip, 2), lax.div(chip, 2), jnp.where(x == nx - 1, 1, 0)
    earlier = (1 - core, odd, high, jnp.where(x > 0, 1, 0))
    later = (core, 1 - odd, 1 - high, 1 - ends)
    barrier = pltpu.get_barrier_semaphore()

    def signal_if(flag, semaphore, target):
        @pl.when(flag == 1)
        def _():
            pl.semaphore_signal(semaphore, inc=1, device_id=target, device_id_type=MESH)

    for flag, target in zip(later, (sibling, across, along, right)):
        signal_if(flag, barrier, target)
    signal_if(jnp.where(x == 0, 1, 0), barrier, left)
    loads = [
        pltpu.make_async_copy(rows_hbm, gath.at[0, core], ins.at[0]),
        pltpu.make_async_copy(owner_hbm, owner_ref, ins.at[1]),
        pltpu.make_async_copy(slot_hbm, slot_ref, ins.at[2]),
    ]
    for copy in loads:
        copy.start()
    expected = sum(earlier) + ends

    @pl.when(expected > 0)
    def _():
        pl.semaphore_wait(barrier, expected)

    for n, target in enumerate((sibling, across, along, left)):
        signal_if(earlier[n], entered.at[n], target)

    numbers, flying, issued = {}, {}, {}
    ways = {"x": (across, 0, 5), "y": (along, 5, 5), "z": (right, 10, 3), "c": (sibling, 13, 4)}

    def number(name):
        return numbers.setdefault(name, len(numbers))

    def ready(way, name, src, dst, other=None):
        target, base, pool = ways[way]
        turn = issued.get(way, 0)
        issued[way] = turn + 1
        i, j = number(name), base + turn % pool
        if j in flying:
            flying[j].wait_send()
        copy = pltpu.make_async_remote_copy(
            src_ref=src, dst_ref=dst, send_sem=ss.at[j], recv_sem=rs.at[i],
            device_id=target, device_id_type=MESH,
        )
        flying[j] = copy
        if other is None:
            return copy
        return copy, pltpu.make_async_remote_copy(
            src_ref=other, dst_ref=dst, send_sem=ss.at[j], recv_sem=rs.at[i],
            device_id=target, device_id_type=MESH,
        )

    def send(*args):
        ready(*args).start()

    def got(name, dst):
        i = number(name)
        pltpu.make_async_remote_copy(
            src_ref=dst, dst_ref=dst, send_sem=rs.at[i], recv_sem=rs.at[i],
            device_id=sibling, device_id_type=MESH,
        ).wait_recv()

    def block(where, side, h):
        return gath.at[where, side, pl.ds(h * half, half)]

    def cross(where, h, name):
        send("c", ("cross", name), block(where, core, h), block(where, core, h))

    def crossed(where, h, name):
        got(("cross", name), block(where, twin, h))
        split(where, twin, h)

    def both_crossed(where):
        got(("cross", where), gath.at[where, twin])
        split(where, twin, 0)
        split(where, twin, 1)

    def strip(where, side, c):
        return gath.at[where, side, :, pl.ds(cuts[c], cuts[c + 1] - cuts[c])]

    def split_at(where, side, part):
        value = gath[where, side, part[0], part[1]]
        hi = value.astype(jnp.bfloat16)
        parts[where, 0, side, part[0], part[1]] = hi
        parts[where, 1, side, part[0], part[1]] = (
            value - hi.astype(jnp.float32)
        ).astype(jnp.bfloat16)

    def split(where, side, h):
        split_at(where, side, (slice(h * half, (h + 1) * half), slice(None)))

    def split_strip(side, c):
        split_at(7, side, (slice(None), slice(cuts[c], cuts[c + 1])))

    own = [rows_hbm.at[pl.ds(h * half, half)] for h in (0, 1)]
    first = [
        [ready("x", ("x", 0, h), block(0, core, h), block(1, core, h), own[h]) for h in (0, 1)],
        [ready("y", ("y", 0, h), block(0, core, h), block(2, core, h), own[h]) for h in (1, 0)],
        [ready("z", ("z", 0, h), block(0, core, h), block(4, core, h), own[h]) for h in (0, 1)],
    ]

    def open_way(n, early):
        @pl.when(later[n] == (0 if early else 1))
        def _():
            if not early:
                pl.semaphore_wait(entered.at[n], 1)
            for copies in first[n - 1]:
                copies[1 if early else 0].start()

    for n in (1, 2, 3):
        open_way(n, True)
    loads[0].wait()
    for n in (1, 2):
        open_way(n, False)

    @pl.when(later[0] == 1)
    def _():
        pl.semaphore_wait(entered.at[0], 1)

    for h in (0, 1):
        cross(0, h, 0)
    for h in (0, 1):
        split(0, core, h)
    open_way(3, False)
    for copy in loads[1:]:
        copy.wait()

    me = x * ny + y

    def look(tile, state):
        i_tile, j_tile = state[0], state[1]
        a, i = lax.div(i_tile, half_tiles), lax.rem(i_tile, half_tiles)
        b, j = lax.div(j_tile, half_tiles), lax.rem(j_tile, half_tiles)
        i_chip, j_chip = jnp.bitwise_xor(i, chip), jnp.bitwise_xor(j, chip)
        i_near, j_near = jnp.where(a == x, 0, half_tiles), jnp.where(b == x, 0, half_tiles)
        same = jnp.where(i_tile == j_tile, 256, 0)
        last = jnp.where((i_near + i_chip == 7) | (j_near + j_chip == 7), 64, 0)
        near = i_near + i_chip + 8 * (j_near + j_chip) + same + last
        far_code = 128 + jnp.where(
            a == x, j_chip + 8 * lax.div(i, 2), i_chip + 8 * lax.div(j, 2)
        )
        code = jnp.where(a - b == nx // 2, far_code, near)
        key = jnp.where(owner_ref[tile] == me, slot_ref[tile], slots)
        found = tuple(jnp.where(key == s, code, state[2 + s]) for s in range(slots))
        wrap = j_tile == i_tile
        return (
            jnp.where(wrap, i_tile + 1, i_tile), jnp.where(wrap, 0, j_tile + 1)
        ) + found

    codes = lax.fori_loop(
        0, owner_ref.shape[0], look, (jnp.int32(0),) * 2 + (jnp.int32(-1),) * slots
    )[2:]
    seen, picks, ranks = jnp.int32(0), [jnp.int32(0)] * 2, []
    kinds = []
    for s in range(slots):
        code = codes[s]
        kind = jnp.where(code < 0, 3, lax.rem(lax.div(code, 64), 4))
        kinds.append(kind)
        todo[s] = jnp.where(kind == 0, code, 0)
        is_last = jnp.where(kind == 1, 1, 0)
        ranks.append(seen)
        picks = [
            jnp.where(is_last * jnp.where(seen == k, 1, 0) == 1, code, picks[k])
            for k in range(2)
        ]
        seen = seen + is_last
    for k in range(2):
        todo[slots + k] = picks[k]

    one = functools.partial(
        lax.dot_general,
        dimension_numbers=(((1,), (1,)), ((), ())),
        preferred_element_type=jnp.float32,
    )

    def product(code, lo, hi):
        lhs, rhs = lax.rem(code, 8), lax.rem(lax.div(code, 8), 8)
        deep = hi - lo

        def part(n):
            return parts[rhs, n, :, :, lo:hi].reshape(2 * rows, deep)

        both = one(parts[lhs, :, :, :, lo:hi].reshape(4 * rows, deep), part(0))
        return both[:2 * rows] + (
            both[2 * rows:]
            + one(parts[lhs, 0, :, :, lo:hi].reshape(2 * rows, deep), part(1))
        )

    def to_zfar(h):
        send("z", ("z", 1, h), block(4, core, h), zfar.at[pl.ds(h * half, half)])

    got(("x", 0, 0), block(1, core, 0))
    send("y", ("near", 3), block(1, core, 0), block(3, core, 0))
    got(("y", 0, 1), block(2, core, 1))
    send("x", ("near", 3), block(2, core, 1), block(3, core, 1))
    cross(1, 0, (1, 0))
    cross(2, 1, (2, 1))
    got(("z", 0, 0), block(4, core, 0))
    to_zfar(0)
    cross(4, 0, (4, 0))
    split(1, core, 0)
    split(2, core, 1)
    split(4, core, 0)
    both_crossed(0)
    crossed(1, 0, (1, 0))
    crossed(2, 1, (2, 1))
    crossed(4, 0, (4, 0))
    got(("x", 0, 1), block(1, core, 1))
    cross(1, 1, (1, 1))
    got(("y", 0, 0), block(2, core, 0))
    cross(2, 0, (2, 0))
    got(("z", 0, 1), block(4, core, 1))
    to_zfar(1)
    for h in (0, 1):
        send("x", ("next", h), block(4, core, h), block(5, core, h))
        send("y", ("next", h), block(4, core, h), block(6, core, h))
    cross(4, 1, (4, 1))
    split(1, core, 1)
    split(2, core, 0)
    split(4, core, 1)
    crossed(1, 1, (1, 1))
    crossed(2, 0, (2, 0))
    crossed(4, 1, (4, 1))
    got(("near", 3), gath.at[3, core])
    for c in (0, 1):
        send("z", ("z", 3, c), strip(3, core, c), strip(7, core, c))
    for h in (0, 1):
        cross(3, h, 3)
    split(3, core, 0)
    split(3, core, 1)
    both_crossed(3)

    def pair(side, h):
        return gath.at[pl.ds(5, 2), side, pl.ds(h * half, half)]

    def take_next(h):
        got(("next", h), pair(core, h))
        cross(5, h, ("next", h))
        cross(6, h, ("next", h))
        split(5, core, h)
        split(6, core, h)

    def twin_next(h):
        got(("cross", ("next", h)), pair(twin, h))
        split(5, twin, h)
        split(6, twin, h)

    take_next(0)
    twin_next(0)

    def split_far(h):
        part = slice(h * half, (h + 1) * half)
        value = zfar[part]
        hi = value.astype(jnp.bfloat16)
        far_parts[0, part] = hi
        far_parts[1, part] = (value - hi.astype(jnp.float32)).astype(jnp.bfloat16)

    def far_at(where, side, t):
        return far.at[where, side, t]

    def far_cross(where, t):
        send("c", ("far",), far_at(where, core, t), far_at(where, core, t))

    flag = jnp.where(x >= nx // 2, 1, 0)
    def far_tile(t, lo, hi):
        count = hi - lo
        col = flag + 2 * lax.rem(t + lax.div(chip, 2), 2)
        both = one(
            far_parts[:, lo:hi].reshape(2 * count, width),
            parts[col, 0].reshape(2 * rows, width),
        )
        return both[:count] + (
            both[count:] + one(far_parts[0, lo:hi], parts[col, 1].reshape(2 * rows, width))
        )

    def far_rows(t, h):
        full = far_tile(t, h * half, (h + 1) * half)
        for k in (0, 1):
            far[0, core, t, k, h * half:(h + 1) * half] = full[:, k * rows:(k + 1) * rows]

    def far_turned(t):
        full = far_tile(t, 0, rows)
        for k in (0, 1):
            far[0, core, t, k] = full[:, k * rows:(k + 1) * rows].T

    def far_piece(where, t, h):
        return far.at[where, core, t, :, pl.ds(h * half, half)]

    def far_ready(h):
        return [
            ready("x", ("fx", 0, h), far_piece(0, 0, h), far_piece(1, 0, h)),
            ready("y", ("fy", 1, h), far_piece(0, 1, h), far_piece(2, 1, h)),
            ready("x", ("f2",), far_piece(0, 1, h), far_piece(1, 1, h)),
            ready("y", ("f2",), far_piece(0, 0, h), far_piece(2, 0, h)),
        ]

    got(("z", 1, 0), zfar.at[pl.ds(0, half)])
    split_far(0)
    upper = far_ready(0)

    @pl.when(flag == 0)
    def _():
        far_rows(0, 0)
        far_rows(1, 0)
        for copy in upper:
            copy.start()

    got(("z", 1, 1), zfar.at[pl.ds(half, half)])
    split_far(1)
    lower = far_ready(1)

    @pl.when(flag == 0)
    def _():
        far_rows(0, 1)
        lower[0].start()
        far_rows(1, 1)
        for copy in lower[1:]:
            copy.start()

    @pl.when(flag == 1)
    def _():
        far_turned(0)
        far_turned(1)
        for pair_of in zip(upper, lower):
            for copy in pair_of:
                copy.start()

    for t in (0, 1):
        far_cross(0, t)

    take_next(1)
    twin_next(1)

    above = jnp.where(
        lax.broadcasted_iota(jnp.int32, (2 * rows, 2 * rows), 0)
        < lax.broadcasted_iota(jnp.int32, (2 * rows, 2 * rows), 1), 1, 0,
    )

    def local(s, carry):
        code = todo[s]
        masked = jnp.where(code >= 256, 1, 0)
        out_ref[s] = jnp.where(above * masked == 1, 0.0, product(code, 0, width))
        return carry

    def take_strip(c):
        got(("z", 3, c), strip(7, core, c))
        send("c", ("cross", (7, c)), strip(7, core, c), strip(7, core, c))
        split_strip(core, c)

    def twin_strip(c):
        got(("cross", (7, c)), strip(7, twin, c))
        split_strip(twin, c)

    def behind(k, carry):
        extra[k] = product(todo[slots + k], 0, cuts[1])
        return carry

    def behind_more(k, carry):
        extra[k] = extra[k] + product(todo[slots + k], cuts[1], width)
        return carry

    middle = slots // 2
    lax.fori_loop(0, middle, local, 0)
    for h in (0, 1):
        got(("fx", 0, h), far_piece(1, 0, h))
        send("y", ("far", 3, h), far_piece(1, 0, h), far_piece(3, 0, h))
        got(("fy", 1, h), far_piece(2, 1, h))
        send("x", ("far", 3, h), far_piece(2, 1, h), far_piece(3, 1, h))
    far_cross(1, 0)
    far_cross(2, 1)
    take_strip(0)
    lax.fori_loop(middle, slots, local, 0)
    twin_strip(0)
    lax.fori_loop(0, 2, behind, 0)
    got(("f2",), far.at[1, core])
    far_cross(1, 1)
    far_cross(2, 0)
    take_strip(1)
    for h in (0, 1):
        both_tiles = far.at[3, core, :, :, pl.ds(h * half, half)]
        got(("far", 3, h), both_tiles)
        send("c", ("far",), both_tiles, both_tiles)
    twin_strip(1)
    lax.fori_loop(0, 2, behind_more, 0)
    got(("far",), far.at[:, twin])

    for s in range(slots):
        kind, code = kinds[s], jnp.maximum(codes[s], 0)
        where = lax.rem(code, 4)
        t = lax.rem(lax.div(code, 8), 2)
        rank = jnp.minimum(ranks[s], 1)
        for i in (0, 1):
            for j in (0, 1):
                side, k = jnp.where(flag == 0, i, j), jnp.where(flag == 0, j, i)
                at = (s, slice(i * rows, (i + 1) * rows), slice(j * rows, (j + 1) * rows))
                value = jnp.where(kind == 1, extra[rank, at[1], at[2]], out_ref[at])
                value = jnp.where(kind == 2, far[where, side, t, k], value)
                out_ref[at] = jnp.where(kind == 3, 0.0, value)
    for copy in flying.values():
        copy.wait_send()


def plane_call(dims, *arrays):
    nx, ny, half_tiles, slots = dims
    matrix_rows, tile_owner, tile_slot = arrays
    rows, width = matrix_rows.shape
    f32, bf16 = jnp.float32, jnp.bfloat16
    dma = pltpu.SemaphoreType.DMA
    hbm = pl.BlockSpec(memory_space=pltpu.HBM)
    return pl.pallas_call(
        functools.partial(plane_kernel, dims),
        out_shape=jax.ShapeDtypeStruct((slots, 2 * rows, 2 * rows), f32),
        in_specs=[hbm, hbm, hbm],
        out_specs=pl.BlockSpec(memory_space=pltpu.VMEM),
        scratch_shapes=[
            pltpu.VMEM((8, 2, rows, width), f32),
            pltpu.VMEM((rows, width), f32),
            pltpu.VMEM((8, 2, 2, rows, width), bf16),
            pltpu.VMEM((2, rows, width), bf16),
            pltpu.VMEM((4, 2, 2, 2, rows, rows), f32),
            pltpu.VMEM((2, 2 * rows, 2 * rows), f32),
            pltpu.SMEM(tile_owner.shape, jnp.int32),
            pltpu.SMEM(tile_slot.shape, jnp.int32),
            pltpu.SMEM((slots + 2,), jnp.int32),
            dma((3,)), dma((17,)), dma((33,)), pltpu.SemaphoreType.REGULAR((4,)),
        ],
        compiler_params=pltpu.CompilerParams(
            collective_id=0, has_side_effects=True,
            vmem_limit_bytes=44 * 1024 * 1024,
        ),
    )(*(pltpu.with_memory_space_constraint(a, pltpu.HBM) for a in arrays))


def ring_call(mesh_shape, matrix_rows, tile_owner, tile_slot):
    nx, ny = mesh_shape
    rows, width = matrix_rows.shape
    half_tiles, half_x = ny // 2, nx // 2
    capacity = nx // 4 + 1
    slots = -(-tile_owner.shape[0] // (nx * ny))
    _, piece_count = piece_lists(half_tiles, half_x)
    reach = max(ny // 4, 1)
    f32, bf16 = jnp.float32, jnp.bfloat16
    dma = pltpu.SemaphoreType.DMA
    return pl.pallas_call(
        functools.partial(kernel, (nx, ny, half_tiles, half_x, capacity, slots)),
        out_shape=jax.ShapeDtypeStruct((slots, 2 * rows, 2 * rows), f32),
        in_specs=[
            pl.BlockSpec(memory_space=pltpu.VMEM),
            pl.BlockSpec(memory_space=pltpu.SMEM),
            pl.BlockSpec(memory_space=pltpu.SMEM),
        ],
        out_specs=pl.BlockSpec(memory_space=pltpu.VMEM),
        scratch_shapes=[
            pltpu.VMEM((ny, rows, width), f32),
            pltpu.VMEM((half_x, rows, width), f32),
            pltpu.VMEM((ny, rows, width), bf16),
            pltpu.VMEM((ny, rows, width), bf16),
            pltpu.VMEM((half_x + 1, 2, rows, width), bf16),
            pltpu.VMEM((2, piece_count, 2, rows // 2, rows), f32),
            pltpu.VMEM((2, ny, 2 * capacity, rows // 2, rows), f32),
            pltpu.VMEM((2, ny * 2 * capacity, rows // 2, rows), f32),
            pltpu.SMEM((piece_count,), jnp.int32),
            dma((reach, 2)), dma((reach, 2)), dma((reach, 2)), dma((reach, 2)),
            dma((2 * reach + 1, 2)), dma((2 * reach + 1, 2)),
            dma((half_x, 2)), dma((half_x, 2)),
            dma((2, ny)), dma((2, ny)),
        ],
        compiler_params=pltpu.CompilerParams(
            collective_id=0, has_side_effects=True, vmem_limit_bytes=44 * 1024 * 1024
        ),
    )(matrix_rows, tile_owner, tile_slot)


def per_device(mesh_shape, matrix_rows, tile_owner, tile_slot):
    nx, ny = mesh_shape
    if ny // 2 == 4 and nx == 4:
        slots = -(-tile_owner.shape[0] // (nx * ny))
        packed = plane_call((nx, ny, ny // 2, slots), matrix_rows, tile_owner, tile_slot)
    else:
        packed = ring_call(mesh_shape, matrix_rows, tile_owner, tile_slot)
    return packed


def solution(mesh):
    placed = (P(("gx", "gy"), None), P(), P())
    return jax.shard_map(
        functools.partial(per_device, (mesh.shape["gx"], mesh.shape["gy"])),
        mesh=mesh,
        in_specs=placed,
        out_specs=P(("gx", "gy"), None, None),
        check_vma=False,
    )
```

```python
import functools

import jax
import jax.numpy as jnp
from jax import lax
from jax.experimental import pallas as pl
from jax.experimental.pallas import tpu as pltpu
from jax.sharding import PartitionSpec as P

MESH = pl.DeviceIdType.MESH


def chip_position(chip, chips):
    row, col = lax.div(chip, 2), lax.rem(chip, 2)
    return col * (1 + row) + (1 - col) * lax.rem(chips - row, chips)


def chip_at(position, chips):
    behind = lax.rem(position + chips - 1, chips)
    far = lax.div(behind, chips // 2)
    return (1 - far) * (2 * behind + 1) + far * 2 * (chips - 1 - behind)


def piece_lists(half_tiles, half_x):
    lists, start = [], 0
    for step in range(half_x + 1):
        if step == 0:
            count = half_tiles // 2 + 1
        elif step < half_x:
            count = half_tiles
        else:
            count = half_tiles // 2
        lists.append((step, start, count))
        start += count
    return lists, start


def piece(x, r, step, i, nx, half_tiles, half_x):
    source = lax.rem(x - step + nx, nx)
    if step == 0:
        col = lax.rem(r - i + half_tiles, half_tiles)
        valid = jnp.logical_or(i < half_tiles // 2, r < half_tiles // 2)
        rowwise = col <= r
    elif step < half_x:
        col = i
        valid = i >= 0
        rowwise = source > x
    else:
        flag = jnp.where(x >= half_x, 1, 0)
        col = 2 * i + lax.rem(r + flag, 2)
        valid = i >= 0
        rowwise = source > x
    other, mine = source * half_tiles + r, x * half_tiles + col
    row_tile = jnp.where(rowwise, other, mine)
    col_tile = jnp.where(rowwise, mine, other)
    tile = jnp.where(valid, row_tile * (row_tile + 1) // 2 + col_tile, 0)
    return col, valid, rowwise, tile


def kernel(
    dims, rows_ref, owner_ref, slot_ref, out_ref,
    gath, zbuf, chi, clo, zsplit, pieces, outgoing, incoming, targets,
    gs_r, gr_r, gs_l, gr_l, ss, sr, zs, zr, xs, xr,
):
    nx, ny, half_tiles, half_x, capacity, slots = dims
    rows = rows_ref.shape[0]
    half = rows // 2
    chips = ny // 2
    reach = chips // 2
    x = lax.axis_index("gx")
    y = lax.axis_index("gy")
    core = lax.rem(y, 2)
    chip = lax.div(y, 2)
    right_x, left_x = lax.rem(x + 1, nx), lax.rem(x + nx - 1, nx)
    sibling = y + 1 - 2 * core
    place = chip_position(chip, chips)

    def at(position):
        return 2 * chip_at(lax.rem(position + chips, chips), chips) + core

    next_y, prev_y = at(place + 1), at(place - 1)
    lists, piece_count = piece_lists(half_tiles, half_x)

    barrier = pltpu.get_barrier_semaphore()
    for other in (right_x, left_x):
        pl.semaphore_signal(barrier, inc=1, device_id=(other, y), device_id_type=MESH)
    for offset in range(1, ny):
        pl.semaphore_signal(
            barrier, inc=1, device_id=(x, lax.rem(y + offset, ny)), device_id_type=MESH
        )
    pl.semaphore_wait(barrier, ny + 1)

    started = []

    def send(src, dst, send_sem, recv_sem, target):
        copy = pltpu.make_async_remote_copy(
            src_ref=src, dst_ref=dst, send_sem=send_sem, recv_sem=recv_sem,
            device_id=target, device_id_type=MESH,
        )
        copy.start()
        started.append(copy)

    def part(h):
        return pl.ds(h * half, half)

    def zcopy(step, h):
        src = rows_ref.at[part(h)] if step == 1 else zbuf.at[step - 2, part(h)]
        send(src, zbuf.at[step - 1, part(h)], zs.at[step - 1, h], zr.at[step - 1, h], (right_x, y))

    def block(owner, h):
        return gath.at[owner, part(h)]

    def ring(direction, distance, h):
        owner = at(place - direction * (distance - 1))
        src = rows_ref.at[part(h)] if distance == 1 else block(owner, h)
        s, r = (gs_r, gr_r) if direction == 1 else (gs_l, gr_l)
        target = next_y if direction == 1 else prev_y
        send(src, block(owner, h), s.at[distance - 1, h], r.at[distance - 1, h], (x, target))

    def cross(number, owner, h):
        src = rows_ref.at[part(h)] if number == 0 else block(owner, h)
        send(src, block(owner, h), ss.at[number, h], sr.at[number, h], (x, sibling))

    def halves_of(direction, distance):
        if distance < reach:
            return (0, 1) if direction == 1 else (1, 0)
        return (0,) if direction == 1 else (1,)

    def split(value, hi_ref, lo_ref, index):
        hi = value.astype(jnp.bfloat16)
        hi_ref[index] = hi
        lo_ref[index] = (value - hi.astype(jnp.float32)).astype(jnp.bfloat16)

    zcopy(1, 0)
    ring(1, 1, 0)
    if reach > 1:
        ring(-1, 1, 1)
        zcopy(1, 1)
        ring(1, 1, 1)
        ring(-1, 1, 0)
    else:
        ring(-1, 1, 1)
        zcopy(1, 1)
    cross(0, y, 0)
    cross(0, y, 1)

    for step, first, count in lists:
        def fill(i, carry, step=step, first=first):
            _, valid, _, tile = piece(x, chip, step, i, nx, half_tiles, half_x)
            targets[first + i] = jnp.where(valid, lax.rem(owner_ref[tile], ny), ny)
            return carry
        lax.fori_loop(0, count, fill, 0)

    me = x * ny + y

    def class_loop(r, carry):
        state = (jnp.int32(0),) + carry
        for step, first, count in lists:
            def look(i, state, step=step):
                seen, found = state[0], state[1:]
                _, valid, rowwise, tile = piece(x, r, step, i, nx, half_tiles, half_x)
                mine = jnp.where(valid, jnp.where(owner_ref[tile] == me, 1, 0), 0)
                slot = slot_ref[tile]
                code = 2 * (r * capacity + jnp.minimum(seen, capacity - 1))
                code = code + jnp.where(rowwise, 1, 0)
                key = jnp.where(mine == 1, slot, slots)
                found = tuple(jnp.where(key == s, code, found[s]) for s in range(slots))
                return (seen + mine,) + found
            state = lax.fori_loop(0, count, look, state)
        return state[1:]

    found = lax.fori_loop(0, half_tiles, class_loop, (jnp.int32(-1),) * slots)

    chosen = []
    for offset in range(ny):
        dest = lax.rem(y + offset, ny)

        def pick(p, state, dest=dest):
            hit = jnp.where(targets[p] == dest, 1, 0)
            seen = state[0]
            key = jnp.where(hit == 1, seen, capacity)
            picks = tuple(jnp.where(key == k, p, state[1 + k]) for k in range(capacity))
            return (seen + hit,) + picks

        chosen.append(lax.fori_loop(0, piece_count, pick, (jnp.int32(0),) * (capacity + 1))[1:])

    def wait_recv(dst, sem):
        pltpu.make_async_remote_copy(
            src_ref=dst, dst_ref=dst, send_sem=sem, recv_sem=sem,
            device_id=(x, sibling), device_id_type=MESH,
        ).wait_recv()

    def split_other(step, h):
        ref = rows_ref.at[part(h)] if step == 0 else zbuf.at[step - 1, part(h)]
        value = ref[...]
        hi = value.astype(jnp.bfloat16)
        zsplit[step, h, :half] = hi
        zsplit[step, h, half:] = (value - hi.astype(jnp.float32)).astype(jnp.bfloat16)

    def take_other(step, h):
        wait_recv(zbuf.at[step - 1, part(h)], zr.at[step - 1, h])
        if step < half_x:
            zcopy(step + 1, h)

    split_other(0, 0)
    split_other(0, 1)
    split(rows_ref[...], chi, clo, y)

    def take_cross(number, owner, halves):
        for h in halves:
            wait_recv(block(owner, h), sr.at[number, h])

    one = functools.partial(
        lax.dot_general,
        dimension_numbers=(((1,), (1,)), ((), ())),
        preferred_element_type=jnp.float32,
    )
    width = rows_ref.shape[1]
    row_inside = core * rows + lax.broadcasted_iota(jnp.int32, (half, 2 * rows), 0)
    col_inside = lax.broadcasted_iota(jnp.int32, (half, 2 * rows), 1)

    def one_piece_of(h):
        above = jnp.where(row_inside + h * half < col_inside, 1, 0)

        def one_piece(i, step, first, col):
            b_hi = chi[pl.ds(2 * col, 2)].reshape(2 * rows, width)
            b_lo = clo[pl.ds(2 * col, 2)].reshape(2 * rows, width)
            both = one(zsplit[step, h], b_hi)
            full = both[:half] + (both[half:] + one(zsplit[step, h, :half], b_lo))
            if step == 0:
                full = jnp.where(above * jnp.where(i == 0, 1, 0) == 1, 0.0, full)
            pieces[h, first + i, 0] = full[:, :rows]
            pieces[h, first + i, 1] = full[:, rows:]

        return one_piece

    farthest = chip_at(lax.rem(place + reach, chips), chips)
    soon = min(reach, half_x) if reach > 1 else 0

    def multiply(h, mode):
        one_piece = one_piece_of(h)
        for step, first, count in lists:
            if mode == "early" and step >= soon:
                continue

            def make(i, carry, step=step, first=first):
                col, _, _, _ = piece(x, chip, step, i, nx, half_tiles, half_x)
                if mode == "all" or step >= soon:
                    one_piece(i, step, first, col)
                else:
                    wanted = (col != farthest) if mode == "early" else (col == farthest)
                    pl.when(wanted)(lambda: one_piece(i, step, first, col))
                return carry
            lax.fori_loop(0, count, make, 0)

    pending = [(0, sibling, (0, 1))]
    for distance in range(1, reach + 1):
        if distance == reach:
            for number, owner, halves in pending[1:]:
                take_cross(number, owner, halves)
                split(gath[owner], chi, clo, owner)
            multiply(0, "early")
        if distance <= half_x:
            for h in (0, 1):
                if (distance, h) != (half_x, 1):
                    take_other(distance, h)
                if h in halves_of(1, distance):
                    owner = at(place - distance)
                    wait_recv(block(owner, h), gr_r.at[distance - 1, h])
                    if distance < reach and h in halves_of(1, distance + 1):
                        ring(1, distance + 1, h)
                    cross(2 * distance - 1, owner, h)
                g = 1 - h
                if g in halves_of(-1, distance):
                    owner = at(place + distance)
                    wait_recv(block(owner, g), gr_l.at[distance - 1, g])
                    if distance < reach and g in halves_of(-1, distance + 1):
                        ring(-1, distance + 1, g)
                    cross(2 * distance, owner, g)
            split_other(distance, 0)
            if distance < half_x:
                split_other(distance, 1)
        behind, ahead = at(place - distance), at(place + distance)
        pending.append((2 * distance - 1, behind + 1 - 2 * core, halves_of(1, distance)))
        pending.append((2 * distance, ahead + 1 - 2 * core, halves_of(-1, distance)))
        split(gath[behind], chi, clo, behind)
        if distance < reach:
            split(gath[ahead], chi, clo, ahead)
        for number, owner, halves in pending[: (1 if distance == 1 else 0)]:
            take_cross(number, owner, halves)
            split(gath[owner], chi, clo, owner)
    for number, owner, halves in pending[-2:]:
        take_cross(number, owner, halves)
    split(gath[pending[-1][1]], chi, clo, pending[-1][1])
    for step in range(reach + 1, half_x + 1):
        for h in (0, 1):
            if (step, h) != (half_x, 1):
                take_other(step, h)
                split_other(step, h)

    def arrival(offset):
        return pl.ds(offset * capacity * 2, capacity * 2)

    def exchange(h, offset):
        send(
            outgoing.at[h, offset], incoming.at[h, arrival(offset)],
            xs.at[h, offset], xr.at[h, offset], (x, lax.rem(y + offset, ny)),
        )

    for h in (0, 1):
        if h == 1:
            take_other(half_x, 1)
            split_other(half_x, 1)
        multiply(h, "all" if h == 1 else "late")
        for offset in range(1, ny):
            for k in range(capacity):
                outgoing[h, offset, 2 * k:2 * k + 2] = pieces[h, chosen[offset][k]]
            if offset > 1:
                exchange(h, offset - 1)
        for k in range(capacity):
            incoming[h, 2 * k:2 * k + 2] = pieces[h, chosen[0][k]]
        exchange(h, ny - 1)
    for h in (0, 1):
        for offset in range(1, ny):
            wait_recv(incoming.at[h, arrival(offset)], xr.at[h, offset])

    for s in range(slots):
        code = found[s]
        there = code >= 0
        safe = jnp.maximum(code, 0)
        rowwise = lax.rem(safe, 2) == 1
        rank = lax.rem(safe // 2, capacity)
        first_source = 2 * (safe // (2 * capacity))
        bases = [
            (lax.rem(y - first_source - h + ny, ny) * capacity + rank) * 2 for h in (0, 1)
        ]
        for i in (0, 1):
            for j in (0, 1):
                place_of = jnp.where(rowwise, bases[i] + j, bases[j] + i)
                value = jnp.concatenate([incoming[0, place_of], incoming[1, place_of]], axis=0)
                value = jnp.where(rowwise, value, value.T)
                out_ref[s, i * rows:(i + 1) * rows, j * rows:(j + 1) * rows] = jnp.where(
                    there, value, 0.0
                )
    for copy in started:
        copy.wait_send()


def plane_kernel(
    dims, rows_hbm, owner_hbm, slot_hbm, out_ref,
    gath, zfar, parts, far_parts, far, extra, owner_ref, slot_ref, todo,
    ins, ss, rs, entered,
):
    nx, ny, half_tiles, slots = dims
    rows, width = zfar.shape
    half = rows // 2
    cuts = (0, width * 5 // 8, width)
    x = lax.axis_index("gx")
    y = lax.axis_index("gy")
    core = lax.rem(y, 2)
    chip = lax.div(y, 2)
    twin = 1 - core
    right, left = (lax.rem(x + 1, nx), y), (lax.rem(x + nx - 1, nx), y)
    sibling = (x, y + 1 - 2 * core)
    across = (x, y + 2 - 4 * lax.rem(chip, 2))
    along = (x, lax.rem(y + 4, ny))

    loads = [
        pltpu.make_async_copy(rows_hbm, gath.at[0, core], ins.at[0]),
        pltpu.make_async_copy(owner_hbm, owner_ref, ins.at[1]),
        pltpu.make_async_copy(slot_hbm, slot_ref, ins.at[2]),
    ]
    for copy in loads:
        copy.start()
    odd, high, ends = lax.rem(chip, 2), lax.div(chip, 2), jnp.where(x == nx - 1, 1, 0)
    earlier = (1 - core, odd, high, jnp.where(x > 0, 1, 0))
    later = (core, 1 - odd, 1 - high, 1 - ends)
    barrier = pltpu.get_barrier_semaphore()

    def signal_if(flag, semaphore, target):
        @pl.when(flag == 1)
        def _():
            pl.semaphore_signal(semaphore, inc=1, device_id=target, device_id_type=MESH)

    for flag, target in zip(later, (sibling, across, along, right)):
        signal_if(flag, barrier, target)
    signal_if(jnp.where(x == 0, 1, 0), barrier, left)
    expected = sum(earlier) + ends

    @pl.when(expected > 0)
    def _():
        pl.semaphore_wait(barrier, expected)

    for n, target in enumerate((sibling, across, along, left)):
        signal_if(earlier[n], entered.at[n], target)

    numbers, flying, issued = {}, {}, {}
    ways = {"x": (across, 0, 5), "y": (along, 5, 5), "z": (right, 10, 3), "c": (sibling, 13, 4)}

    def number(name):
        return numbers.setdefault(name, len(numbers))

    def ready(way, name, src, dst, other=None):
        target, base, pool = ways[way]
        turn = issued.get(way, 0)
        issued[way] = turn + 1
        i, j = number(name), base + turn % pool
        if j in flying:
            flying[j].wait_send()
        copy = pltpu.make_async_remote_copy(
            src_ref=src, dst_ref=dst, send_sem=ss.at[j], recv_sem=rs.at[i],
            device_id=target, device_id_type=MESH,
        )
        flying[j] = copy
        if other is None:
            return copy
        return copy, pltpu.make_async_remote_copy(
            src_ref=other, dst_ref=dst, send_sem=ss.at[j], recv_sem=rs.at[i],
            device_id=target, device_id_type=MESH,
        )

    def send(*args):
        ready(*args).start()

    def got(name, dst):
        i = number(name)
        pltpu.make_async_remote_copy(
            src_ref=dst, dst_ref=dst, send_sem=rs.at[i], recv_sem=rs.at[i],
            device_id=sibling, device_id_type=MESH,
        ).wait_recv()

    def block(where, side, h):
        return gath.at[where, side, pl.ds(h * half, half)]

    def cross(where, h, name):
        send("c", ("cross", name), block(where, core, h), block(where, core, h))

    def crossed(where, h, name):
        got(("cross", name), block(where, twin, h))
        split(where, twin, h)

    def both_crossed(where):
        got(("cross", where), gath.at[where, twin])
        split(where, twin, 0)
        split(where, twin, 1)

    def strip(where, side, c):
        return gath.at[where, side, :, pl.ds(cuts[c], cuts[c + 1] - cuts[c])]

    def split_at(where, side, part):
        value = gath[where, side, part[0], part[1]]
        hi = value.astype(jnp.bfloat16)
        parts[where, 0, side, part[0], part[1]] = hi
        parts[where, 1, side, part[0], part[1]] = (
            value - hi.astype(jnp.float32)
        ).astype(jnp.bfloat16)

    def split(where, side, h):
        split_at(where, side, (slice(h * half, (h + 1) * half), slice(None)))

    def split_strip(side, c):
        split_at(7, side, (slice(None), slice(cuts[c], cuts[c + 1])))

    own = [rows_hbm.at[pl.ds(h * half, half)] for h in (0, 1)]
    first = [
        [ready("x", ("x", 0, h), block(0, core, h), block(1, core, h), own[h]) for h in (0, 1)],
        [ready("y", ("y", 0, h), block(0, core, h), block(2, core, h), own[h]) for h in (1, 0)],
        [ready("z", ("z", 0, h), block(0, core, h), block(4, core, h), own[h]) for h in (0, 1)],
    ]

    def open_way(n, early):
        @pl.when(later[n] == (0 if early else 1))
        def _():
            if not early:
                pl.semaphore_wait(entered.at[n], 1)
            for copies in first[n - 1]:
                copies[1 if early else 0].start()

    for n in (1, 2, 3):
        open_way(n, True)
    loads[0].wait()
    for n in (1, 2):
        open_way(n, False)

    @pl.when(later[0] == 1)
    def _():
        pl.semaphore_wait(entered.at[0], 1)

    for h in (0, 1):
        cross(0, h, 0)
    for h in (0, 1):
        split(0, core, h)
    open_way(3, False)
    for copy in loads[1:]:
        copy.wait()

    me = x * ny + y

    def look(tile, state):
        i_tile, j_tile = state[0], state[1]
        a, i = lax.div(i_tile, half_tiles), lax.rem(i_tile, half_tiles)
        b, j = lax.div(j_tile, half_tiles), lax.rem(j_tile, half_tiles)
        i_chip, j_chip = jnp.bitwise_xor(i, chip), jnp.bitwise_xor(j, chip)
        i_near, j_near = jnp.where(a == x, 0, half_tiles), jnp.where(b == x, 0, half_tiles)
        same = jnp.where(i_tile == j_tile, 256, 0)
        last = jnp.where((i_near + i_chip == 7) | (j_near + j_chip == 7), 64, 0)
        near = i_near + i_chip + 8 * (j_near + j_chip) + same + last
        far_code = 128 + jnp.where(
            a == x, j_chip + 8 * lax.div(i, 2), i_chip + 8 * lax.div(j, 2)
        )
        code = jnp.where(a - b == nx // 2, far_code, near)
        key = jnp.where(owner_ref[tile] == me, slot_ref[tile], slots)
        found = tuple(jnp.where(key == s, code, state[2 + s]) for s in range(slots))
        wrap = j_tile == i_tile
        return (
            jnp.where(wrap, i_tile + 1, i_tile), jnp.where(wrap, 0, j_tile + 1)
        ) + found

    codes = lax.fori_loop(
        0, owner_ref.shape[0], look, (jnp.int32(0),) * 2 + (jnp.int32(-1),) * slots
    )[2:]
    seen, picks, ranks = jnp.int32(0), [jnp.int32(0)] * 2, []
    kinds = []
    for s in range(slots):
        code = codes[s]
        kind = jnp.where(code < 0, 3, lax.rem(lax.div(code, 64), 4))
        kinds.append(kind)
        todo[s] = jnp.where(kind == 0, code, 0)
        is_last = jnp.where(kind == 1, 1, 0)
        ranks.append(seen)
        picks = [
            jnp.where(is_last * jnp.where(seen == k, 1, 0) == 1, code, picks[k])
            for k in range(2)
        ]
        seen = seen + is_last
    for k in range(2):
        todo[slots + k] = picks[k]

    one = functools.partial(
        lax.dot_general,
        dimension_numbers=(((1,), (1,)), ((), ())),
        preferred_element_type=jnp.float32,
    )

    def product(code, lo, hi):
        lhs, rhs = lax.rem(code, 8), lax.rem(lax.div(code, 8), 8)
        deep = hi - lo

        def part(n):
            return parts[rhs, n, :, :, lo:hi].reshape(2 * rows, deep)

        both = one(parts[lhs, :, :, :, lo:hi].reshape(4 * rows, deep), part(0))
        return both[:2 * rows] + (
            both[2 * rows:]
            + one(parts[lhs, 0, :, :, lo:hi].reshape(2 * rows, deep), part(1))
        )

    def to_zfar(h):
        send("z", ("z", 1, h), block(4, core, h), zfar.at[pl.ds(h * half, half)])

    got(("x", 0, 0), block(1, core, 0))
    send("y", ("near", 3), block(1, core, 0), block(3, core, 0))
    got(("y", 0, 1), block(2, core, 1))
    send("x", ("near", 3), block(2, core, 1), block(3, core, 1))
    cross(1, 0, (1, 0))
    cross(2, 1, (2, 1))
    got(("z", 0, 0), block(4, core, 0))
    to_zfar(0)
    cross(4, 0, (4, 0))
    split(1, core, 0)
    split(2, core, 1)
    split(4, core, 0)
    both_crossed(0)
    crossed(1, 0, (1, 0))
    crossed(2, 1, (2, 1))
    crossed(4, 0, (4, 0))
    got(("x", 0, 1), block(1, core, 1))
    cross(1, 1, (1, 1))
    got(("y", 0, 0), block(2, core, 0))
    cross(2, 0, (2, 0))
    got(("z", 0, 1), block(4, core, 1))
    to_zfar(1)
    for h in (0, 1):
        send("x", ("next", h), block(4, core, h), block(5, core, h))
        send("y", ("next", h), block(4, core, h), block(6, core, h))
    cross(4, 1, (4, 1))
    split(1, core, 1)
    split(2, core, 0)
    split(4, core, 1)
    crossed(1, 1, (1, 1))
    crossed(2, 0, (2, 0))
    crossed(4, 1, (4, 1))
    got(("near", 3), gath.at[3, core])
    for c in (0, 1):
        send("z", ("z", 3, c), strip(3, core, c), strip(7, core, c))
    for h in (0, 1):
        cross(3, h, 3)
    split(3, core, 0)
    split(3, core, 1)
    both_crossed(3)

    def pair(side, h):
        return gath.at[pl.ds(5, 2), side, pl.ds(h * half, half)]

    def take_next(h):
        got(("next", h), pair(core, h))
        cross(5, h, ("next", h))
        cross(6, h, ("next", h))
        split(5, core, h)
        split(6, core, h)

    def twin_next(h):
        got(("cross", ("next", h)), pair(twin, h))
        split(5, twin, h)
        split(6, twin, h)

    take_next(0)
    twin_next(0)

    def split_far(h):
        part = slice(h * half, (h + 1) * half)
        value = zfar[part]
        hi = value.astype(jnp.bfloat16)
        far_parts[0, part] = hi
        far_parts[1, part] = (value - hi.astype(jnp.float32)).astype(jnp.bfloat16)

    def far_at(where, side, t):
        return far.at[where, side, t]

    def far_cross(where, t):
        send("c", ("far",), far_at(where, core, t), far_at(where, core, t))

    flag = jnp.where(x >= nx // 2, 1, 0)
    def far_tile(t, lo, hi):
        count = hi - lo
        col = flag + 2 * lax.rem(t + lax.div(chip, 2), 2)
        both = one(
            far_parts[:, lo:hi].reshape(2 * count, width),
            parts[col, 0].reshape(2 * rows, width),
        )
        return both[:count] + (
            both[count:] + one(far_parts[0, lo:hi], parts[col, 1].reshape(2 * rows, width))
        )

    def far_rows(t, h):
        full = far_tile(t, h * half, (h + 1) * half)
        for k in (0, 1):
            far[0, core, t, k, h * half:(h + 1) * half] = full[:, k * rows:(k + 1) * rows]

    def far_turned(t):
        full = far_tile(t, 0, rows)
        for k in (0, 1):
            far[0, core, t, k] = full[:, k * rows:(k + 1) * rows].T

    def far_piece(where, t, h):
        return far.at[where, core, t, :, pl.ds(h * half, half)]

    def far_ready(h):
        return [
            ready("x", ("fx", 0, h), far_piece(0, 0, h), far_piece(1, 0, h)),
            ready("y", ("fy", 1, h), far_piece(0, 1, h), far_piece(2, 1, h)),
            ready("x", ("f2",), far_piece(0, 1, h), far_piece(1, 1, h)),
            ready("y", ("f2",), far_piece(0, 0, h), far_piece(2, 0, h)),
        ]

    got(("z", 1, 0), zfar.at[pl.ds(0, half)])
    split_far(0)
    upper = far_ready(0)

    @pl.when(flag == 0)
    def _():
        far_rows(0, 0)
        far_rows(1, 0)
        for copy in upper:
            copy.start()

    got(("z", 1, 1), zfar.at[pl.ds(half, half)])
    split_far(1)
    lower = far_ready(1)

    @pl.when(flag == 0)
    def _():
        far_rows(0, 1)
        lower[0].start()
        far_rows(1, 1)
        for copy in lower[1:]:
            copy.start()

    @pl.when(flag == 1)
    def _():
        far_turned(0)
        far_turned(1)
        for pair_of in zip(upper, lower):
            for copy in pair_of:
                copy.start()

    for t in (0, 1):
        far_cross(0, t)

    take_next(1)
    twin_next(1)

    above = jnp.where(
        lax.broadcasted_iota(jnp.int32, (2 * rows, 2 * rows), 0)
        < lax.broadcasted_iota(jnp.int32, (2 * rows, 2 * rows), 1), 1, 0,
    )

    def local(s, carry):
        code = todo[s]
        masked = jnp.where(code >= 256, 1, 0)
        out_ref[s] = jnp.where(above * masked == 1, 0.0, product(code, 0, width))
        return carry

    def take_strip(c):
        got(("z", 3, c), strip(7, core, c))
        send("c", ("cross", (7, c)), strip(7, core, c), strip(7, core, c))
        split_strip(core, c)

    def twin_strip(c):
        got(("cross", (7, c)), strip(7, twin, c))
        split_strip(twin, c)

    def behind(k, carry):
        extra[k] = product(todo[slots + k], 0, cuts[1])
        return carry

    def behind_more(k, carry):
        extra[k] = extra[k] + product(todo[slots + k], cuts[1], width)
        return carry

    middle = slots // 2
    lax.fori_loop(0, middle, local, 0)
    for h in (0, 1):
        got(("fx", 0, h), far_piece(1, 0, h))
        send("y", ("far", 3, h), far_piece(1, 0, h), far_piece(3, 0, h))
        got(("fy", 1, h), far_piece(2, 1, h))
        send("x", ("far", 3, h), far_piece(2, 1, h), far_piece(3, 1, h))
    far_cross(1, 0)
    far_cross(2, 1)
    take_strip(0)
    lax.fori_loop(middle, slots, local, 0)
    twin_strip(0)
    lax.fori_loop(0, 2, behind, 0)
    got(("f2",), far.at[1, core])
    far_cross(1, 1)
    far_cross(2, 0)
    take_strip(1)
    for h in (0, 1):
        both_tiles = far.at[3, core, :, :, pl.ds(h * half, half)]
        got(("far", 3, h), both_tiles)
        send("c", ("far",), both_tiles, both_tiles)
    twin_strip(1)
    lax.fori_loop(0, 2, behind_more, 0)
    got(("far",), far.at[:, twin])

    for s in range(slots):
        kind, code = kinds[s], jnp.maximum(codes[s], 0)
        where = lax.rem(code, 4)
        t = lax.rem(lax.div(code, 8), 2)
        rank = jnp.minimum(ranks[s], 1)
        for i in (0, 1):
            for j in (0, 1):
                side, k = jnp.where(flag == 0, i, j), jnp.where(flag == 0, j, i)
                at = (s, slice(i * rows, (i + 1) * rows), slice(j * rows, (j + 1) * rows))
                value = jnp.where(kind == 1, extra[rank, at[1], at[2]], out_ref[at])
                value = jnp.where(kind == 2, far[where, side, t, k], value)
                out_ref[at] = jnp.where(kind == 3, 0.0, value)
    for copy in flying.values():
        copy.wait_send()


def plane_call(dims, *arrays):
    nx, ny, half_tiles, slots = dims
    matrix_rows, tile_owner, tile_slot = arrays
    rows, width = matrix_rows.shape
    f32, bf16 = jnp.float32, jnp.bfloat16
    dma = pltpu.SemaphoreType.DMA
    hbm = pl.BlockSpec(memory_space=pltpu.HBM)
    return pl.pallas_call(
        functools.partial(plane_kernel, dims),
        out_shape=jax.ShapeDtypeStruct((slots, 2 * rows, 2 * rows), f32),
        in_specs=[hbm, hbm, hbm],
        out_specs=pl.BlockSpec(memory_space=pltpu.VMEM),
        scratch_shapes=[
            pltpu.VMEM((8, 2, rows, width), f32),
            pltpu.VMEM((rows, width), f32),
            pltpu.VMEM((8, 2, 2, rows, width), bf16),
            pltpu.VMEM((2, rows, width), bf16),
            pltpu.VMEM((4, 2, 2, 2, rows, rows), f32),
            pltpu.VMEM((2, 2 * rows, 2 * rows), f32),
            pltpu.SMEM(tile_owner.shape, jnp.int32),
            pltpu.SMEM(tile_slot.shape, jnp.int32),
            pltpu.SMEM((slots + 2,), jnp.int32),
            dma((3,)), dma((17,)), dma((33,)), pltpu.SemaphoreType.REGULAR((4,)),
        ],
        compiler_params=pltpu.CompilerParams(
            collective_id=0, has_side_effects=True,
            vmem_limit_bytes=44 * 1024 * 1024,
        ),
    )(*(pltpu.with_memory_space_constraint(a, pltpu.HBM) for a in arrays))


def ring_call(mesh_shape, matrix_rows, tile_owner, tile_slot):
    nx, ny = mesh_shape
    rows, width = matrix_rows.shape
    half_tiles, half_x = ny // 2, nx // 2
    capacity = nx // 4 + 1
    slots = -(-tile_owner.shape[0] // (nx * ny))
    _, piece_count = piece_lists(half_tiles, half_x)
    reach = max(ny // 4, 1)
    f32, bf16 = jnp.float32, jnp.bfloat16
    dma = pltpu.SemaphoreType.DMA
    return pl.pallas_call(
        functools.partial(kernel, (nx, ny, half_tiles, half_x, capacity, slots)),
        out_shape=jax.ShapeDtypeStruct((slots, 2 * rows, 2 * rows), f32),
        in_specs=[
            pl.BlockSpec(memory_space=pltpu.VMEM),
            pl.BlockSpec(memory_space=pltpu.SMEM),
            pl.BlockSpec(memory_space=pltpu.SMEM),
        ],
        out_specs=pl.BlockSpec(memory_space=pltpu.VMEM),
        scratch_shapes=[
            pltpu.VMEM((ny, rows, width), f32),
            pltpu.VMEM((half_x, rows, width), f32),
            pltpu.VMEM((ny, rows, width), bf16),
            pltpu.VMEM((ny, rows, width), bf16),
            pltpu.VMEM((half_x + 1, 2, rows, width), bf16),
            pltpu.VMEM((2, piece_count, 2, rows // 2, rows), f32),
            pltpu.VMEM((2, ny, 2 * capacity, rows // 2, rows), f32),
            pltpu.VMEM((2, ny * 2 * capacity, rows // 2, rows), f32),
            pltpu.SMEM((piece_count,), jnp.int32),
            dma((reach, 2)), dma((reach, 2)), dma((reach, 2)), dma((reach, 2)),
            dma((2 * reach + 1, 2)), dma((2 * reach + 1, 2)),
            dma((half_x, 2)), dma((half_x, 2)),
            dma((2, ny)), dma((2, ny)),
        ],
        compiler_params=pltpu.CompilerParams(
            collective_id=0, has_side_effects=True, vmem_limit_bytes=44 * 1024 * 1024
        ),
    )(matrix_rows, tile_owner, tile_slot)


def per_device(mesh_shape, matrix_rows, tile_owner, tile_slot):
    nx, ny = mesh_shape
    if ny // 2 == 4 and nx == 4:
        slots = -(-tile_owner.shape[0] // (nx * ny))
        packed = plane_call((nx, ny, ny // 2, slots), matrix_rows, tile_owner, tile_slot)
    else:
        packed = ring_call(mesh_shape, matrix_rows, tile_owner, tile_slot)
    return packed


def solution(mesh):
    placed = (P(("gx", "gy"), None), P(), P())
    return jax.shard_map(
        functools.partial(per_device, (mesh.shape["gx"], mesh.shape["gy"])),
        mesh=mesh,
        in_specs=placed,
        out_specs=P(("gx", "gy"), None, None),
        check_vma=False,
    )
```
